32 devices in a mesh: ctx: 8 (over z, x), head: 4 (over y, core).
Axes of the slice: x: 2, y: 2, z: 4, core: 2. Of those that a mesh axis runs over, the one named last changes fastest.
Arguments:
- queries: bfloat16 [4096, 4096], P('ctx', 'head'), may hold values from -6 to 6
- keys: bfloat16 [2, 4096, 4096], P(None, 'ctx', 'head'), may hold values from -6 to 6
- values: bfloat16 [2, 4096, 4096], P(None, 'ctx', 'head'), may hold values from -6 to 6
- betas: float32 [32, 2, 4096], P('head', None, 'ctx'), may hold values from 1.9 to 2
- gate: bfloat16 [4096, 4096], P('ctx', 'head'), may hold values from -6 to 6
- out_weight: bfloat16 [4096, 4096], P('head'), may hold values from -0.125 to 0.125
Outputs:
- mixed: bfloat16 [4096, 4096], P('ctx', 'head')
The draws below stay inside these ranges and needn't reach their ends.
All inputs are finite; a program needn't handle non-finite values.
Results may differ from the reference program's by a relative error of at most 0.02.
Values may be sent and summed in bfloat16 or wider, within the bound.
A program may use at most 128 MiB of HBM per device.

```python
import math
import jax
import jax.numpy as jnp
from jax import lax

D = 4096
HEADS = 32
HEAD_DIM = 128
SPAN = 64
TOKENS = 4096
N_HEAD = 4


def strengthened(values, own_key, source, target, parts, factor):
    owner, partner = [(jnp.arange(values.shape[dim]) // (values.shape[dim] // parts)).reshape([-1 if axis == dim else 1 for axis in range(values.ndim)]) for dim in (source, target)]
    chosen = jax.random.permutation(own_key, parts)[partner]
    strong = (owner == chosen) | (owner == (partner + parts // 2) % parts)
    return jnp.where(strong, factor * values, values)


def block_levels(key, shape, shards, low, largest):
    gain, own = 1.0, jax.random.fold_in(key, 6)
    for axis_at, blocks in shards:
        heights = jnp.exp(jax.random.uniform(jax.random.fold_in(own, axis_at), (blocks,), jnp.float32, low / len(shards), largest / len(shards)))
        gain = gain * jnp.repeat(heights, shape[axis_at] // blocks).reshape([-1 if axis == axis_at else 1 for axis in range(len(shape))])
    return gain


def scatter_about(key, extent, deviation, limit, shards=(), kind=jnp.bfloat16):
    loudness = block_levels(key, extent, shards, -0.22, 0.18) if shards else 1.0
    values = jax.random.normal(key, extent, jnp.float32) * deviation * loudness
    return jnp.minimum(jnp.maximum(values, -limit), limit).astype(kind)


def noise_with(key, shape, deviation, limit, cuts, heavy, kind=jnp.bfloat16):
    entries = deviation * jax.random.normal(key, shape, jnp.float32)
    if cuts:
        entries = entries * block_levels(key, shape, cuts, -0.22, 0.18)
    return jnp.clip(strengthened(entries, jax.random.fold_in(key, 3), *heavy), -limit, limit).astype(kind)


def setup_inputs(seed: int = 0) -> dict:
    key_list = jax.random.split(jax.random.key(seed), 7)
    return {
        "queries": scatter_about(key_list[0], (TOKENS, HEADS * HEAD_DIM), 1.0, 6.0, ((0, 8), (1, 4))),
        "keys": scatter_about(key_list[1], (2, TOKENS, HEADS * HEAD_DIM), 1.0, 6.0, ((1, 8), (2, 4))),
        "values": scatter_about(key_list[2], (2, TOKENS, HEADS * HEAD_DIM), 1.0, 6.0, ((1, 8), (2, 4))),
        "betas": jnp.clip(1.9 + 0.100000024 * jax.random.uniform(key_list[3], (HEADS, 2, TOKENS), jnp.float32) ** block_levels(key_list[3], (HEADS, 2, TOKENS), ((0, 4), (2, 8)), -0.2, 0.2), 1.9, 2.0),
        "gate": scatter_about(key_list[4], (TOKENS, HEADS * HEAD_DIM), 1.0, 6.0, ((0, 8), (1, 4))),
        "out_weight": noise_with(key_list[5], (HEADS * HEAD_DIM, D), (HEADS * HEAD_DIM) ** -0.5, 0.125, ((0, 4),), (0, 1, 4, 2.0)),
    }


def product(left, right_part):
    return jnp.matmul(left, right_part, precision=lax.Precision.HIGHEST)

def flipped(array):
    return jnp.swapaxes(array, -1, -2)

def unit_rows(array):
    array = array.astype(jnp.float32)
    return array * lax.rsqrt(lax.optimization_barrier(jnp.sum(array * array, axis=-1, keepdims=True)) + 1e-06)

def unit_lower_solve(system, right_side):
    order = system.shape[-1]
    width = math.gcd(16, order)
    eye_block = jnp.eye(width, dtype=jnp.float32)
    pieces = []
    for index in range(order // width):
        first = index * width
        rhs = right_side[..., first:first + width, :]
        if index > 0:
            rhs = rhs - product(system[..., first:first + width, :first], jnp.concatenate(pieces, axis=-2))
        lower = system[..., first:first + width, first:first + width] - eye_block
        inverse = eye_block - lower
        power = lower
        degree = 1
        while 2 * degree < width:
            power = product(power, power)
            inverse = product(inverse, eye_block + power)
            degree = 2 * degree
        pieces.append(product(inverse, rhs))
    return jnp.concatenate(pieces, axis=-2)

def block_factors(keys_c, values_c, betas_c, queries_c):
    sub_steps = keys_c.shape[-2]
    block_tokens = queries_c.shape[-2]
    head_size = keys_c.shape[-1]
    row_index = lax.broadcasted_iota(jnp.int32, (sub_steps, sub_steps), 0)
    col_index = lax.broadcasted_iota(jnp.int32, (sub_steps, sub_steps), 1)
    strict_lower = (col_index < row_index).astype(jnp.float32)
    system = jnp.eye(sub_steps, dtype=jnp.float32) + betas_c[..., :, None] * product(keys_c, flipped(keys_c)) * strict_lower
    right_side = betas_c[..., :, None] * jnp.concatenate([keys_c, values_c], axis=-1)
    solved = unit_lower_solve(system, right_side)
    mixing = solved[..., :head_size]
    updates = solved[..., head_size:]
    query_row = lax.broadcasted_iota(jnp.int32, (block_tokens, sub_steps), 0)
    key_col = lax.broadcasted_iota(jnp.int32, (block_tokens, sub_steps), 1)
    causal = (key_col <= 2 * query_row + 1).astype(jnp.float32)
    scores = product(queries_c, flipped(keys_c)) * causal
    local_out = product(scores, updates)
    carry_map = queries_c - product(scores, mixing)
    transit = jnp.eye(head_size, dtype=jnp.float32) - product(flipped(keys_c), mixing)
    source = product(flipped(keys_c), updates)
    return (local_out, carry_map, transit, source)

def reference(queries, keys, values, betas, gate, out_weight):
    blocks = TOKENS // SPAN
    query_seq = queries.reshape(blocks, SPAN, HEADS, HEAD_DIM).transpose(0, 2, 1, 3)
    key_seq = keys.reshape(2, blocks, SPAN, HEADS, HEAD_DIM).transpose(1, 3, 2, 0, 4).reshape(blocks, HEADS, 2 * SPAN, HEAD_DIM)
    value_seq = values.reshape(2, blocks, SPAN, HEADS, HEAD_DIM).transpose(1, 3, 2, 0, 4).reshape(blocks, HEADS, 2 * SPAN, HEAD_DIM)
    beta_seq = betas.reshape(HEADS, 2, blocks, SPAN).transpose(2, 0, 3, 1).reshape(blocks, HEADS, 2 * SPAN)

    def advance(state, pieces):
        query_c, key_c, value_c, beta_c = pieces
        local_out, carry_map, transit, source = block_factors(unit_rows(key_c), value_c.astype(jnp.float32), beta_c, unit_rows(query_c))
        return (product(transit, state) + source, local_out + product(carry_map, state))
    start = jnp.zeros((HEADS, HEAD_DIM, HEAD_DIM), jnp.float32)
    final_state, outputs = lax.scan(advance, start, (query_seq, key_seq, value_seq, beta_seq))
    attended = outputs.transpose(0, 2, 1, 3).reshape(TOKENS, HEADS, HEAD_DIM)
    scale = lax.rsqrt(lax.optimization_barrier(jnp.mean(attended * attended, axis=-1, keepdims=True)) + 1e-06)
    mixed_in = (attended * scale * jax.nn.silu(gate.astype(jnp.float32).reshape(TOKENS, HEADS, HEAD_DIM))).astype(jnp.bfloat16)
    mixed_in = mixed_in.reshape(TOKENS, HEADS * HEAD_DIM)
    group = HEADS * HEAD_DIM // N_HEAD

    def add_group(index, total):
        cols = lax.dynamic_slice_in_dim(mixed_in, index * group, group, 1)
        weight = lax.dynamic_slice_in_dim(out_weight, index * group, group, 0)
        part_sum = jnp.dot(cols, weight, preferred_element_type=jnp.float32).astype(jnp.bfloat16)
        part_sum = lax.optimization_barrier(part_sum)
        return total + part_sum.astype(jnp.float32)
    total = lax.fori_loop(0, N_HEAD, add_group, jnp.zeros((TOKENS, D), jnp.float32))
    return total.astype(jnp.bfloat16)
```

```python
import functools

import jax
import jax.numpy as jnp
from jax import lax
from jax.experimental import pallas as pl
from jax.experimental.pallas import tpu as pltpu
from jax.sharding import PartitionSpec as P

HEAD_DIM = 128
SPAN = 64
BASE = 16
F32 = jnp.float32
BF16 = jnp.bfloat16
VMEM_LIMIT = 60 * 1024 * 1024
MESH = pl.DeviceIdType.MESH
PIECES = 4


def iota(shape, dim):
    return lax.broadcasted_iota(jnp.int32, shape, dim)


def split(a):
    high = a.astype(BF16)
    return high, (a - high.astype(F32)).astype(BF16)


def dot(a, b):
    return jnp.dot(a, b, preferred_element_type=F32)


def dot3(a, b):
    ah, al = split(a)
    bh, bl = split(b)
    return dot(jnp.concatenate([ah, al, ah], axis=1), jnp.concatenate([bh, bh, bl], axis=0))


def inverse(lowers, order):
    lane = iota((BASE, order), 1)
    compact = []
    for low in lowers:
        total = jnp.zeros((BASE, order), F32)
        for blk in range(order // BASE):
            total = jnp.where(lane // BASE == blk, low[blk * BASE : (blk + 1) * BASE, :], total)
        compact.append(total)
    inv = [(iota((BASE, order), 0) == lane % BASE).astype(F32) for _ in lowers]
    for j in range(BASE - 1):
        pick = (lane // BASE) * BASE + j
        for n, low in enumerate(compact):
            column = jnp.take_along_axis(low, pick, axis=1, mode="promise_in_bounds")
            inv[n] = inv[n] - column * inv[n][j : j + 1, :]
    row = iota((order, order), 0)
    col = iota((order, order), 1)
    width = BASE
    while width < order:
        corner = (row // (2 * width) == col // (2 * width)) & (row // width != col // width)
        diagonal = row // width == col // width
        second = (iota((width, order), 1) // width) % 2 == 1
        half = [dot3(jnp.where(second, t, 0.0), jnp.where(corner, low, 0.0)) for t, low in zip(inv, lowers)]
        full = [
            jnp.where(diagonal, jnp.concatenate([t] * (order // width), axis=0), 0.0) for t in inv
        ]
        fill = [dot3(y, e) for y, e in zip(half, full)]
        inv = [
            jnp.concatenate([jnp.where(second, 0.0, t), jnp.where(second, t, 0.0) - r], axis=0)
            for t, r in zip(inv, fill)
        ]
        width *= 2
    return inv


def mix_kernel(q_ref, k_ref, v_ref, b_ref, o_ref, m_ref, x_out, x_ref):
    heads = q_ref.shape[1] // HEAD_DIM
    span = q_ref.shape[0]
    order = 2 * span
    step = pl.program_id(0)

    @pl.when(step == 0)
    def _():
        start = (iota((HEAD_DIM, 2 * HEAD_DIM), 0) == iota((HEAD_DIM, 2 * HEAD_DIM), 1)).astype(F32)
        for h in range(heads):
            x_ref[h] = start

    row = iota((order, order), 0)
    col = iota((order, order), 1)
    strict = col < row
    weave = (row == 2 * (col % span) + col // span).astype(BF16)
    causal = iota((span, order), 1) <= 2 * iota((span, order), 0) + 1
    data = []
    lowers = []
    for h in range(heads):
        cols = slice(h * HEAD_DIM, (h + 1) * HEAD_DIM)
        query = q_ref[:, cols]
        pair = jnp.concatenate(
            [
                jnp.concatenate([k_ref[0, :, cols], v_ref[0, :, cols]], axis=1),
                jnp.concatenate([k_ref[1, :, cols], v_ref[1, :, cols]], axis=1),
            ],
            axis=0,
        )
        woven = dot(weave, pair)
        key = woven[:, :HEAD_DIM]
        value = woven[:, HEAD_DIM:]
        key_b = key.astype(BF16)
        norm = lax.rsqrt(jnp.sum(key * key, axis=1, keepdims=True) + 1e-06)
        beta = b_ref[:, h : h + 1]
        both = jnp.concatenate([key_b, query], axis=0)
        gram = lax.dot_general(both, key_b, (((1,), (1,)), ((), ())), preferred_element_type=F32)
        weight = beta * norm * norm
        lowers.append(jnp.where(strict, weight * gram[:order], 0.0))
        scores = jnp.where(causal, gram[order:], 0.0).astype(BF16)
        qf = query.astype(F32)
        q_norm = lax.rsqrt(jnp.sum(qf * qf, axis=1, keepdims=True) + 1e-06)
        readers = jnp.concatenate([key.T.astype(BF16), scores], axis=0)
        data.append((both, readers, beta * norm * value, weight, q_norm))
    solved = inverse(lowers, order)
    seen = []
    for h in range(heads):
        both = data[h][0]
        high, low = split(x_ref[h])
        seen.append(
            dot(jnp.concatenate([both, both], axis=1), jnp.concatenate([high, low], axis=0))
        )
    writes = []
    for h in range(heads):
        _, _, scaled, weight, _ = data[h]
        gap = -weight * seen[h][:order]
        gap = jnp.concatenate([gap[:, :HEAD_DIM], gap[:, HEAD_DIM:] + scaled], axis=1)
        writes.append(dot3(solved[h], gap))
    for h in range(heads):
        cols = slice(h * HEAD_DIM, (h + 1) * HEAD_DIM)
        readers, q_norm = data[h][1], data[h][4]
        high, low = split(writes[h])
        change = dot(
            jnp.concatenate([readers, readers], axis=1), jnp.concatenate([high, low], axis=0)
        )
        x_ref[h] = x_ref[h] + change[:HEAD_DIM]
        out = q_norm * (seen[h][order:] + change[HEAD_DIM:])
        m_ref[:, cols] = out[:, :HEAD_DIM].astype(BF16)
        o_ref[:, cols] = out[:, HEAD_DIM:]

    @pl.when(step == pl.num_programs(0) - 1)
    def _():
        for h in range(heads):
            x_out[h] = x_ref[h].astype(BF16)


def mix(queries, keys, values, beta_cols):
    tokens, width = queries.shape
    heads = width // HEAD_DIM
    return pl.pallas_call(
        mix_kernel,
        grid=(tokens // SPAN,),
        in_specs=[
            pl.BlockSpec((SPAN, width), lambda c: (c, 0)),
            pl.BlockSpec((2, SPAN, width), lambda c: (0, c, 0)),
            pl.BlockSpec((2, SPAN, width), lambda c: (0, c, 0)),
            pl.BlockSpec((2 * SPAN, heads), lambda c: (c, 0)),
        ],
        out_specs=[
            pl.BlockSpec((SPAN, width), lambda c: (c, 0)),
            pl.BlockSpec((SPAN, width), lambda c: (c, 0)),
            pl.BlockSpec((heads, HEAD_DIM, 2 * HEAD_DIM), lambda c: (0, 0, 0)),
        ],
        out_shape=[
            jax.ShapeDtypeStruct((tokens, width), F32),
            jax.ShapeDtypeStruct((tokens, width), BF16),
            jax.ShapeDtypeStruct((heads, HEAD_DIM, 2 * HEAD_DIM), BF16),
        ],
        scratch_shapes=[pltpu.VMEM((heads, HEAD_DIM, 2 * HEAD_DIM), F32)],
        compiler_params=pltpu.CompilerParams(
            dimension_semantics=("arbitrary",), vmem_limit_bytes=VMEM_LIMIT
        ),
    )(queries, keys, values, beta_cols)


def chain_kernel(peers, x_ref, s_ref):
    heads = x_ref.shape[0] // peers
    for h in range(heads):
        state = jnp.zeros((HEAD_DIM, HEAD_DIM), F32)
        for k in range(peers):
            s_ref[k * heads + h] = state.astype(BF16)
            if k < peers - 1:
                maps = x_ref[k * heads + h]
                turn = maps[:, :HEAD_DIM]
                high, low = split(state)
                state = maps[:, HEAD_DIM:].astype(F32) + dot(
                    jnp.concatenate([turn, turn], axis=1), jnp.concatenate([high, low], axis=0)
                )


def dot_t(a, b):
    return lax.dot_general(a, b, (((1,), (1,)), ((), ())), preferred_element_type=F32)


def pair_dot(a, low, high_b, low_b):
    rows = a.shape[0]
    both = dot(jnp.concatenate([a, low], axis=0), jnp.concatenate([high_b, low_b], axis=1))
    width = high_b.shape[1]
    return both[:rows, :width] + both[rows:, :width] + both[:rows, width:]


def block_inverse(lowers, span):
    order = 2 * span
    base = BASE // 2
    lane = iota((base, order), 1)
    group = (lane % span) // base
    compact = []
    for low in lowers:
        halves = []
        for j in range(2):
            total = jnp.zeros((base, order), F32)
            for blk in range(span // base):
                start = j * span + blk * base
                total = jnp.where(group == blk, low[start : start + base, :], total)
            halves.append(total)
        compact.append(jnp.concatenate(halves, axis=0))
    row16, lane16 = iota((BASE, order), 0), iota((BASE, order), 1)
    group16 = (lane16 % span) // base
    own = (row16 % base == lane16 % base) & (row16 // base == lane16 // span)
    inv = [own.astype(F32) for _ in lowers]
    for s in range(BASE - 1):
        t, j = s // 2, s % 2
        pick = j * span + group16 * base + t
        for n, low in enumerate(compact):
            column = jnp.take_along_axis(low, pick, axis=1, mode="promise_in_bounds")
            inv[n] = inv[n] - column * inv[n][j * base + t : j * base + t + 1, :]
    tok_r = iota((order, order), 0) % span
    tok_c = iota((order, order), 1) % span
    pieces = [split(low) for low in lowers]
    width = base
    zero = jnp.zeros((), BF16)
    while width < span:
        diagonal = tok_r // width == tok_c // width
        corner = (tok_r // (2 * width) == tok_c // (2 * width)) & (tok_r // width != tok_c // width)
        second = ((iota((2 * width, order), 1) % span) // width) % 2 == 1
        odd = [jnp.where(second, t, 0.0) for t in inv]
        half = []
        for t, (high, low) in zip(odd, pieces):
            th, tl = split(t)
            half.append(
                pair_dot(th, tl, jnp.where(corner, high, zero), jnp.where(corner, low, zero))
            )
        fill = []
        for t, y in zip(inv, half):
            yh, yl = split(y)
            wide = []
            for j in range(2):
                part = t[j * width : (j + 1) * width]
                if width < 16:
                    part = jnp.concatenate([part] * (16 // width), axis=0)
                ph, pl_ = split(part)
                count = span // part.shape[0]
                wide.append(([ph] * count, [pl_] * count))
            full_h = jnp.concatenate(wide[0][0] + wide[1][0], axis=0)
            full_l = jnp.concatenate(wide[0][1] + wide[1][1], axis=0)
            fill.append(
                pair_dot(yh, yl, jnp.where(diagonal, full_h, zero), jnp.where(diagonal, full_l, zero))
            )
        merged = []
        for t, o, r in zip(inv, odd, fill):
            even, lower = t - o, o - r
            merged.append(
                jnp.concatenate(
                    [even[:width], lower[:width], even[width:], lower[width:]], axis=0
                )
            )
        inv = merged
        width *= 2
    return inv


def prepare(blocks, span):
    order = 2 * span
    row, col = iota((order, order), 0), iota((order, order), 1)
    tok_r, tok_c = row % span, col % span
    strict = (tok_c < tok_r) | ((tok_c == tok_r) & (col < row))
    eye = row == col
    grams = [dot_t(key, key) for key, _, _ in blocks]
    squares = jnp.concatenate(
        [jnp.sum(jnp.where(eye, g, 0.0), axis=0, keepdims=True) for g in grams], axis=0
    )
    beta = jnp.concatenate([b for _, _, b in blocks], axis=0)
    norm = lax.rsqrt(squares + 1e-06)
    value_weight = beta * norm
    weight = value_weight * norm
    weight_cols = weight.T
    lowers = [
        jnp.where(strict, weight_cols[:, n : n + 1] * g, 0.0) for n, g in enumerate(grams)
    ]
    solved = block_inverse(lowers, span)
    results = []
    for n, (key, value, _) in enumerate(blocks):
        th, tl = split(solved[n] * weight[n : n + 1])
        tv = (solved[n] * value_weight[n : n + 1]).astype(BF16)
        turn = dot(jnp.concatenate([th, tl], axis=1), jnp.concatenate([key, key], axis=0))
        write = dot(tv, value)
        ah, al = split(turn)
        bh, bl = split(write)
        stack = jnp.concatenate(
            [jnp.concatenate([ah, bh], axis=1), jnp.concatenate([al, bl], axis=1)], axis=0
        )
        key_t = key.T
        change = dot(jnp.concatenate([key_t, key_t], axis=1), stack)
        transit = jnp.where(eye, 1.0, 0.0) - change[:, :HEAD_DIM]
        results.append((stack, split(transit), change[:, HEAD_DIM:]))
    return results


def fused_kernel(
    seq_axis, peers, axis, q_hbm, k_hbm, v_hbm, b_ref, g_hbm, w_hbm, y_hbm,
    q_ref, k_ref, v_ref, g_ref, beta_ref, stack_ref, turn_ref, source_ref, x_ref, start_ref,
    maps, held, carry_ref, states, s_ref, o_ref, m_ref,
    mixed, weight, total, far_out, far_in, near_out, near_in, cross_out, cross_in, y_ref,
    kv_sem, q_sem, g_sem, load_sem, y_sem, map_send, map_recv, back_send, back_recv,
    far_send, far_recv, near_send, near_recv, cross_send, cross_recv,
):
    heads, blocks, span = q_ref.shape[0], q_ref.shape[1], q_ref.shape[2]
    pairs = heads // 2
    parts = 2
    batch = blocks // parts
    seq = lax.axis_index(seq_axis)
    me = lax.axis_index(axis)
    chip, core = me // 2, me % 2
    sibling = 2 * chip + 1 - core
    across = 2 * (1 - chip) + core
    beyond = 2 * (1 - chip) + 1 - core
    width = y_ref.shape[1]
    rows = y_ref.shape[0] // PIECES

    barrier = pltpu.get_barrier_semaphore()
    for other in (sibling, across):
        pl.semaphore_signal(barrier, inc=1, device_id={axis: other}, device_id_type=MESH)
    for away in range(1, peers):
        pl.semaphore_signal(
            barrier,
            inc=1,
            device_id={seq_axis: lax.rem(seq + away, peers)},
            device_id_type=MESH,
        )

    def columns(h):
        return pl.ds(pl.multiple_of(h * HEAD_DIM, HEAD_DIM), HEAD_DIM)

    def fetch_kv(h):
        return (
            pltpu.make_async_copy(k_hbm.at[:, :, :, columns(h)], k_ref.at[h], kv_sem.at[0, h]),
            pltpu.make_async_copy(v_hbm.at[:, :, :, columns(h)], v_ref.at[h], kv_sem.at[1, h]),
        )

    def fetch_q(h):
        return pltpu.make_async_copy(q_hbm.at[:, :, columns(h)], q_ref.at[h], q_sem.at[h])

    def fetch_g(h):
        return pltpu.make_async_copy(g_hbm.at[:, :, columns(h)], g_ref.at[h], g_sem.at[h])

    def load(n):
        owner = (beyond, across, sibling, me)[n]
        return pltpu.make_async_copy(
            w_hbm.at[:, pl.ds(pl.multiple_of(owner * width, width), width)],
            weight.at[n],
            load_sem.at[n],
        )

    for h in range(heads):
        for copy in fetch_kv(h):
            copy.start()
    for h in range(heads):
        fetch_q(h).start()
    for blk in range(blocks):
        window = slice(blk * span, (blk + 1) * span)
        beta_ref[blk] = jnp.concatenate([b_ref[:, 0, window], b_ref[:, 1, window]], axis=1)
    begin = (iota((HEAD_DIM, 2 * HEAD_DIM), 0) == iota((HEAD_DIM, 2 * HEAD_DIM), 1)).astype(F32)
    for h in range(heads + 2):
        x_ref[h] = begin
    for n in range(2 * batch):
        turn_ref[1, n] = jnp.zeros((HEAD_DIM, 2 * HEAD_DIM), BF16)
        source_ref[1, n] = jnp.zeros((HEAD_DIM, HEAD_DIM), F32)

    def solve(it):
        pair, part = it // parts, it % parts
        work = []
        for b in range(batch):
            for i in range(2):
                h = 2 * pair + i
                blk = part * batch + b
                key = jnp.concatenate([k_ref[h, 0, blk], k_ref[h, 1, blk]], axis=0)
                value = jnp.concatenate([v_ref[h, 0, blk], v_ref[h, 1, blk]], axis=0)
                work.append((key, value, beta_ref[blk, pl.ds(h, 1), :]))
        for n, (stack, (th, tl), source) in enumerate(prepare(work, span)):
            b, i = n // 2, n % 2
            stack_ref[2 * pair + i, part * batch + b] = stack
            turn_ref[it % 2, n] = jnp.concatenate([th, tl], axis=1)
            source_ref[it % 2, n] = source

    def compose(it, pair, part):
        states_now = [x_ref[2 * pair + i] for i in range(2)]
        for b in range(batch):
            for i in range(2):
                n = 2 * b + i
                high, low = split(states_now[i])
                start_ref[2 * pair + i, part * batch + b] = high
                both = turn_ref[it % 2, n]
                moved = dot(
                    jnp.concatenate([both, both[:, :HEAD_DIM]], axis=1),
                    jnp.concatenate([high, high, low], axis=0),
                )
                states_now[i] = jnp.concatenate(
                    [moved[:, :HEAD_DIM], moved[:, HEAD_DIM:] + source_ref[it % 2, n]], axis=1
                )
        for i in range(2):
            x_ref[2 * pair + i] = states_now[i]

    def owner_of(pair, i):
        side = lax.rem(pair + core, 2)
        return peers // 2 - 2 + side + i * (3 - 2 * side)

    def send_map(pair, i, source):
        h = 2 * pair + i
        return pltpu.make_async_remote_copy(
            src_ref=maps.at[h],
            dst_ref=held.at[pair, source],
            send_sem=map_send.at[h],
            recv_sem=map_recv.at[pair, source],
            device_id={seq_axis: owner_of(pair, i)},
            device_id_type=MESH,
        )

    def send_state(pair, i, target):
        h = 2 * pair + i
        return pltpu.make_async_remote_copy(
            src_ref=states.at[pair, target],
            dst_ref=s_ref.at[h],
            send_sem=back_send.at[pair, target],
            recv_sem=back_recv.at[h],
            device_id={seq_axis: target},
            device_id_type=MESH,
        )

    def post(pair):
        for i in range(2):
            h = 2 * pair + i
            maps[h] = x_ref[h].astype(BF16)

            @pl.when((seq != owner_of(pair, i)) & (seq != peers - 1))
            def _():
                send_map(pair, i, seq).start()

            @pl.when(seq == owner_of(pair, i))
            def _():
                held[pair, seq] = maps[h]

    def chain(pair):
        for i in range(2):

            @pl.when(seq == owner_of(pair, i))
            def _():
                carry_ref[...] = jnp.zeros((HEAD_DIM, HEAD_DIM), F32)
                for k in range(peers - 1):

                    @pl.when(seq != k)
                    def _():
                        send_map(pair, i, k).wait_recv()

                    here = held[pair, k]
                    high, low = split(carry_ref[...])
                    turn = here[:, :HEAD_DIM]
                    state = here[:, HEAD_DIM:].astype(F32) + dot(
                        jnp.concatenate([turn, turn], axis=1),
                        jnp.concatenate([high, low], axis=0),
                    )
                    carry_ref[...] = state
                    states[pair, k + 1] = state.astype(BF16)

                    @pl.when(seq != k + 1)
                    def _():
                        send_state(pair, i, k + 1).start()

                    @pl.when(seq == k + 1)
                    def _():
                        s_ref[2 * pair + i] = states[pair, k + 1]

    @pl.when(seq == 0)
    def _():
        s_ref[...] = jnp.zeros(s_ref.shape, BF16)

    def step(it, _):
        @pl.when(it % parts == 0)
        def _():
            for i in range(2):
                for copy in fetch_kv(2 * (it // parts) + i):
                    copy.wait()

        before = it + parts * pairs
        slot = jnp.where(it == 0, pairs, (it - 1 + parts) // parts - 1)
        compose(it + 1, slot, (it + parts - 1) % parts)
        solve(it)

        @pl.when(it == 1)
        def _():
            for n in range(4):
                load(n).start()
            for h in range(heads):
                fetch_g(h).start()

        @pl.when(it == parts)
        def _():
            pl.semaphore_wait(barrier, peers + 1)

        @pl.when((it % parts == 0) & (it > 0))
        def _():
            post(it // parts - 1)

        @pl.when(it == parts * pairs - 2)
        def _():
            chain(0)

        return 0

    lax.fori_loop(0, parts * pairs, step, 0)
    compose(parts * pairs + 1, pairs - 1, parts - 1)
    post(pairs - 1)
    for h in range(heads):
        fetch_q(h).wait()

    def read(pair, _):
        causal = iota((span, 2 * span), 1) % span <= iota((span, 2 * span), 0)
        for i in range(2):
            h = 2 * pair + i
            scores = []
            for blk in range(blocks):
                key = jnp.concatenate([k_ref[h, 0, blk], k_ref[h, 1, blk]], axis=0)
                found = jnp.where(causal, dot_t(q_ref[h, blk], key), 0.0).astype(BF16)
                scores.append(jnp.concatenate([found, found], axis=1))
            drawn = [dot(score, stack_ref[h, blk]) for blk, score in enumerate(scores)]
            for blk in range(blocks):
                kept = (q_ref[h, blk].astype(F32) - drawn[blk][:, :HEAD_DIM]).astype(BF16)
                out = dot(kept, start_ref[h, blk])
                m_ref[h, blk] = out[:, :HEAD_DIM].astype(BF16)
                o_ref[h, blk] = out[:, HEAD_DIM:] + drawn[blk][:, HEAD_DIM:]

        @pl.when(pair != 1)
        def _():
            chain(jnp.maximum(pair, 1))

        return 0

    lax.fori_loop(0, pairs, read, 0)
    for pair in range(pairs):
        for i in range(2):

            @pl.when((seq != owner_of(pair, i)) & (seq != 0))
            def _():
                send_state(pair, i, seq).wait_recv()

    for h in range(heads):
        fetch_g(h).wait()

    def send(source, target, send_sem, recv_sem, t, device):
        return pltpu.make_async_remote_copy(
            src_ref=source.at[t],
            dst_ref=target.at[t],
            send_sem=send_sem.at[t],
            recv_sem=recv_sem.at[t],
            device_id={axis: device},
            device_id_type=MESH,
        )

    def far(t):
        return send(far_out, far_in, far_send, far_recv, t, sibling)

    def near(t):
        return send(near_out, near_in, near_send, near_recv, t, sibling)

    def cross(t):
        return send(cross_out, cross_in, cross_send, cross_recv, t, across)

    def pass_on(t):
        far(t).wait()
        cross_out[t] = (total[t] + far_in[t].astype(F32)).astype(BF16)
        cross(t).start()

    def blend(t):
        count = rows // span
        for h in range(heads):
            window = slice(t * count, (t + 1) * count)
            query = q_ref[h, window].reshape(rows, HEAD_DIM).astype(F32)
            unit = lax.rsqrt(jnp.sum(query * query, axis=1, keepdims=True) + 1e-06)
            seen = o_ref[h, window].reshape(rows, HEAD_DIM) + dot(
                m_ref[h, window].reshape(rows, HEAD_DIM), s_ref[h]
            )
            seen = unit * seen
            scale = lax.rsqrt(jnp.mean(seen * seen, axis=1, keepdims=True) + 1e-06)
            gate = g_ref[h, window].reshape(rows, HEAD_DIM).astype(F32)
            mixed[t, :, h * HEAD_DIM : (h + 1) * HEAD_DIM] = (
                seen * scale * (gate / (1.0 + jnp.exp(-gate)))
            ).astype(BF16)

    for t in range(PIECES):
        blend(t)
        if t == 0:
            load(0).wait()
        far_out[t] = dot(mixed[t], weight[0]).astype(BF16)
        far(t).start()
        if t == 0:
            load(1).wait()
        total[t] = dot(mixed[t], weight[1])
        if t > 0:
            pass_on(t - 1)
    load(2).wait()
    for t in range(PIECES):
        near_out[t] = dot(mixed[t], weight[2]).astype(BF16)
        near(t).start()
        if t == 0:
            pass_on(PIECES - 1)
    load(3).wait()
    for t in range(PIECES):
        total[t] = dot(mixed[t], weight[3])

    def put(t):
        span_t = pl.ds(t * rows, rows)
        return pltpu.make_async_copy(y_ref.at[span_t], y_hbm.at[span_t], y_sem.at[t])

    for t in range(PIECES):
        near(t).wait()
        cross(t).wait()
        y_ref[t * rows : (t + 1) * rows, :] = (
            total[t] + near_in[t].astype(F32) + cross_in[t].astype(F32)
        ).astype(BF16)
        put(t).start()
    for pair in range(pairs):
        for i in range(2):

            @pl.when((seq != owner_of(pair, i)) & (seq != peers - 1))
            def _():
                send_map(pair, i, seq).wait_send()

            @pl.when(seq == owner_of(pair, i))
            def _():
                for k in range(1, peers):

                    @pl.when(seq != k)
                    def _():
                        send_state(pair, i, k).wait_send()

    for t in range(PIECES):
        put(t).wait()


def fused(queries, keys, values, betas, gate, out_weight, seq_axis, axis):
    tokens, depth = queries.shape
    heads = depth // HEAD_DIM
    peers = lax.axis_size(seq_axis)
    width = out_weight.shape[1] // lax.axis_size(axis)
    blocks = tokens // SPAN
    batch = blocks // 2
    vmem = pl.BlockSpec(memory_space=pltpu.VMEM)
    hbm = pl.BlockSpec(memory_space=pl.ANY)
    piece = (PIECES, tokens // PIECES, width)
    square = (HEAD_DIM, HEAD_DIM)
    wide = (HEAD_DIM, 2 * HEAD_DIM)
    pairs = heads // 2
    dma = pltpu.SemaphoreType.DMA
    per_head = (heads, blocks, SPAN, HEAD_DIM)
    both = (heads, 2, blocks, SPAN, HEAD_DIM)
    return pl.pallas_call(
        functools.partial(fused_kernel, seq_axis, peers, axis),
        in_specs=[hbm, hbm, hbm, vmem, hbm, hbm],
        out_specs=hbm,
        out_shape=jax.ShapeDtypeStruct((tokens, width), BF16),
        scratch_shapes=[
            pltpu.VMEM(per_head, BF16),
            pltpu.VMEM(both, BF16),
            pltpu.VMEM(both, BF16),
            pltpu.VMEM(per_head, BF16),
            pltpu.VMEM((blocks, heads, 2 * SPAN), F32),
            pltpu.VMEM((heads, blocks, 4 * SPAN, 2 * HEAD_DIM), BF16),
            pltpu.VMEM((2, 2 * batch) + wide, BF16),
            pltpu.VMEM((2, 2 * batch) + square, F32),
            pltpu.VMEM((heads + 2,) + wide, F32),
            pltpu.VMEM((heads + 2, blocks) + wide, BF16),
            pltpu.VMEM((heads,) + wide, BF16),
            pltpu.VMEM((pairs, peers) + wide, BF16),
            pltpu.VMEM(square, F32),
            pltpu.VMEM((pairs, peers) + square, BF16),
            pltpu.VMEM((heads,) + square, BF16),
            pltpu.VMEM(per_head, F32),
            pltpu.VMEM(per_head, BF16),
            pltpu.VMEM((PIECES, tokens // PIECES, depth), BF16),
            pltpu.VMEM((4, depth, width), BF16),
            pltpu.VMEM(piece, F32),
        ]
        + [pltpu.VMEM(piece, BF16)] * 6
        + [
            pltpu.VMEM((tokens, width), BF16),
            dma((2, heads)),
            dma((heads,)),
            dma((heads,)),
            dma((4,)),
            dma((PIECES,)),
            dma((heads,)),
            dma((pairs, peers)),
            dma((pairs, peers)),
            dma((heads,)),
        ]
        + [dma((PIECES,))] * 6,
        compiler_params=pltpu.CompilerParams(
            collective_id=0, has_side_effects=True, vmem_limit_bytes=VMEM_LIMIT
        ),
    )(
        queries.reshape(blocks, SPAN, depth),
        keys.reshape(2, blocks, SPAN, depth),
        values.reshape(2, blocks, SPAN, depth),
        betas,
        gate.reshape(blocks, SPAN, depth),
        out_weight,
    )


def start_state(maps, axis):
    peers, index = lax.axis_size(axis), lax.axis_index(axis)
    heads = maps.shape[0]
    held = lax.all_gather(maps, axis, axis=0, tiled=True)
    states = pl.pallas_call(
        functools.partial(chain_kernel, peers),
        out_shape=jax.ShapeDtypeStruct((held.shape[0], HEAD_DIM, HEAD_DIM), BF16),
        compiler_params=pltpu.CompilerParams(vmem_limit_bytes=VMEM_LIMIT),
    )(held)
    return lax.dynamic_slice_in_dim(states, index * heads, heads, 0)


def out_kernel(o_ref, m_ref, s_ref, g_ref, w_ref, y_ref, mixed_ref):
    @pl.when(pl.program_id(0) == 0)
    def _():
        for h in range(s_ref.shape[0]):
            cols = slice(h * HEAD_DIM, (h + 1) * HEAD_DIM)
            seen = o_ref[:, cols] + dot(m_ref[:, cols], s_ref[h])
            scale = lax.rsqrt(jnp.mean(seen * seen, axis=1, keepdims=True) + 1e-06)
            gate = g_ref[:, cols].astype(F32)
            mixed_ref[:, cols] = (seen * scale * (gate / (1.0 + jnp.exp(-gate)))).astype(BF16)

    y_ref[...] = dot(mixed_ref[...], w_ref[...]).astype(BF16)


def project(local, reach, states, gate, out_weight):
    tokens, width = local.shape
    total = out_weight.shape[1]
    tile = 512
    whole = pl.BlockSpec((tokens, width), lambda n: (0, 0))
    return pl.pallas_call(
        out_kernel,
        grid=(total // tile,),
        in_specs=[
            whole,
            whole,
            pl.BlockSpec(states.shape, lambda n: (0, 0, 0)),
            whole,
            pl.BlockSpec((width, tile), lambda n: (0, n)),
        ],
        out_specs=pl.BlockSpec((tokens, tile), lambda n: (0, n)),
        out_shape=jax.ShapeDtypeStruct((tokens, total), BF16),
        scratch_shapes=[pltpu.VMEM((tokens, width), BF16)],
        compiler_params=pltpu.CompilerParams(
            dimension_semantics=("arbitrary",), vmem_limit_bytes=VMEM_LIMIT
        ),
    )(local, reach, states, gate, out_weight)


def per_device(queries, keys, values, betas, gate, out_weight):
    heads, _, tokens = betas.shape
    peers, index = lax.axis_size("ctx"), lax.axis_size("head")
    if index == 4 and peers >= 4 and peers % 2 == 0 and heads % 8 == 0 and tokens % (8 * SPAN) == 0:
        return fused(queries, keys, values, betas, gate, out_weight, "ctx", "head")
    beta_cols = betas.transpose(2, 1, 0).reshape(2 * tokens, heads)
    local, reach, maps = mix(queries, keys, values, beta_cols)
    states = start_state(maps, "ctx")
    partial_sum = project(local, reach, states, gate, out_weight)
    return lax.psum_scatter(partial_sum, "head", scatter_dimension=1, tiled=True)


def solution(mesh):
    return jax.shard_map(
        per_device,
        mesh=mesh,
        in_specs=(
            P("ctx", "head"),
            P(None, "ctx", "head"),
            P(None, "ctx", "head"),
            P("head", None, "ctx"),
            P("ctx", "head"),
            P("head", None),
        ),
        out_specs=P("ctx", "head"),
        check_vma=False,
    )
```

```python
import functools

import jax
import jax.numpy as jnp
from jax import lax
from jax.experimental import pallas as pl
from jax.experimental.pallas import tpu as pltpu
from jax.sharding import PartitionSpec as P

HEAD_DIM = 128
SPAN = 64
BASE = 16
F32 = jnp.float32
BF16 = jnp.bfloat16
VMEM_LIMIT = 60 * 1024 * 1024
MESH = pl.DeviceIdType.MESH
PIECES = 4


def iota(shape, dim):
    return lax.broadcasted_iota(jnp.int32, shape, dim)


def split(a):
    high = a.astype(BF16)
    return high, (a - high.astype(F32)).astype(BF16)


def dot(a, b):
    return jnp.dot(a, b, preferred_element_type=F32)


def dot3(a, b):
    ah, al = split(a)
    bh, bl = split(b)
    return dot(jnp.concatenate([ah, al, ah], axis=1), jnp.concatenate([bh, bh, bl], axis=0))


def inverse(lowers, order):
    lane = iota((BASE, order), 1)
    compact = []
    for low in lowers:
        total = jnp.zeros((BASE, order), F32)
        for blk in range(order // BASE):
            total = jnp.where(lane // BASE == blk, low[blk * BASE : (blk + 1) * BASE, :], total)
        compact.append(total)
    inv = [(iota((BASE, order), 0) == lane % BASE).astype(F32) for _ in lowers]
    for j in range(BASE - 1):
        pick = (lane // BASE) * BASE + j
        for n, low in enumerate(compact):
            column = jnp.take_along_axis(low, pick, axis=1, mode="promise_in_bounds")
            inv[n] = inv[n] - column * inv[n][j : j + 1, :]
    row = iota((order, order), 0)
    col = iota((order, order), 1)
    width = BASE
    while width < order:
        corner = (row // (2 * width) == col // (2 * width)) & (row // width != col // width)
        diagonal = row // width == col // width
        second = (iota((width, order), 1) // width) % 2 == 1
        half = [dot3(jnp.where(second, t, 0.0), jnp.where(corner, low, 0.0)) for t, low in zip(inv, lowers)]
        full = [
            jnp.where(diagonal, jnp.concatenate([t] * (order // width), axis=0), 0.0) for t in inv
        ]
        fill = [dot3(y, e) for y, e in zip(half, full)]
        inv = [
            jnp.concatenate([jnp.where(second, 0.0, t), jnp.where(second, t, 0.0) - r], axis=0)
            for t, r in zip(inv, fill)
        ]
        width *= 2
    return inv


def mix_kernel(q_ref, k_ref, v_ref, b_ref, o_ref, m_ref, x_out, x_ref):
    heads = q_ref.shape[1] // HEAD_DIM
    span = q_ref.shape[0]
    order = 2 * span
    step = pl.program_id(0)

    @pl.when(step == 0)
    def _():
        start = (iota((HEAD_DIM, 2 * HEAD_DIM), 0) == iota((HEAD_DIM, 2 * HEAD_DIM), 1)).astype(F32)
        for h in range(heads):
            x_ref[h] = start

    row = iota((order, order), 0)
    col = iota((order, order), 1)
    strict = col < row
    weave = (row == 2 * (col % span) + col // span).astype(BF16)
    causal = iota((span, order), 1) <= 2 * iota((span, order), 0) + 1
    data = []
    lowers = []
    for h in range(heads):
        cols = slice(h * HEAD_DIM, (h + 1) * HEAD_DIM)
        query = q_ref[:, cols]
        pair = jnp.concatenate(
            [
                jnp.concatenate([k_ref[0, :, cols], v_ref[0, :, cols]], axis=1),
                jnp.concatenate([k_ref[1, :, cols], v_ref[1, :, cols]], axis=1),
            ],
            axis=0,
        )
        woven = dot(weave, pair)
        key = woven[:, :HEAD_DIM]
        value = woven[:, HEAD_DIM:]
        key_b = key.astype(BF16)
        norm = lax.rsqrt(jnp.sum(key * key, axis=1, keepdims=True) + 1e-06)
        beta = b_ref[:, h : h + 1]
        both = jnp.concatenate([key_b, query], axis=0)
        gram = lax.dot_general(both, key_b, (((1,), (1,)), ((), ())), preferred_element_type=F32)
        weight = beta * norm * norm
        lowers.append(jnp.where(strict, weight * gram[:order], 0.0))
        scores = jnp.where(causal, gram[order:], 0.0).astype(BF16)
        qf = query.astype(F32)
        q_norm = lax.rsqrt(jnp.sum(qf * qf, axis=1, keepdims=True) + 1e-06)
        readers = jnp.concatenate([key.T.astype(BF16), scores], axis=0)
        data.append((both, readers, beta * norm * value, weight, q_norm))
    solved = inverse(lowers, order)
    seen = []
    for h in range(heads):
        both = data[h][0]
        high, low = split(x_ref[h])
        seen.append(
            dot(jnp.concatenate([both, both], axis=1), jnp.concatenate([high, low], axis=0))
        )
    writes = []
    for h in range(heads):
        _, _, scaled, weight, _ = data[h]
        gap = -weight * seen[h][:order]
        gap = jnp.concatenate([gap[:, :HEAD_DIM], gap[:, HEAD_DIM:] + scaled], axis=1)
        writes.append(dot3(solved[h], gap))
    for h in range(heads):
        cols = slice(h * HEAD_DIM, (h + 1) * HEAD_DIM)
        readers, q_norm = data[h][1], data[h][4]
        high, low = split(writes[h])
        change = dot(
            jnp.concatenate([readers, readers], axis=1), jnp.concatenate([high, low], axis=0)
        )
        x_ref[h] = x_ref[h] + change[:HEAD_DIM]
        out = q_norm * (seen[h][order:] + change[HEAD_DIM:])
        m_ref[:, cols] = out[:, :HEAD_DIM].astype(BF16)
        o_ref[:, cols] = out[:, HEAD_DIM:]

    @pl.when(step == pl.num_programs(0) - 1)
    def _():
        for h in range(heads):
            x_out[h] = x_ref[h].astype(BF16)


def mix(queries, keys, values, beta_cols):
    tokens, width = queries.shape
    heads = width // HEAD_DIM
    return pl.pallas_call(
        mix_kernel,
        grid=(tokens // SPAN,),
        in_specs=[
            pl.BlockSpec((SPAN, width), lambda c: (c, 0)),
            pl.BlockSpec((2, SPAN, width), lambda c: (0, c, 0)),
            pl.BlockSpec((2, SPAN, width), lambda c: (0, c, 0)),
            pl.BlockSpec((2 * SPAN, heads), lambda c: (c, 0)),
        ],
        out_specs=[
            pl.BlockSpec((SPAN, width), lambda c: (c, 0)),
            pl.BlockSpec((SPAN, width), lambda c: (c, 0)),
            pl.BlockSpec((heads, HEAD_DIM, 2 * HEAD_DIM), lambda c: (0, 0, 0)),
        ],
        out_shape=[
            jax.ShapeDtypeStruct((tokens, width), F32),
            jax.ShapeDtypeStruct((tokens, width), BF16),
            jax.ShapeDtypeStruct((heads, HEAD_DIM, 2 * HEAD_DIM), BF16),
        ],
        scratch_shapes=[pltpu.VMEM((heads, HEAD_DIM, 2 * HEAD_DIM), F32)],
        compiler_params=pltpu.CompilerParams(
            dimension_semantics=("arbitrary",), vmem_limit_bytes=VMEM_LIMIT
        ),
    )(queries, keys, values, beta_cols)


def chain_kernel(peers, x_ref, s_ref):
    heads = x_ref.shape[0] // peers
    for h in range(heads):
        state = jnp.zeros((HEAD_DIM, HEAD_DIM), F32)
        for k in range(peers):
            s_ref[k * heads + h] = state.astype(BF16)
            if k < peers - 1:
                maps = x_ref[k * heads + h]
                turn = maps[:, :HEAD_DIM]
                high, low = split(state)
                state = maps[:, HEAD_DIM:].astype(F32) + dot(
                    jnp.concatenate([turn, turn], axis=1), jnp.concatenate([high, low], axis=0)
                )


def dot_t(a, b):
    return lax.dot_general(a, b, (((1,), (1,)), ((), ())), preferred_element_type=F32)


def pair_dot(a, low, high_b, low_b):
    rows = a.shape[0]
    both = dot(jnp.concatenate([a, low], axis=0), jnp.concatenate([high_b, low_b], axis=1))
    width = high_b.shape[1]
    return both[:rows, :width] + both[rows:, :width] + both[:rows, width:]


def weave(*streams):
    order = []
    for n, (count, _) in enumerate(streams):
        order += [((k + 0.5) / count, n) for k in range(count)]
    for _, n in sorted(order):
        next(streams[n][1], None)
    for _, stream in streams:
        for _ in stream:
            pass


def base_solve(lowers, span):
    order = 2 * span
    base = BASE // 2
    lane = iota((base, order), 1)
    group = (lane % span) // base
    compact = []
    for low in lowers:
        halves = []
        for j in range(2):
            total = jnp.zeros((base, order), F32)
            for blk in range(span // base):
                start = j * span + blk * base
                total = jnp.where(group == blk, low[start : start + base, :], total)
            halves.append(total)
        compact.append(jnp.concatenate(halves, axis=0))
        yield
    row16, lane16 = iota((BASE, order), 0), iota((BASE, order), 1)
    group16 = (lane16 % span) // base
    own = (row16 % base == lane16 % base) & (row16 // base == lane16 // span)
    inv = [own.astype(F32) for _ in lowers]
    for s in range(BASE - 1):
        t, j = s // 2, s % 2
        pick = j * span + group16 * base + t
        for n, low in enumerate(compact):
            column = jnp.take_along_axis(low, pick, axis=1, mode="promise_in_bounds")
            inv[n] = inv[n] - column * inv[n][j * base + t : j * base + t + 1, :]
        yield
    return inv


def merge(inv, pieces, span):
    order = 2 * span
    tok_r = iota((order, order), 0) % span
    tok_c = iota((order, order), 1) % span
    width = BASE // 2
    zero = jnp.zeros((), BF16)
    while width < span:
        last = 2 * width == span
        diagonal = tok_r // width == tok_c // width
        corner = (tok_r // (2 * width) == tok_c // (2 * width)) & (tok_r // width != tok_c // width)
        second = ((iota((2 * width, order), 1) % span) // width) % 2 == 1
        odd, half, fill, wide, merged = [], [], [], [], []
        for n, t in enumerate(inv):
            odd.append(jnp.where(second, t, 0.0))
            th, tl = split(odd[n])
            high, low = pieces(n)
            if last:
                y = jnp.where(second, 0.0, pair_dot(th, tl, high, low))
            else:
                y = pair_dot(th, tl, jnp.where(corner, high, zero), jnp.where(corner, low, zero))
            half.append(y)
            parts = []
            for j in range(2):
                part = t[j * width : (j + 1) * width]
                if width < 16:
                    part = jnp.concatenate([part] * (16 // width), axis=0)
                parts.append((split(part), span // part.shape[0]))
            full = [
                jnp.concatenate([p[k] for p, count in parts for _ in range(count)], axis=0)
                for k in range(2)
            ]
            if not last:
                full = [jnp.where(diagonal, f, zero) for f in full]
            wide.append(full)
            yield
        for y, full in zip(half, wide):
            yh, yl = split(y)
            r = pair_dot(yh, yl, full[0], full[1])
            fill.append(jnp.where(second, 0.0, r) if last else r)
            yield
        for t, o, r in zip(inv, odd, fill):
            even, lower = t - o, o - r
            merged.append(
                jnp.concatenate(
                    [even[:width], lower[:width], even[width:], lower[width:]], axis=0
                )
            )
        inv = merged
        width *= 2
    return inv


def fused_kernel(
    seq_axis, peers, axis, q_hbm, k_hbm, v_hbm, b_ref, g_hbm, w_hbm, y_hbm,
    q_ref, k_ref, v_ref, g_ref, beta_ref, stack_ref, turn_ref, source_ref, x_ref, start_ref,
    low_ref, inv_ref, weight_ref, eye_ref,
    maps, held, carry_ref, states, s_ref, o_ref, m_ref,
    mixed, weight, total, far_out, far_in, near_out, near_in, cross_out, cross_in, y_ref,
    kv_sem, q_sem, g_sem, load_sem, y_sem, map_send, map_recv, back_send, back_recv,
    far_send, far_recv, near_send, near_recv, cross_send, cross_recv,
):
    heads, blocks, span = q_ref.shape[0], q_ref.shape[1], q_ref.shape[2]
    pairs = heads // 2
    parts = 2
    batch = blocks // parts
    seq = lax.axis_index(seq_axis)
    me = lax.axis_index(axis)
    chip, core = me // 2, me % 2
    sibling = 2 * chip + 1 - core
    across = 2 * (1 - chip) + core
    beyond = 2 * (1 - chip) + 1 - core
    width = y_ref.shape[1]
    rows = y_ref.shape[0] // PIECES

    barrier = pltpu.get_barrier_semaphore()
    for other in (sibling, across):
        pl.semaphore_signal(barrier, inc=1, device_id={axis: other}, device_id_type=MESH)
    for away in range(1, peers):
        pl.semaphore_signal(
            barrier,
            inc=1,
            device_id={seq_axis: lax.rem(seq + away, peers)},
            device_id_type=MESH,
        )

    def columns(h):
        return pl.ds(pl.multiple_of(h * HEAD_DIM, HEAD_DIM), HEAD_DIM)

    def fetch_kv(h):
        return (
            pltpu.make_async_copy(k_hbm.at[:, :, :, columns(h)], k_ref.at[h], kv_sem.at[0, h]),
            pltpu.make_async_copy(v_hbm.at[:, :, :, columns(h)], v_ref.at[h], kv_sem.at[1, h]),
        )

    def fetch_q(h):
        return pltpu.make_async_copy(q_hbm.at[:, :, columns(h)], q_ref.at[h], q_sem.at[h])

    def fetch_g(h):
        return pltpu.make_async_copy(g_hbm.at[:, :, columns(h)], g_ref.at[h], g_sem.at[h])

    def load(n):
        owner = (beyond, across, sibling, me)[n]
        return pltpu.make_async_copy(
            w_hbm.at[:, pl.ds(pl.multiple_of(owner * width, width), width)],
            weight.at[n],
            load_sem.at[n],
        )

    for h in range(heads):
        for copy in fetch_kv(h):
            copy.start()
    for h in range(heads):
        fetch_q(h).start()
    for blk in range(blocks):
        window = slice(blk * span, (blk + 1) * span)
        beta_ref[blk] = jnp.concatenate([b_ref[:, 0, window], b_ref[:, 1, window]], axis=1)
    begin = (iota((HEAD_DIM, 2 * HEAD_DIM), 0) == iota((HEAD_DIM, 2 * HEAD_DIM), 1)).astype(F32)
    for h in range(heads):
        x_ref[h] = begin
    eye_ref[...] = (iota(eye_ref.shape, 0) == iota(eye_ref.shape, 1)).astype(F32)

    def place(it, n):
        pair, part = it // parts, it % parts
        return 2 * pair + n % 2, part * batch + n // 2

    count = 2 * batch

    def key_of(h, blk):
        return jnp.concatenate([k_ref[h, 0, blk], k_ref[h, 1, blk]], axis=0)

    def solve(it):
        order = 2 * span
        row, col = iota((order, order), 0), iota((order, order), 1)
        tok_r, tok_c = row % span, col % span
        strict = (tok_c < tok_r) | ((tok_c == tok_r) & (col < row))
        slot = it % 2
        grams, squares = [], []
        for n in range(count):
            key = key_of(*place(it, n))
            grams.append(dot_t(key, key))
            yield
        for g in grams:
            squares.append(jnp.sum(eye_ref[...] * g, axis=0, keepdims=True))
            yield
        beta = jnp.concatenate(
            [beta_ref[place(it, n)[1], pl.ds(place(it, n)[0], 1), :] for n in range(count)], axis=0
        )
        norm = lax.rsqrt(jnp.concatenate(squares, axis=0) + 1e-06)
        value_weight = beta * norm
        weight_rows = value_weight * norm
        weight_ref[slot, 0] = weight_rows
        weight_ref[slot, 1] = value_weight
        weight_cols = weight_rows.T
        yield
        lowers = []
        for n, g in enumerate(grams):
            low = jnp.where(strict, weight_cols[:, n : n + 1] * g, 0.0)
            lowers.append(low)
            low_ref[slot, n] = jnp.concatenate(split(low), axis=1)
            yield
        inv = yield from base_solve(lowers, span)
        for n in range(count):
            inv_ref[slot, n] = inv[n]

    def transit(it):
        slot = it % 2

        def pieces(n):
            return low_ref[slot, n, :, : 2 * span], low_ref[slot, n, :, 2 * span :]

        solved = yield from merge([inv_ref[slot, n] for n in range(count)], pieces, span)
        turns, writes, changes = [], [], []
        for n in range(count):
            h, blk = place(it, n)
            th, tl = split(solved[n] * weight_ref[slot, 0, n : n + 1, :])
            tv = (solved[n] * weight_ref[slot, 1, n : n + 1, :]).astype(BF16)
            key = key_of(h, blk)
            value = jnp.concatenate([v_ref[h, 0, blk], v_ref[h, 1, blk]], axis=0)
            turns.append(
                dot(jnp.concatenate([th, tl], axis=1), jnp.concatenate([key, key], axis=0))
            )
            writes.append(dot(tv, value))
            yield
        for n in range(count):
            h, blk = place(it, n)
            ah, al = split(turns[n])
            bh, bl = split(writes[n])
            stack = jnp.concatenate(
                [jnp.concatenate([ah, bh], axis=1), jnp.concatenate([al, bl], axis=1)], axis=0
            )
            stack_ref[h, blk] = stack
            key_t = key_of(h, blk).T
            changes.append(dot(jnp.concatenate([key_t, key_t], axis=1), stack))
            yield
        for n in range(count):
            step = eye_ref[...] - changes[n][:, :HEAD_DIM]
            turn_ref[slot, n] = jnp.concatenate(split(step), axis=1)
            source_ref[slot, n] = changes[n][:, HEAD_DIM:]
            yield

    def compose(it):
        slot = it % 2
        pair, part = it // parts, it % parts
        states_now = [x_ref[2 * pair + i] for i in range(2)]
        for n in range(count):
            h, blk = place(it, n)
            i = n % 2
            high, low = split(states_now[i])
            start_ref[h, blk] = high
            both = turn_ref[slot, n]
            moved = dot(
                jnp.concatenate([both, both[:, :HEAD_DIM]], axis=1),
                jnp.concatenate([high, high, low], axis=0),
            )
            states_now[i] = jnp.concatenate(
                [moved[:, :HEAD_DIM], moved[:, HEAD_DIM:] + source_ref[slot, n]], axis=1
            )
            yield
        for i in range(2):
            x_ref[2 * pair + i] = states_now[i]

    def a_stream(it):
        return 4 * count + BASE, solve(it)

    def b_stream(it):
        return 9 * count, transit(it)

    def c_stream(it):
        return count, compose(it)

    def owner_of(pair, i):
        side = lax.rem(pair + core, 2)
        return peers // 2 - 2 + side + i * (3 - 2 * side)

    def send_map(pair, i, source):
        h = 2 * pair + i
        return pltpu.make_async_remote_copy(
            src_ref=maps.at[h],
            dst_ref=held.at[pair, source],
            send_sem=map_send.at[h],
            recv_sem=map_recv.at[pair, source],
            device_id={seq_axis: owner_of(pair, i)},
            device_id_type=MESH,
        )

    def send_state(pair, i, target):
        h = 2 * pair + i
        return pltpu.make_async_remote_copy(
            src_ref=states.at[pair, target],
            dst_ref=s_ref.at[h],
            send_sem=back_send.at[pair, target],
            recv_sem=back_recv.at[h],
            device_id={seq_axis: target},
            device_id_type=MESH,
        )

    def post(pair):
        for i in range(2):
            h = 2 * pair + i
            maps[h] = x_ref[h].astype(BF16)

            @pl.when((seq != owner_of(pair, i)) & (seq != peers - 1))
            def _():
                send_map(pair, i, seq).start()

            @pl.when(seq == owner_of(pair, i))
            def _():
                held[pair, seq] = maps[h]

    def chain(pair):
        for i in range(2):

            @pl.when(seq == owner_of(pair, i))
            def _():
                carry_ref[...] = jnp.zeros((HEAD_DIM, HEAD_DIM), F32)
                for k in range(peers - 1):

                    @pl.when(seq != k)
                    def _():
                        send_map(pair, i, k).wait_recv()

                    here = held[pair, k]
                    high, low = split(carry_ref[...])
                    turn = here[:, :HEAD_DIM]
                    state = here[:, HEAD_DIM:].astype(F32) + dot(
                        jnp.concatenate([turn, turn], axis=1),
                        jnp.concatenate([high, low], axis=0),
                    )
                    carry_ref[...] = state
                    states[pair, k + 1] = state.astype(BF16)

                    @pl.when(seq != k + 1)
                    def _():
                        send_state(pair, i, k + 1).start()

                    @pl.when(seq == k + 1)
                    def _():
                        s_ref[2 * pair + i] = states[pair, k + 1]

    @pl.when(seq == 0)
    def _():
        s_ref[...] = jnp.zeros(s_ref.shape, BF16)

    def wait_kv(pair):
        for i in range(2):
            for copy in fetch_kv(2 * pair + i):
                copy.wait()

    steps = parts * pairs
    wait_kv(0)
    weave(a_stream(0))
    for n in range(4):
        load(n).start()
    for h in range(heads):
        fetch_g(h).start()
    weave(a_stream(1), b_stream(0))

    def step(it, _):
        @pl.when(it % parts == 0)
        def _():
            wait_kv(it // parts)

        weave(a_stream(it), b_stream(it - 1), c_stream(it - 2))

        @pl.when(it == parts + 1)
        def _():
            pl.semaphore_wait(barrier, peers + 1)

        @pl.when(it % parts == 1)
        def _():
            post(it // parts - 1)

        @pl.when(it == steps - 2)
        def _():
            chain(0)

        return 0

    lax.fori_loop(2, steps, step, 0)
    weave(b_stream(steps - 1), c_stream(steps - 2))
    weave(c_stream(steps - 1))
    post(pairs - 1)
    for h in range(heads):
        fetch_q(h).wait()

    def read(pair, _):
        causal = iota((span, 2 * span), 1) % span <= iota((span, 2 * span), 0)
        for i in range(2):
            h = 2 * pair + i
            scores = []
            for blk in range(blocks):
                found = jnp.where(causal, dot_t(q_ref[h, blk], key_of(h, blk)), 0.0).astype(BF16)
                scores.append(jnp.concatenate([found, found], axis=1))
            drawn = [dot(score, stack_ref[h, blk]) for blk, score in enumerate(scores)]
            for blk in range(blocks):
                kept = (q_ref[h, blk].astype(F32) - drawn[blk][:, :HEAD_DIM]).astype(BF16)
                out = dot(kept, start_ref[h, blk])
                m_ref[h, blk] = out[:, :HEAD_DIM].astype(BF16)
                o_ref[h, blk] = out[:, HEAD_DIM:] + drawn[blk][:, HEAD_DIM:]

        @pl.when(pair != 1)
        def _():
            chain(jnp.maximum(pair, 1))

        return 0

    lax.fori_loop(0, pairs, read, 0)
    for pair in range(pairs):
        for i in range(2):

            @pl.when((seq != owner_of(pair, i)) & (seq != 0))
            def _():
                send_state(pair, i, seq).wait_recv()

    for h in range(heads):
        fetch_g(h).wait()

    def send(source, target, send_sem, recv_sem, t, device):
        return pltpu.make_async_remote_copy(
            src_ref=source.at[t],
            dst_ref=target.at[t],
            send_sem=send_sem.at[t],
            recv_sem=recv_sem.at[t],
            device_id={axis: device},
            device_id_type=MESH,
        )

    def far(t):
        return send(far_out, far_in, far_send, far_recv, t, sibling)

    def near(t):
        return send(near_out, near_in, near_send, near_recv, t, sibling)

    def cross(t):
        return send(cross_out, cross_in, cross_send, cross_recv, t, across)

    def pass_on(t):
        far(t).wait()
        cross_out[t] = (total[t] + far_in[t].astype(F32)).astype(BF16)
        cross(t).start()

    def blend(t):
        held_blocks = rows // span
        for h in range(heads):
            window = slice(t * held_blocks, (t + 1) * held_blocks)
            query = q_ref[h, window].reshape(rows, HEAD_DIM).astype(F32)
            unit = lax.rsqrt(jnp.sum(query * query, axis=1, keepdims=True) + 1e-06)
            seen = o_ref[h, window].reshape(rows, HEAD_DIM) + dot(
                m_ref[h, window].reshape(rows, HEAD_DIM), s_ref[h]
            )
            seen = unit * seen
            scale = lax.rsqrt(jnp.mean(seen * seen, axis=1, keepdims=True) + 1e-06)
            gate = g_ref[h, window].reshape(rows, HEAD_DIM).astype(F32)
            mixed[t, :, h * HEAD_DIM : (h + 1) * HEAD_DIM] = (
                seen * scale * (gate / (1.0 + jnp.exp(-gate)))
            ).astype(BF16)

    for t in range(PIECES):
        blend(t)
        if t == 0:
            load(0).wait()
        far_out[t] = dot(mixed[t], weight[0]).astype(BF16)
        far(t).start()
        if t == 0:
            load(1).wait()
        total[t] = dot(mixed[t], weight[1])
        if t > 0:
            pass_on(t - 1)
    load(2).wait()
    for t in range(PIECES):
        near_out[t] = dot(mixed[t], weight[2]).astype(BF16)
        near(t).start()
        if t == 0:
            pass_on(PIECES - 1)
    load(3).wait()
    for t in range(PIECES):
        total[t] = dot(mixed[t], weight[3])

    def put(t):
        span_t = pl.ds(t * rows, rows)
        return pltpu.make_async_copy(y_ref.at[span_t], y_hbm.at[span_t], y_sem.at[t])

    for t in range(PIECES):
        near(t).wait()
        cross(t).wait()
        y_ref[t * rows : (t + 1) * rows, :] = (
            total[t] + near_in[t].astype(F32) + cross_in[t].astype(F32)
        ).astype(BF16)
        put(t).start()
    for pair in range(pairs):
        for i in range(2):

            @pl.when((seq != owner_of(pair, i)) & (seq != peers - 1))
            def _():
                send_map(pair, i, seq).wait_send()

            @pl.when(seq == owner_of(pair, i))
            def _():
                for k in range(1, peers):

                    @pl.when(seq != k)
                    def _():
                        send_state(pair, i, k).wait_send()

    for t in range(PIECES):
        put(t).wait()


def fused(queries, keys, values, betas, gate, out_weight, seq_axis, axis):
    tokens, depth = queries.shape
    heads = depth // HEAD_DIM
    peers = lax.axis_size(seq_axis)
    width = out_weight.shape[1] // lax.axis_size(axis)
    blocks = tokens // SPAN
    batch = blocks // 2
    vmem = pl.BlockSpec(memory_space=pltpu.VMEM)
    hbm = pl.BlockSpec(memory_space=pl.ANY)
    piece = (PIECES, tokens // PIECES, width)
    square = (HEAD_DIM, HEAD_DIM)
    wide = (HEAD_DIM, 2 * HEAD_DIM)
    pairs = heads // 2
    dma = pltpu.SemaphoreType.DMA
    per_head = (heads, blocks, SPAN, HEAD_DIM)
    both = (heads, 2, blocks, SPAN, HEAD_DIM)
    return pl.pallas_call(
        functools.partial(fused_kernel, seq_axis, peers, axis),
        in_specs=[hbm, hbm, hbm, vmem, hbm, hbm],
        out_specs=hbm,
        out_shape=jax.ShapeDtypeStruct((tokens, width), BF16),
        scratch_shapes=[
            pltpu.VMEM(per_head, BF16),
            pltpu.VMEM(both, BF16),
            pltpu.VMEM(both, BF16),
            pltpu.VMEM(per_head, BF16),
            pltpu.VMEM((blocks, heads, 2 * SPAN), F32),
            pltpu.VMEM((heads, blocks, 4 * SPAN, 2 * HEAD_DIM), BF16),
            pltpu.VMEM((2, 2 * batch) + wide, BF16),
            pltpu.VMEM((2, 2 * batch) + square, F32),
            pltpu.VMEM((heads,) + wide, F32),
            pltpu.VMEM((heads, blocks) + wide, BF16),
            pltpu.VMEM((2, 2 * batch) + wide, BF16),
            pltpu.VMEM((2, 2 * batch, BASE, 2 * SPAN), F32),
            pltpu.VMEM((2, 2, 2 * batch, 2 * SPAN), F32),
            pltpu.VMEM(square, F32),
            pltpu.VMEM((heads,) + wide, BF16),
            pltpu.VMEM((pairs, peers) + wide, BF16),
            pltpu.VMEM(square, F32),
            pltpu.VMEM((pairs, peers) + square, BF16),
            pltpu.VMEM((heads,) + square, BF16),
            pltpu.VMEM(per_head, F32),
            pltpu.VMEM(per_head, BF16),
            pltpu.VMEM((PIECES, tokens // PIECES, depth), BF16),
            pltpu.VMEM((4, depth, width), BF16),
            pltpu.VMEM(piece, F32),
        ]
        + [pltpu.VMEM(piece, BF16)] * 6
        + [
            pltpu.VMEM((tokens, width), BF16),
            dma((2, heads)),
            dma((heads,)),
            dma((heads,)),
            dma((4,)),
            dma((PIECES,)),
            dma((heads,)),
            dma((pairs, peers)),
            dma((pairs, peers)),
            dma((heads,)),
        ]
        + [dma((PIECES,))] * 6,
        compiler_params=pltpu.CompilerParams(
            collective_id=0, has_side_effects=True, vmem_limit_bytes=VMEM_LIMIT
        ),
    )(
        queries.reshape(blocks, SPAN, depth),
        keys.reshape(2, blocks, SPAN, depth),
        values.reshape(2, blocks, SPAN, depth),
        betas,
        gate.reshape(blocks, SPAN, depth),
        out_weight,
    )


def start_state(maps, axis):
    peers, index = lax.axis_size(axis), lax.axis_index(axis)
    heads = maps.shape[0]
    held = lax.all_gather(maps, axis, axis=0, tiled=True)
    states = pl.pallas_call(
        functools.partial(chain_kernel, peers),
        out_shape=jax.ShapeDtypeStruct((held.shape[0], HEAD_DIM, HEAD_DIM), BF16),
        compiler_params=pltpu.CompilerParams(vmem_limit_bytes=VMEM_LIMIT),
    )(held)
    return lax.dynamic_slice_in_dim(states, index * heads, heads, 0)


def out_kernel(o_ref, m_ref, s_ref, g_ref, w_ref, y_ref, mixed_ref):
    @pl.when(pl.program_id(0) == 0)
    def _():
        for h in range(s_ref.shape[0]):
            cols = slice(h * HEAD_DIM, (h + 1) * HEAD_DIM)
            seen = o_ref[:, cols] + dot(m_ref[:, cols], s_ref[h])
            scale = lax.rsqrt(jnp.mean(seen * seen, axis=1, keepdims=True) + 1e-06)
            gate = g_ref[:, cols].astype(F32)
            mixed_ref[:, cols] = (seen * scale * (gate / (1.0 + jnp.exp(-gate)))).astype(BF16)

    y_ref[...] = dot(mixed_ref[...], w_ref[...]).astype(BF16)


def project(local, reach, states, gate, out_weight):
    tokens, width = local.shape
    total = out_weight.shape[1]
    tile = 512
    whole = pl.BlockSpec((tokens, width), lambda n: (0, 0))
    return pl.pallas_call(
        out_kernel,
        grid=(total // tile,),
        in_specs=[
            whole,
            whole,
            pl.BlockSpec(states.shape, lambda n: (0, 0, 0)),
            whole,
            pl.BlockSpec((width, tile), lambda n: (0, n)),
        ],
        out_specs=pl.BlockSpec((tokens, tile), lambda n: (0, n)),
        out_shape=jax.ShapeDtypeStruct((tokens, total), BF16),
        scratch_shapes=[pltpu.VMEM((tokens, width), BF16)],
        compiler_params=pltpu.CompilerParams(
            dimension_semantics=("arbitrary",), vmem_limit_bytes=VMEM_LIMIT
        ),
    )(local, reach, states, gate, out_weight)


def per_device(queries, keys, values, betas, gate, out_weight):
    heads, _, tokens = betas.shape
    peers, index = lax.axis_size("ctx"), lax.axis_size("head")
    if index == 4 and peers >= 4 and peers % 2 == 0 and heads % 8 == 0 and tokens % (8 * SPAN) == 0:
        return fused(queries, keys, values, betas, gate, out_weight, "ctx", "head")
    beta_cols = betas.transpose(2, 1, 0).reshape(2 * tokens, heads)
    local, reach, maps = mix(queries, keys, values, beta_cols)
    states = start_state(maps, "ctx")
    partial_sum = project(local, reach, states, gate, out_weight)
    return lax.psum_scatter(partial_sum, "head", scatter_dimension=1, tiled=True)


def solution(mesh):
    return jax.shard_map(
        per_device,
        mesh=mesh,
        in_specs=(
            P("ctx", "head"),
            P(None, "ctx", "head"),
            P(None, "ctx", "head"),
            P("head", None, "ctx"),
            P("ctx", "head"),
            P("head", None),
        ),
        out_specs=P("ctx", "head"),
        check_vma=False,
    )
```

```python
import functools

import jax
import jax.numpy as jnp
from jax import lax
from jax.experimental import pallas as pl
from jax.experimental.pallas import tpu as pltpu
from jax.sharding import PartitionSpec as P

HEAD_DIM = 128
SPAN = 64
BASE = 16
F32 = jnp.float32
BF16 = jnp.bfloat16
VMEM_LIMIT = 60 * 1024 * 1024
MESH = pl.DeviceIdType.MESH
PIECES = 4


def iota(shape, dim):
    return lax.broadcasted_iota(jnp.int32, shape, dim)


def split(a):
    high = a.astype(BF16)
    return high, (a - high.astype(F32)).astype(BF16)


def dot(a, b):
    return jnp.dot(a, b, preferred_element_type=F32)


def dot3(a, b):
    ah, al = split(a)
    bh, bl = split(b)
    return dot(jnp.concatenate([ah, al, ah], axis=1), jnp.concatenate([bh, bh, bl], axis=0))


def inverse(lowers, order):
    lane = iota((BASE, order), 1)
    compact = []
    for low in lowers:
        total = jnp.zeros((BASE, order), F32)
        for blk in range(order // BASE):
            total = jnp.where(lane // BASE == blk, low[blk * BASE : (blk + 1) * BASE, :], total)
        compact.append(total)
    inv = [(iota((BASE, order), 0) == lane % BASE).astype(F32) for _ in lowers]
    for j in range(BASE - 1):
        pick = (lane // BASE) * BASE + j
        for n, low in enumerate(compact):
            column = jnp.take_along_axis(low, pick, axis=1, mode="promise_in_bounds")
            inv[n] = inv[n] - column * inv[n][j : j + 1, :]
    row = iota((order, order), 0)
    col = iota((order, order), 1)
    width = BASE
    while width < order:
        corner = (row // (2 * width) == col // (2 * width)) & (row // width != col // width)
        diagonal = row // width == col // width
        second = (iota((width, order), 1) // width) % 2 == 1
        half = [dot3(jnp.where(second, t, 0.0), jnp.where(corner, low, 0.0)) for t, low in zip(inv, lowers)]
        full = [
            jnp.where(diagonal, jnp.concatenate([t] * (order // width), axis=0), 0.0) for t in inv
        ]
        fill = [dot3(y, e) for y, e in zip(half, full)]
        inv = [
            jnp.concatenate([jnp.where(second, 0.0, t), jnp.where(second, t, 0.0) - r], axis=0)
            for t, r in zip(inv, fill)
        ]
        width *= 2
    return inv


def mix_kernel(q_ref, k_ref, v_ref, b_ref, o_ref, m_ref, x_out, x_ref):
    heads = q_ref.shape[1] // HEAD_DIM
    span = q_ref.shape[0]
    order = 2 * span
    step = pl.program_id(0)

    @pl.when(step == 0)
    def _():
        start = (iota((HEAD_DIM, 2 * HEAD_DIM), 0) == iota((HEAD_DIM, 2 * HEAD_DIM), 1)).astype(F32)
        for h in range(heads):
            x_ref[h] = start

    row = iota((order, order), 0)
    col = iota((order, order), 1)
    strict = col < row
    weave = (row == 2 * (col % span) + col // span).astype(BF16)
    causal = iota((span, order), 1) <= 2 * iota((span, order), 0) + 1
    data = []
    lowers = []
    for h in range(heads):
        cols = slice(h * HEAD_DIM, (h + 1) * HEAD_DIM)
        query = q_ref[:, cols]
        pair = jnp.concatenate(
            [
                jnp.concatenate([k_ref[0, :, cols], v_ref[0, :, cols]], axis=1),
                jnp.concatenate([k_ref[1, :, cols], v_ref[1, :, cols]], axis=1),
            ],
            axis=0,
        )
        woven = dot(weave, pair)
        key = woven[:, :HEAD_DIM]
        value = woven[:, HEAD_DIM:]
        key_b = key.astype(BF16)
        norm = lax.rsqrt(jnp.sum(key * key, axis=1, keepdims=True) + 1e-06)
        beta = b_ref[:, h : h + 1]
        both = jnp.concatenate([key_b, query], axis=0)
        gram = lax.dot_general(both, key_b, (((1,), (1,)), ((), ())), preferred_element_type=F32)
        weight = beta * norm * norm
        lowers.append(jnp.where(strict, weight * gram[:order], 0.0))
        scores = jnp.where(causal, gram[order:], 0.0).astype(BF16)
        qf = query.astype(F32)
        q_norm = lax.rsqrt(jnp.sum(qf * qf, axis=1, keepdims=True) + 1e-06)
        readers = jnp.concatenate([key.T.astype(BF16), scores], axis=0)
        data.append((both, readers, beta * norm * value, weight, q_norm))
    solved = inverse(lowers, order)
    seen = []
    for h in range(heads):
        both = data[h][0]
        high, low = split(x_ref[h])
        seen.append(
            dot(jnp.concatenate([both, both], axis=1), jnp.concatenate([high, low], axis=0))
        )
    writes = []
    for h in range(heads):
        _, _, scaled, weight, _ = data[h]
        gap = -weight * seen[h][:order]
        gap = jnp.concatenate([gap[:, :HEAD_DIM], gap[:, HEAD_DIM:] + scaled], axis=1)
        writes.append(dot3(solved[h], gap))
    for h in range(heads):
        cols = slice(h * HEAD_DIM, (h + 1) * HEAD_DIM)
        readers, q_norm = data[h][1], data[h][4]
        high, low = split(writes[h])
        change = dot(
            jnp.concatenate([readers, readers], axis=1), jnp.concatenate([high, low], axis=0)
        )
        x_ref[h] = x_ref[h] + change[:HEAD_DIM]
        out = q_norm * (seen[h][order:] + change[HEAD_DIM:])
        m_ref[:, cols] = out[:, :HEAD_DIM].astype(BF16)
        o_ref[:, cols] = out[:, HEAD_DIM:]

    @pl.when(step == pl.num_programs(0) - 1)
    def _():
        for h in range(heads):
            x_out[h] = x_ref[h].astype(BF16)


def mix(queries, keys, values, beta_cols):
    tokens, width = queries.shape
    heads = width // HEAD_DIM
    return pl.pallas_call(
        mix_kernel,
        grid=(tokens // SPAN,),
        in_specs=[
            pl.BlockSpec((SPAN, width), lambda c: (c, 0)),
            pl.BlockSpec((2, SPAN, width), lambda c: (0, c, 0)),
            pl.BlockSpec((2, SPAN, width), lambda c: (0, c, 0)),
            pl.BlockSpec((2 * SPAN, heads), lambda c: (c, 0)),
        ],
        out_specs=[
            pl.BlockSpec((SPAN, width), lambda c: (c, 0)),
            pl.BlockSpec((SPAN, width), lambda c: (c, 0)),
            pl.BlockSpec((heads, HEAD_DIM, 2 * HEAD_DIM), lambda c: (0, 0, 0)),
        ],
        out_shape=[
            jax.ShapeDtypeStruct((tokens, width), F32),
            jax.ShapeDtypeStruct((tokens, width), BF16),
            jax.ShapeDtypeStruct((heads, HEAD_DIM, 2 * HEAD_DIM), BF16),
        ],
        scratch_shapes=[pltpu.VMEM((heads, HEAD_DIM, 2 * HEAD_DIM), F32)],
        compiler_params=pltpu.CompilerParams(
            dimension_semantics=("arbitrary",), vmem_limit_bytes=VMEM_LIMIT
        ),
    )(queries, keys, values, beta_cols)


def chain_kernel(peers, x_ref, s_ref):
    heads = x_ref.shape[0] // peers
    for h in range(heads):
        state = jnp.zeros((HEAD_DIM, HEAD_DIM), F32)
        for k in range(peers):
            s_ref[k * heads + h] = state.astype(BF16)
            if k < peers - 1:
                maps = x_ref[k * heads + h]
                turn = maps[:, :HEAD_DIM]
                high, low = split(state)
                state = maps[:, HEAD_DIM:].astype(F32) + dot(
                    jnp.concatenate([turn, turn], axis=1), jnp.concatenate([high, low], axis=0)
                )


def dot_t(a, b):
    return lax.dot_general(a, b, (((1,), (1,)), ((), ())), preferred_element_type=F32)


def pair_dot(a, low, high_b, low_b):
    rows = a.shape[0]
    both = dot(jnp.concatenate([a, low], axis=0), jnp.concatenate([high_b, low_b], axis=1))
    width = high_b.shape[1]
    return both[:rows, :width] + both[rows:, :width] + both[:rows, width:]


def weave(*streams):
    order = []
    for n, (count, _, first, last) in enumerate(streams):
        order += [(first + (last - first) * (k + 0.5) / count, n) for k in range(count)]
    for _, n in sorted(order):
        next(streams[n][1], None)
    for _, stream, _, _ in streams:
        for _ in stream:
            pass


def base_solve(lowers, span):
    order = 2 * span
    base = BASE // 2
    lane = iota((base, order), 1)
    group = (lane % span) // base
    row16, lane16 = iota((BASE, order), 0), iota((BASE, order), 1)
    group16 = (lane16 % span) // base
    row_tok, lane_tok = row16 % base, lane16 % base
    before = (lane_tok < row_tok) | ((lane_tok == row_tok) & (lane16 // span < row16 // base))
    compact = []
    for n, low in enumerate(lowers):
        halves = []
        for j in range(2):
            total = jnp.zeros((base, order), F32)
            for blk in range(span // base):
                start = j * span + blk * base
                total = jnp.where(group == blk, low[start : start + base, :], total)
            halves.append(total)
        compact.append(jnp.where(before, jnp.concatenate(halves, axis=0), 0.0))
        if n % 2:
            yield
    own = (row16 % base == lane16 % base) & (row16 // base == lane16 // span)
    inv = [own.astype(F32) for _ in lowers]
    for s in range(BASE - 1):
        t, j = s // 2, s % 2
        pick = j * span + group16 * base + t
        for n, low in enumerate(compact):
            column = jnp.take_along_axis(low, pick, axis=1, mode="promise_in_bounds")
            inv[n] = inv[n] - column * inv[n][j * base + t : j * base + t + 1, :]
        yield
    return inv


def merge(inv, pieces, span):
    order = 2 * span
    tok_r = iota((order, order), 0) % span
    tok_c = iota((order, order), 1) % span
    width = BASE // 2
    zero = jnp.zeros((), BF16)
    while width < span:
        last = 2 * width == span
        diagonal = tok_r // width == tok_c // width
        corner = (tok_r // (2 * width) == tok_c // (2 * width)) & (tok_r // width != tok_c // width)
        second = ((iota((2 * width, order), 1) % span) // width) % 2 == 1
        odd, half, fill, wide, merged = [], [], [], [], []
        for n, t in enumerate(inv):
            odd.append(jnp.where(second, t, 0.0))
            th, tl = split(odd[n])
            high, low = pieces(n)
            if last:
                y = jnp.where(second, 0.0, pair_dot(th, tl, high, low))
            else:
                y = pair_dot(th, tl, jnp.where(corner, high, zero), jnp.where(corner, low, zero))
            half.append(y)
            parts = []
            for j in range(2):
                part = t[j * width : (j + 1) * width]
                if width < 16:
                    part = jnp.concatenate([part] * (16 // width), axis=0)
                parts.append((split(part), span // part.shape[0]))
            full = [
                jnp.concatenate([p[k] for p, count in parts for _ in range(count)], axis=0)
                for k in range(2)
            ]
            if not last:
                full = [jnp.where(diagonal, f, zero) for f in full]
            wide.append(full)
            yield
        for y, full in zip(half, wide):
            yh, yl = split(y)
            r = pair_dot(yh, yl, full[0], full[1])
            fill.append(jnp.where(second, 0.0, r) if last else r)
            yield
        for t, o, r in zip(inv, odd, fill):
            even, lower = t - o, o - r
            merged.append(
                jnp.concatenate(
                    [even[:width], lower[:width], even[width:], lower[width:]], axis=0
                )
            )
        inv = merged
        width *= 2
    return inv


def fused_kernel(
    seq_axis, peers, axis, q_hbm, k_hbm, v_hbm, b_ref, g_hbm, w_hbm, y_hbm,
    q_ref, k_ref, v_ref, g_ref, beta_ref, stack_ref, turn_ref, source_ref, x_ref, start_ref,
    low_ref, inv_ref, weight_ref, eye_ref,
    maps, held, carry_ref, states, s_ref, o_ref, m_ref,
    mixed, weight, total, far_out, far_in, near_out, near_in, cross_out, cross_in, y_ref,
    kv_sem, q_sem, g_sem, load_sem, y_sem, map_send, map_recv, back_send, back_recv,
    far_send, far_recv, near_send, near_recv, cross_send, cross_recv,
):
    heads, blocks, span = q_ref.shape[0], q_ref.shape[1], q_ref.shape[2]
    pairs = heads // 2
    parts = 2
    batch = blocks // parts
    seq = lax.axis_index(seq_axis)
    me = lax.axis_index(axis)
    chip, core = me // 2, me % 2
    sibling = 2 * chip + 1 - core
    across = 2 * (1 - chip) + core
    beyond = 2 * (1 - chip) + 1 - core
    width = y_ref.shape[2]

    barrier = pltpu.get_barrier_semaphore()
    for other in (sibling, across):
        pl.semaphore_signal(barrier, inc=1, device_id={axis: other}, device_id_type=MESH)
    for away in range(1, peers):
        pl.semaphore_signal(
            barrier,
            inc=1,
            device_id={seq_axis: lax.rem(seq + away, peers)},
            device_id_type=MESH,
        )

    def columns(h):
        return pl.ds(pl.multiple_of(h * HEAD_DIM, HEAD_DIM), HEAD_DIM)

    def fetch_kv(h):
        return (
            pltpu.make_async_copy(k_hbm.at[:, :, :, columns(h)], k_ref.at[h], kv_sem.at[0, h]),
            pltpu.make_async_copy(v_hbm.at[:, :, :, columns(h)], v_ref.at[h], kv_sem.at[1, h]),
        )

    def fetch_q(h):
        return pltpu.make_async_copy(q_hbm.at[:, :, columns(h)], q_ref.at[h], q_sem.at[h])

    def fetch_g(h):
        return pltpu.make_async_copy(g_hbm.at[:, :, columns(h)], g_ref.at[h], g_sem.at[h])

    def load(n):
        owner = (beyond, across, sibling, me)[n]
        return pltpu.make_async_copy(
            w_hbm.at[:, pl.ds(pl.multiple_of(owner * width, width), width)],
            weight.at[n],
            load_sem.at[n],
        )

    for h in range(heads):
        for copy in fetch_kv(h):
            copy.start()
    for h in range(heads):
        fetch_q(h).start()
    for blk in range(blocks):
        window = slice(blk * span, (blk + 1) * span)
        beta_ref[blk] = jnp.concatenate([b_ref[:, 0, window], b_ref[:, 1, window]], axis=1)
    begin = (iota((HEAD_DIM, 2 * HEAD_DIM), 0) == iota((HEAD_DIM, 2 * HEAD_DIM), 1)).astype(F32)
    for h in range(heads):
        x_ref[h] = begin
    eye_ref[...] = (iota(eye_ref.shape, 0) == iota(eye_ref.shape, 1)).astype(F32)

    def place(it, n):
        pair, part = it // parts, it % parts
        return 2 * pair + n % 2, part * batch + n // 2

    count = 2 * batch

    def key_of(h, blk):
        return jnp.concatenate([k_ref[h, 0, blk], k_ref[h, 1, blk]], axis=0)

    def stack_of(h, blk):
        none = jnp.zeros((HEAD_DIM, HEAD_DIM), BF16)
        return jnp.concatenate(
            [
                jnp.concatenate([stack_ref[h, blk, 0], stack_ref[h, blk, 2]], axis=1),
                jnp.concatenate([stack_ref[h, blk, 1], none], axis=1),
            ],
            axis=0,
        )

    def solve(it):
        slot = it % 2
        grams, squares = [], []
        for n in range(count):
            key = key_of(*place(it, n))
            grams.append(dot_t(key, key))
            if n % 2:
                yield
        for n, g in enumerate(grams):
            squares.append(jnp.sum(eye_ref[...] * g, axis=0, keepdims=True))
            if n % 4 == 3:
                yield
        beta = jnp.concatenate(
            [beta_ref[place(it, n)[1], pl.ds(place(it, n)[0], 1), :] for n in range(count)], axis=0
        )
        norm = lax.rsqrt(jnp.concatenate(squares, axis=0) + 1e-06)
        value_weight = beta * norm
        weight_rows = value_weight * norm
        weight_ref[slot, 0] = weight_rows
        weight_ref[slot, 1] = value_weight
        weight_cols = weight_rows.T
        yield
        lowers = []
        for n, g in enumerate(grams):
            low = weight_cols[:, n : n + 1] * g
            lowers.append(low)
            low_ref[slot, n, 0], low_ref[slot, n, 1] = split(low)
            if n % 2:
                yield
        inv = yield from base_solve(lowers, span)
        for n in range(count):
            inv_ref[slot, n] = inv[n]

    def transit(it):
        slot = it % 2

        def pieces(n):
            return low_ref[slot, n, 0], low_ref[slot, n, 1]

        solved = yield from merge([inv_ref[slot, n] for n in range(count)], pieces, span)
        turns, writes, changes = [], [], []
        for n in range(count):
            h, blk = place(it, n)
            th, tl = split(solved[n] * weight_ref[slot, 0, n : n + 1, :])
            tv = (solved[n] * weight_ref[slot, 1, n : n + 1, :]).astype(BF16)
            key = key_of(h, blk)
            value = jnp.concatenate([v_ref[h, 0, blk], v_ref[h, 1, blk]], axis=0)
            turns.append(
                dot(jnp.concatenate([th, tl], axis=1), jnp.concatenate([key, key], axis=0))
            )
            writes.append(dot(tv, value))
            yield
        for n in range(count):
            h, blk = place(it, n)
            turn_h, turn_l = split(turns[n])
            stack_ref[h, blk, 0], stack_ref[h, blk, 1] = turn_h, turn_l
            stack_ref[h, blk, 2] = writes[n].astype(BF16)
            stack = stack_of(h, blk)
            key_t = key_of(h, blk).T
            changes.append(dot(jnp.concatenate([key_t, key_t], axis=1), stack))
            yield
        for n in range(count):
            step = eye_ref[...] - changes[n][:, :HEAD_DIM]
            turn_ref[slot, n, 0], turn_ref[slot, n, 1] = split(step)
            source_ref[slot, n] = changes[n][:, HEAD_DIM:]
            yield

    def compose(it):
        slot = it % 2
        pair, part = it // parts, it % parts
        states_now = [x_ref[2 * pair + i] for i in range(2)]
        for n in range(count):
            h, blk = place(it, n)
            i = n % 2
            high, low = split(states_now[i])
            start_ref[h, blk, 0] = high[:, :HEAD_DIM]
            start_ref[h, blk, 1] = high[:, HEAD_DIM:]
            turn_h, turn_l = turn_ref[slot, n, 0], turn_ref[slot, n, 1]
            moved = dot(
                jnp.concatenate([turn_h, turn_l, turn_h], axis=1),
                jnp.concatenate([high, high, low], axis=0),
            )
            states_now[i] = jnp.concatenate(
                [moved[:, :HEAD_DIM], moved[:, HEAD_DIM:] + source_ref[slot, n]], axis=1
            )
            if n >= count - 2:
                x_ref[h] = states_now[i]
            yield

    def a_stream(it, first=0.0, last=1.0):
        return 7 * count // 4 + BASE, solve(it), first, last

    def b_stream(it, first=0.0, last=1.0):
        return 9 * count, transit(it), first, last

    def c_stream(it, first=0.0, last=1.0):
        return count, compose(it), first, last

    def owner_of(pair, i):
        side = lax.rem(pair + core, 2)
        return peers // 2 - 2 + side + i * (3 - 2 * side)

    def send_map(pair, i, source):
        h = 2 * pair + i
        return pltpu.make_async_remote_copy(
            src_ref=maps.at[h],
            dst_ref=held.at[pair, source],
            send_sem=map_send.at[h],
            recv_sem=map_recv.at[pair, source],
            device_id={seq_axis: owner_of(pair, i)},
            device_id_type=MESH,
        )

    def send_state(pair, i, target):
        h = 2 * pair + i
        return pltpu.make_async_remote_copy(
            src_ref=states.at[pair, target],
            dst_ref=s_ref.at[h],
            send_sem=back_send.at[pair, target],
            recv_sem=back_recv.at[h],
            device_id={seq_axis: target},
            device_id_type=MESH,
        )

    def post(pair):
        for i in range(2):
            h = 2 * pair + i
            maps[h, 0] = x_ref[h, :, :HEAD_DIM].astype(BF16)
            maps[h, 1] = x_ref[h, :, HEAD_DIM:].astype(BF16)

            @pl.when((seq != owner_of(pair, i)) & (seq != peers - 1))
            def _():
                send_map(pair, i, seq).start()

            @pl.when(seq == owner_of(pair, i))
            def _():
                held[pair, seq] = maps[h]

    def chain(pair):
        for i in range(2):

            @pl.when(seq == owner_of(pair, i))
            def _():
                carry_ref[...] = jnp.zeros((HEAD_DIM, HEAD_DIM), F32)
                for k in range(peers - 1):

                    @pl.when(seq != k)
                    def _():
                        send_map(pair, i, k).wait_recv()

                    high, low = split(carry_ref[...])
                    turn = held[pair, k, 0]
                    state = held[pair, k, 1].astype(F32) + dot(
                        jnp.concatenate([turn, turn], axis=1),
                        jnp.concatenate([high, low], axis=0),
                    )
                    carry_ref[...] = state
                    states[pair, k + 1] = state.astype(BF16)

                    @pl.when(seq != k + 1)
                    def _():
                        send_state(pair, i, k + 1).start()

                    @pl.when(seq == k + 1)
                    def _():
                        s_ref[2 * pair + i] = states[pair, k + 1]

    @pl.when(seq == 0)
    def _():
        s_ref[...] = jnp.zeros(s_ref.shape, BF16)

    def wait_kv(pair):
        for i in range(2):
            for copy in fetch_kv(2 * pair + i):
                copy.wait()

    steps = parts * pairs
    wait_kv(0)
    weave(a_stream(0))
    for n in range(4):
        load(n).start()
    for h in range(heads):
        fetch_g(h).start()
    weave(a_stream(1), b_stream(0))

    def step(it, _):
        @pl.when(it % parts == 0)
        def _():
            wait_kv(it // parts)

        weave(a_stream(it), b_stream(it - 1), c_stream(it - 2))

        @pl.when(it == parts + 1)
        def _():
            pl.semaphore_wait(barrier, peers + 1)

        @pl.when(it % parts == 1)
        def _():
            post(it // parts - 1)

        @pl.when(it == steps - 2)
        def _():
            chain(0)

        return 0

    lax.fori_loop(2, steps, step, 0)
    weave(
        b_stream(steps - 1, 0.0, 9.0),
        c_stream(steps - 2, 0.0, 6.0),
        c_stream(steps - 1, 8.1, 9.1),
    )
    post(pairs - 1)
    for h in range(heads):
        fetch_q(h).wait()

    def read(pair, _):
        causal = iota((span, 2 * span), 1) % span <= iota((span, 2 * span), 0)
        for i in range(2):
            h = 2 * pair + i
            scores = []
            for blk in range(blocks):
                found = jnp.where(causal, dot_t(q_ref[h, blk], key_of(h, blk)), 0.0).astype(BF16)
                scores.append(jnp.concatenate([found, found], axis=1))
            drawn = [dot(score, stack_of(h, blk)) for blk, score in enumerate(scores)]
            for blk in range(blocks):
                kept = (q_ref[h, blk].astype(F32) - drawn[blk][:, :HEAD_DIM]).astype(BF16)
                out = dot(kept, jnp.concatenate([start_ref[h, blk, 0], start_ref[h, blk, 1]], axis=1))
                m_ref[h, blk] = out[:, :HEAD_DIM].astype(BF16)
                o_ref[h, blk] = out[:, HEAD_DIM:] + drawn[blk][:, HEAD_DIM:]

        @pl.when(pair % 2 == 0)
        def _():
            chain(1 + pair // 2)

        return 0

    lax.fori_loop(0, pairs, read, 0)
    for h in range(heads):
        fetch_g(h).wait()

    def wait_state(pair):
        for i in range(2):

            @pl.when((seq != owner_of(pair, i)) & (seq != 0))
            def _():
                send_state(pair, i, seq).wait_recv()

    def blend(pair, t):
        for i in range(2):
            h = 2 * pair + i
            query = q_ref[h, t].astype(F32)
            unit = lax.rsqrt(jnp.sum(query * query, axis=1, keepdims=True) + 1e-06)
            seen = unit * (o_ref[h, t] + dot(m_ref[h, t], s_ref[h]))
            scale = lax.rsqrt(jnp.mean(seen * seen, axis=1, keepdims=True) + 1e-06)
            gate = g_ref[h, t].astype(F32)
            mixed[t, h] = (seen * scale * (gate / (1.0 + jnp.exp(-gate)))).astype(BF16)

    def blend_pair(pair, _):
        wait_state(pair)
        for t in range(blocks):
            blend(pair, t)
        return 0

    lax.fori_loop(0, pairs - 2, blend_pair, 0)
    chain(pairs - 1)
    blend_pair(pairs - 2, 0)

    def send(source, target, send_sem, recv_sem, t, device):
        return pltpu.make_async_remote_copy(
            src_ref=source.at[t],
            dst_ref=target.at[t],
            send_sem=send_sem.at[t],
            recv_sem=recv_sem.at[t],
            device_id={axis: device},
            device_id_type=MESH,
        )

    def far(t):
        return send(far_out, far_in, far_send, far_recv, t, sibling)

    def near(t):
        return send(near_out, near_in, near_send, near_recv, t, sibling)

    def cross(t):
        return send(cross_out, cross_in, cross_send, cross_recv, t, across)

    def pass_on(t):
        far(t).wait()
        cross_out[t] = (total[t] + far_in[t].astype(F32)).astype(BF16)
        cross(t).start()

    def rows_of(t, first, last):
        return jnp.concatenate([mixed[t, h] for h in range(first, last)], axis=1)

    def product(t, n):
        return dot(rows_of(t, 0, heads), weight[n])

    early = (heads - 2) * HEAD_DIM
    load(0).wait()
    total[0] = dot(rows_of(0, 0, heads - 2), weight[0, :early, :])
    wait_state(pairs - 1)
    blend(pairs - 1, 0)
    far_out[0] = (total[0] + dot(rows_of(0, heads - 2, heads), weight[0, early:, :])).astype(BF16)
    far(0).start()
    load(1).wait()
    total[0] = product(0, 1)

    def first_half(t, _):
        blend(pairs - 1, t)
        far_out[t] = product(t, 0).astype(BF16)
        far(t).start()
        pass_on(t - 1)
        total[t] = product(t, 1)
        return 0

    lax.fori_loop(1, blocks, first_half, 0)
    load(2).wait()
    near_out[0] = product(0, 2).astype(BF16)
    near(0).start()
    pass_on(blocks - 1)

    def second_half(t, _):
        near_out[t] = product(t, 2).astype(BF16)
        near(t).start()
        return 0

    lax.fori_loop(1, blocks, second_half, 0)
    load(3).wait()

    def own_part(t, _):
        total[t] = product(t, 3)
        return 0

    lax.fori_loop(0, blocks, own_part, 0)

    def put(t):
        window = pl.ds(pl.multiple_of(t * span, span), span)
        return pltpu.make_async_copy(y_ref.at[t], y_hbm.at[window], y_sem.at[t])

    def close(t, _):
        near(t).wait()
        cross(t).wait()
        y_ref[t] = (total[t] + near_in[t].astype(F32) + cross_in[t].astype(F32)).astype(BF16)
        put(t).start()
        return 0

    lax.fori_loop(0, blocks, close, 0)
    for pair in range(pairs):
        for i in range(2):

            @pl.when((seq != owner_of(pair, i)) & (seq != peers - 1))
            def _():
                send_map(pair, i, seq).wait_send()

            @pl.when(seq == owner_of(pair, i))
            def _():
                for k in range(1, peers):

                    @pl.when(seq != k)
                    def _():
                        send_state(pair, i, k).wait_send()

    for t in range(blocks):
        put(t).wait()


def fused(queries, keys, values, betas, gate, out_weight, seq_axis, axis):
    tokens, depth = queries.shape
    heads = depth // HEAD_DIM
    peers = lax.axis_size(seq_axis)
    width = out_weight.shape[1] // lax.axis_size(axis)
    blocks = tokens // SPAN
    batch = blocks // 2
    vmem = pl.BlockSpec(memory_space=pltpu.VMEM)
    hbm = pl.BlockSpec(memory_space=pl.ANY)
    piece = (blocks, SPAN, width)
    square = (HEAD_DIM, HEAD_DIM)
    wide = (HEAD_DIM, 2 * HEAD_DIM)
    two = (2,) + square
    pairs = heads // 2
    dma = pltpu.SemaphoreType.DMA
    per_head = (heads, blocks, SPAN, HEAD_DIM)
    both = (heads, 2, blocks, SPAN, HEAD_DIM)
    return pl.pallas_call(
        functools.partial(fused_kernel, seq_axis, peers, axis),
        in_specs=[hbm, hbm, hbm, vmem, hbm, hbm],
        out_specs=hbm,
        out_shape=jax.ShapeDtypeStruct((tokens, width), BF16),
        scratch_shapes=[
            pltpu.VMEM(per_head, BF16),
            pltpu.VMEM(both, BF16),
            pltpu.VMEM(both, BF16),
            pltpu.VMEM(per_head, BF16),
            pltpu.VMEM((blocks, heads, 2 * SPAN), F32),
            pltpu.VMEM((heads, blocks, 3) + square, BF16),
            pltpu.VMEM((2, 2 * batch) + two, BF16),
            pltpu.VMEM((2, 2 * batch) + square, F32),
            pltpu.VMEM((heads,) + wide, F32),
            pltpu.VMEM((heads, blocks) + two, BF16),
            pltpu.VMEM((2, 2 * batch) + two, BF16),
            pltpu.VMEM((2, 2 * batch, BASE, 2 * SPAN), F32),
            pltpu.VMEM((2, 2, 2 * batch, 2 * SPAN), F32),
            pltpu.VMEM(square, F32),
            pltpu.VMEM((heads,) + two, BF16),
            pltpu.VMEM((pairs, peers) + two, BF16),
            pltpu.VMEM(square, F32),
            pltpu.VMEM((pairs, peers) + square, BF16),
            pltpu.VMEM((heads,) + square, BF16),
            pltpu.VMEM(per_head, F32),
            pltpu.VMEM(per_head, BF16),
            pltpu.VMEM((blocks, heads, SPAN, HEAD_DIM), BF16),
            pltpu.VMEM((4, depth, width), BF16),
            pltpu.VMEM(piece, F32),
        ]
        + [pltpu.VMEM(piece, BF16)] * 6
        + [
            pltpu.VMEM(piece, BF16),
            dma((2, heads)),
            dma((heads,)),
            dma((heads,)),
            dma((4,)),
            dma((blocks,)),
            dma((heads,)),
            dma((pairs, peers)),
            dma((pairs, peers)),
            dma((heads,)),
        ]
        + [dma((blocks,))] * 6,
        compiler_params=pltpu.CompilerParams(
            collective_id=0, has_side_effects=True, vmem_limit_bytes=VMEM_LIMIT
        ),
    )(
        queries.reshape(blocks, SPAN, depth),
        keys.reshape(2, blocks, SPAN, depth),
        values.reshape(2, blocks, SPAN, depth),
        betas,
        gate.reshape(blocks, SPAN, depth),
        out_weight,
    )


def start_state(maps, axis):
    peers, index = lax.axis_size(axis), lax.axis_index(axis)
    heads = maps.shape[0]
    held = lax.all_gather(maps, axis, axis=0, tiled=True)
    states = pl.pallas_call(
        functools.partial(chain_kernel, peers),
        out_shape=jax.ShapeDtypeStruct((held.shape[0], HEAD_DIM, HEAD_DIM), BF16),
        compiler_params=pltpu.CompilerParams(vmem_limit_bytes=VMEM_LIMIT),
    )(held)
    return lax.dynamic_slice_in_dim(states, index * heads, heads, 0)


def out_kernel(o_ref, m_ref, s_ref, g_ref, w_ref, y_ref, mixed_ref):
    @pl.when(pl.program_id(0) == 0)
    def _():
        for h in range(s_ref.shape[0]):
            cols = slice(h * HEAD_DIM, (h + 1) * HEAD_DIM)
            seen = o_ref[:, cols] + dot(m_ref[:, cols], s_ref[h])
            scale = lax.rsqrt(jnp.mean(seen * seen, axis=1, keepdims=True) + 1e-06)
            gate = g_ref[:, cols].astype(F32)
            mixed_ref[:, cols] = (seen * scale * (gate / (1.0 + jnp.exp(-gate)))).astype(BF16)

    y_ref[...] = dot(mixed_ref[...], w_ref[...]).astype(BF16)


def project(local, reach, states, gate, out_weight):
    tokens, width = local.shape
    total = out_weight.shape[1]
    tile = 512
    whole = pl.BlockSpec((tokens, width), lambda n: (0, 0))
    return pl.pallas_call(
        out_kernel,
        grid=(total // tile,),
        in_specs=[
            whole,
            whole,
            pl.BlockSpec(states.shape, lambda n: (0, 0, 0)),
            whole,
            pl.BlockSpec((width, tile), lambda n: (0, n)),
        ],
        out_specs=pl.BlockSpec((tokens, tile), lambda n: (0, n)),
        out_shape=jax.ShapeDtypeStruct((tokens, total), BF16),
        scratch_shapes=[pltpu.VMEM((tokens, width), BF16)],
        compiler_params=pltpu.CompilerParams(
            dimension_semantics=("arbitrary",), vmem_limit_bytes=VMEM_LIMIT
        ),
    )(local, reach, states, gate, out_weight)


def per_device(queries, keys, values, betas, gate, out_weight):
    heads, _, tokens = betas.shape
    peers, index = lax.axis_size("ctx"), lax.axis_size("head")
    if index == 4 and peers >= 4 and peers % 2 == 0 and heads % 8 == 0 and tokens % (8 * SPAN) == 0:
        return fused(queries, keys, values, betas, gate, out_weight, "ctx", "head")
    beta_cols = betas.transpose(2, 1, 0).reshape(2 * tokens, heads)
    local, reach, maps = mix(queries, keys, values, beta_cols)
    states = start_state(maps, "ctx")
    partial_sum = project(local, reach, states, gate, out_weight)
    return lax.psum_scatter(partial_sum, "head", scatter_dimension=1, tiled=True)


def solution(mesh):
    return jax.shard_map(
        per_device,
        mesh=mesh,
        in_specs=(
            P("ctx", "head"),
            P(None, "ctx", "head"),
            P(None, "ctx", "head"),
            P("head", None, "ctx"),
            P("ctx", "head"),
            P("head", None),
        ),
        out_specs=P("ctx", "head"),
        check_vma=False,
    )
```

```python
import functools

import jax
import jax.numpy as jnp
from jax import lax
from jax.experimental import pallas as pl
from jax.experimental.pallas import tpu as pltpu
from jax.sharding import PartitionSpec as P

HEAD_DIM = 128
SPAN = 64
BASE = 16
F32 = jnp.float32
BF16 = jnp.bfloat16
VMEM_LIMIT = 60 * 1024 * 1024
MESH = pl.DeviceIdType.MESH
PIECES = 4


def iota(shape, dim):
    return lax.broadcasted_iota(jnp.int32, shape, dim)


def split(a):
    high = a.astype(BF16)
    return high, (a - high.astype(F32)).astype(BF16)


def dot(a, b):
    return jnp.dot(a, b, preferred_element_type=F32)


def dot3(a, b):
    ah, al = split(a)
    bh, bl = split(b)
    return dot(jnp.concatenate([ah, al, ah], axis=1), jnp.concatenate([bh, bh, bl], axis=0))


def inverse(lowers, order):
    lane = iota((BASE, order), 1)
    compact = []
    for low in lowers:
        total = jnp.zeros((BASE, order), F32)
        for blk in range(order // BASE):
            total = jnp.where(lane // BASE == blk, low[blk * BASE : (blk + 1) * BASE, :], total)
        compact.append(total)
    inv = [(iota((BASE, order), 0) == lane % BASE).astype(F32) for _ in lowers]
    for j in range(BASE - 1):
        pick = (lane // BASE) * BASE + j
        for n, low in enumerate(compact):
            column = jnp.take_along_axis(low, pick, axis=1, mode="promise_in_bounds")
            inv[n] = inv[n] - column * inv[n][j : j + 1, :]
    row = iota((order, order), 0)
    col = iota((order, order), 1)
    width = BASE
    while width < order:
        corner = (row // (2 * width) == col // (2 * width)) & (row // width != col // width)
        diagonal = row // width == col // width
        second = (iota((width, order), 1) // width) % 2 == 1
        half = [dot3(jnp.where(second, t, 0.0), jnp.where(corner, low, 0.0)) for t, low in zip(inv, lowers)]
        full = [
            jnp.where(diagonal, jnp.concatenate([t] * (order // width), axis=0), 0.0) for t in inv
        ]
        fill = [dot3(y, e) for y, e in zip(half, full)]
        inv = [
            jnp.concatenate([jnp.where(second, 0.0, t), jnp.where(second, t, 0.0) - r], axis=0)
            for t, r in zip(inv, fill)
        ]
        width *= 2
    return inv


def mix_kernel(q_ref, k_ref, v_ref, b_ref, o_ref, m_ref, x_out, x_ref):
    heads = q_ref.shape[1] // HEAD_DIM
    span = q_ref.shape[0]
    order = 2 * span
    step = pl.program_id(0)

    @pl.when(step == 0)
    def _():
        start = (iota((HEAD_DIM, 2 * HEAD_DIM), 0) == iota((HEAD_DIM, 2 * HEAD_DIM), 1)).astype(F32)
        for h in range(heads):
            x_ref[h] = start

    row = iota((order, order), 0)
    col = iota((order, order), 1)
    strict = col < row
    weave = (row == 2 * (col % span) + col // span).astype(BF16)
    causal = iota((span, order), 1) <= 2 * iota((span, order), 0) + 1
    data = []
    lowers = []
    for h in range(heads):
        cols = slice(h * HEAD_DIM, (h + 1) * HEAD_DIM)
        query = q_ref[:, cols]
        pair = jnp.concatenate(
            [
                jnp.concatenate([k_ref[0, :, cols], v_ref[0, :, cols]], axis=1),
                jnp.concatenate([k_ref[1, :, cols], v_ref[1, :, cols]], axis=1),
            ],
            axis=0,
        )
        woven = dot(weave, pair)
        key = woven[:, :HEAD_DIM]
        value = woven[:, HEAD_DIM:]
        key_b = key.astype(BF16)
        norm = lax.rsqrt(jnp.sum(key * key, axis=1, keepdims=True) + 1e-06)
        beta = b_ref[:, h : h + 1]
        both = jnp.concatenate([key_b, query], axis=0)
        gram = lax.dot_general(both, key_b, (((1,), (1,)), ((), ())), preferred_element_type=F32)
        weight = beta * norm * norm
        lowers.append(jnp.where(strict, weight * gram[:order], 0.0))
        scores = jnp.where(causal, gram[order:], 0.0).astype(BF16)
        qf = query.astype(F32)
        q_norm = lax.rsqrt(jnp.sum(qf * qf, axis=1, keepdims=True) + 1e-06)
        readers = jnp.concatenate([key.T.astype(BF16), scores], axis=0)
        data.append((both, readers, beta * norm * value, weight, q_norm))
    solved = inverse(lowers, order)
    seen = []
    for h in range(heads):
        both = data[h][0]
        high, low = split(x_ref[h])
        seen.append(
            dot(jnp.concatenate([both, both], axis=1), jnp.concatenate([high, low], axis=0))
        )
    writes = []
    for h in range(heads):
        _, _, scaled, weight, _ = data[h]
        gap = -weight * seen[h][:order]
        gap = jnp.concatenate([gap[:, :HEAD_DIM], gap[:, HEAD_DIM:] + scaled], axis=1)
        writes.append(dot3(solved[h], gap))
    for h in range(heads):
        cols = slice(h * HEAD_DIM, (h + 1) * HEAD_DIM)
        readers, q_norm = data[h][1], data[h][4]
        high, low = split(writes[h])
        change = dot(
            jnp.concatenate([readers, readers], axis=1), jnp.concatenate([high, low], axis=0)
        )
        x_ref[h] = x_ref[h] + change[:HEAD_DIM]
        out = q_norm * (seen[h][order:] + change[HEAD_DIM:])
        m_ref[:, cols] = out[:, :HEAD_DIM].astype(BF16)
        o_ref[:, cols] = out[:, HEAD_DIM:]

    @pl.when(step == pl.num_programs(0) - 1)
    def _():
        for h in range(heads):
            x_out[h] = x_ref[h].astype(BF16)


def mix(queries, keys, values, beta_cols):
    tokens, width = queries.shape
    heads = width // HEAD_DIM
    return pl.pallas_call(
        mix_kernel,
        grid=(tokens // SPAN,),
        in_specs=[
            pl.BlockSpec((SPAN, width), lambda c: (c, 0)),
            pl.BlockSpec((2, SPAN, width), lambda c: (0, c, 0)),
            pl.BlockSpec((2, SPAN, width), lambda c: (0, c, 0)),
            pl.BlockSpec((2 * SPAN, heads), lambda c: (c, 0)),
        ],
        out_specs=[
            pl.BlockSpec((SPAN, width), lambda c: (c, 0)),
            pl.BlockSpec((SPAN, width), lambda c: (c, 0)),
            pl.BlockSpec((heads, HEAD_DIM, 2 * HEAD_DIM), lambda c: (0, 0, 0)),
        ],
        out_shape=[
            jax.ShapeDtypeStruct((tokens, width), F32),
            jax.ShapeDtypeStruct((tokens, width), BF16),
            jax.ShapeDtypeStruct((heads, HEAD_DIM, 2 * HEAD_DIM), BF16),
        ],
        scratch_shapes=[pltpu.VMEM((heads, HEAD_DIM, 2 * HEAD_DIM), F32)],
        compiler_params=pltpu.CompilerParams(
            dimension_semantics=("arbitrary",), vmem_limit_bytes=VMEM_LIMIT
        ),
    )(queries, keys, values, beta_cols)


def chain_kernel(peers, x_ref, s_ref):
    heads = x_ref.shape[0] // peers
    for h in range(heads):
        state = jnp.zeros((HEAD_DIM, HEAD_DIM), F32)
        for k in range(peers):
            s_ref[k * heads + h] = state.astype(BF16)
            if k < peers - 1:
                maps = x_ref[k * heads + h]
                turn = maps[:, :HEAD_DIM]
                high, low = split(state)
                state = maps[:, HEAD_DIM:].astype(F32) + dot(
                    jnp.concatenate([turn, turn], axis=1), jnp.concatenate([high, low], axis=0)
                )


def dot_t(a, b):
    return lax.dot_general(a, b, (((1,), (1,)), ((), ())), preferred_element_type=F32)


def pair_dot(a, low, high_b, low_b):
    rows = a.shape[0]
    both = dot(jnp.concatenate([a, low], axis=0), jnp.concatenate([high_b, low_b], axis=1))
    width = high_b.shape[1]
    return both[:rows, :width] + both[rows:, :width] + both[:rows, width:]


def weave(*streams):
    order = []
    for n, (count, _, first, last) in enumerate(streams):
        order += [(first + (last - first) * (k + 0.5) / count, n) for k in range(count)]
    for _, n in sorted(order):
        next(streams[n][1], None)
    for _, stream, _, _ in streams:
        for _ in stream:
            pass


def base_solve(lowers, span):
    order = 2 * span
    base = BASE // 2
    lane = iota((base, order), 1)
    group = (lane % span) // base
    row16, lane16 = iota((BASE, order), 0), iota((BASE, order), 1)
    group16 = (lane16 % span) // base
    row_tok, lane_tok = row16 % base, lane16 % base
    before = (lane_tok < row_tok) | ((lane_tok == row_tok) & (lane16 // span < row16 // base))
    compact = []
    for n, low in enumerate(lowers):
        halves = []
        for j in range(2):
            total = jnp.zeros((base, order), F32)
            for blk in range(span // base):
                start = j * span + blk * base
                total = jnp.where(group == blk, low[start : start + base, :], total)
            halves.append(total)
        compact.append(jnp.where(before, jnp.concatenate(halves, axis=0), 0.0))
        if n % 2:
            yield
    own = (row16 % base == lane16 % base) & (row16 // base == lane16 // span)
    inv = [own.astype(F32) for _ in lowers]
    for s in range(BASE - 1):
        t, j = s // 2, s % 2
        pick = j * span + group16 * base + t
        for n, low in enumerate(compact):
            column = jnp.take_along_axis(low, pick, axis=1, mode="promise_in_bounds")
            inv[n] = inv[n] - column * inv[n][j * base + t : j * base + t + 1, :]
        yield
    return inv


def merge(inv, pieces, span):
    order = 2 * span
    tok_r = iota((order, order), 0) % span
    tok_c = iota((order, order), 1) % span
    width = BASE // 2
    zero = jnp.zeros((), BF16)
    while width < span:
        last = 2 * width == span
        diagonal = tok_r // width == tok_c // width
        corner = (tok_r // (2 * width) == tok_c // (2 * width)) & (tok_r // width != tok_c // width)
        second = ((iota((2 * width, order), 1) % span) // width) % 2 == 1
        odd, half, fill, wide, merged = [], [], [], [], []
        for n, t in enumerate(inv):
            odd.append(jnp.where(second, t, 0.0))
            th, tl = split(odd[n])
            high, low = pieces(n)
            if last:
                y = jnp.where(second, 0.0, pair_dot(th, tl, high, low))
            else:
                y = pair_dot(th, tl, jnp.where(corner, high, zero), jnp.where(corner, low, zero))
            half.append(y)
            parts = []
            for j in range(2):
                part = t[j * width : (j + 1) * width]
                if width < 16:
                    part = jnp.concatenate([part] * (16 // width), axis=0)
                parts.append((split(part), span // part.shape[0]))
            full = [
                jnp.concatenate([p[k] for p, count in parts for _ in range(count)], axis=0)
                for k in range(2)
            ]
            if not last:
                full = [jnp.where(diagonal, f, zero) for f in full]
            wide.append(full)
            yield
        for y, full in zip(half, wide):
            yh, yl = split(y)
            r = pair_dot(yh, yl, full[0], full[1])
            fill.append(jnp.where(second, 0.0, r) if last else r)
            yield
        for t, o, r in zip(inv, odd, fill):
            even, lower = t - o, o - r
            merged.append(
                jnp.concatenate(
                    [even[:width], lower[:width], even[width:], lower[width:]], axis=0
                )
            )
        inv = merged
        width *= 2
    return inv


def fused_kernel(
    seq_axis, peers, axis, q_hbm, k_hbm, v_hbm, b_ref, g_hbm, w_hbm, y_hbm,
    q_ref, k_ref, v_ref, g_ref, beta_ref, stack_ref, turn_ref, source_ref, x_ref, start_ref,
    low_ref, inv_ref, weight_ref, eye_ref,
    maps, held, carry_ref, states, s_ref, o_ref, m_ref,
    mixed, weight, total, far_out, far_in, near_out, near_in, cross_out, cross_in, y_ref,
    kv_sem, q_sem, g_sem, load_sem, y_sem, map_send, map_recv, back_send, back_recv,
    far_send, far_recv, near_send, near_recv, cross_send, cross_recv,
):
    heads, blocks, span = q_ref.shape[0], q_ref.shape[1], q_ref.shape[2]
    pairs = heads // 2
    parts = 2
    batch = blocks // parts
    seq = lax.axis_index(seq_axis)
    me = lax.axis_index(axis)
    chip, core = me // 2, me % 2
    sibling = 2 * chip + 1 - core
    across = 2 * (1 - chip) + core
    beyond = 2 * (1 - chip) + 1 - core
    width = y_ref.shape[2]

    barrier = pltpu.get_barrier_semaphore()
    for other in (sibling, across):
        pl.semaphore_signal(barrier, inc=1, device_id={axis: other}, device_id_type=MESH)
    for away in range(1, peers):
        pl.semaphore_signal(
            barrier,
            inc=1,
            device_id={seq_axis: lax.rem(seq + away, peers)},
            device_id_type=MESH,
        )

    def columns(h):
        return pl.ds(pl.multiple_of(h * HEAD_DIM, HEAD_DIM), HEAD_DIM)

    def fetch_kv(h):
        return (
            pltpu.make_async_copy(k_hbm.at[:, :, :, columns(h)], k_ref.at[h], kv_sem.at[0, h]),
            pltpu.make_async_copy(v_hbm.at[:, :, :, columns(h)], v_ref.at[h], kv_sem.at[1, h]),
        )

    def fetch_q(h):
        return pltpu.make_async_copy(q_hbm.at[:, :, columns(h)], q_ref.at[h], q_sem.at[h])

    def fetch_g(h):
        return pltpu.make_async_copy(g_hbm.at[:, :, columns(h)], g_ref.at[h], g_sem.at[h])

    def load(n):
        owner = (beyond, across, sibling, me)[n]
        return pltpu.make_async_copy(
            w_hbm.at[:, pl.ds(pl.multiple_of(owner * width, width), width)],
            weight.at[n],
            load_sem.at[n],
        )

    for h in range(heads):
        for copy in fetch_kv(h):
            copy.start()
    for h in range(heads):
        fetch_q(h).start()
    for blk in range(blocks):
        window = slice(blk * span, (blk + 1) * span)
        beta_ref[blk] = jnp.concatenate([b_ref[:, 0, window], b_ref[:, 1, window]], axis=1)
    begin = (iota((HEAD_DIM, 2 * HEAD_DIM), 0) == iota((HEAD_DIM, 2 * HEAD_DIM), 1)).astype(F32)
    for h in range(heads):
        x_ref[h] = begin
    eye_ref[...] = (iota(eye_ref.shape, 0) == iota(eye_ref.shape, 1)).astype(F32)

    def place(it, n):
        pair, part = it // parts, it % parts
        return 2 * pair + n % 2, part * batch + n // 2

    count = 2 * batch

    def key_of(h, blk):
        return jnp.concatenate([k_ref[h, 0, blk], k_ref[h, 1, blk]], axis=0)

    def stack_of(h, blk):
        none = jnp.zeros((HEAD_DIM, HEAD_DIM), BF16)
        return jnp.concatenate(
            [
                jnp.concatenate([stack_ref[h, blk, 0], stack_ref[h, blk, 2]], axis=1),
                jnp.concatenate([stack_ref[h, blk, 1], none], axis=1),
            ],
            axis=0,
        )

    def solve(it):
        slot = it % 2
        grams, squares = [], []
        for n in range(count):
            key = key_of(*place(it, n))
            grams.append(dot_t(key, key))
            if n % 2:
                yield
        for n, g in enumerate(grams):
            squares.append(jnp.sum(eye_ref[...] * g, axis=0, keepdims=True))
            if n % 4 == 3:
                yield
        beta = jnp.concatenate(
            [beta_ref[place(it, n)[1], pl.ds(place(it, n)[0], 1), :] for n in range(count)], axis=0
        )
        norm = lax.rsqrt(jnp.concatenate(squares, axis=0) + 1e-06)
        value_weight = beta * norm
        weight_rows = value_weight * norm
        weight_ref[slot, 0] = weight_rows
        weight_ref[slot, 1] = value_weight
        weight_cols = weight_rows.T
        yield
        lowers = []
        for n, g in enumerate(grams):
            low = weight_cols[:, n : n + 1] * g
            lowers.append(low)
            low_ref[slot, n, 0], low_ref[slot, n, 1] = split(low)
            if n % 2:
                yield
        inv = yield from base_solve(lowers, span)
        for n in range(count):
            inv_ref[slot, n] = inv[n]

    def transit(it):
        slot = it % 2

        def pieces(n):
            return low_ref[slot, n, 0], low_ref[slot, n, 1]

        solved = yield from merge([inv_ref[slot, n] for n in range(count)], pieces, span)
        turns, writes, changes = [], [], []
        for n in range(count):
            h, blk = place(it, n)
            th, tl = split(solved[n] * weight_ref[slot, 0, n : n + 1, :])
            tv = (solved[n] * weight_ref[slot, 1, n : n + 1, :]).astype(BF16)
            key = key_of(h, blk)
            value = jnp.concatenate([v_ref[h, 0, blk], v_ref[h, 1, blk]], axis=0)
            turns.append(
                dot(jnp.concatenate([th, tl], axis=1), jnp.concatenate([key, key], axis=0))
            )
            writes.append(dot(tv, value))
            yield
        for n in range(count):
            h, blk = place(it, n)
            turn_h, turn_l = split(turns[n])
            stack_ref[h, blk, 0], stack_ref[h, blk, 1] = turn_h, turn_l
            stack_ref[h, blk, 2] = writes[n].astype(BF16)
            stack = stack_of(h, blk)
            key_t = key_of(h, blk).T
            changes.append(dot(jnp.concatenate([key_t, key_t], axis=1), stack))
            yield
        for n in range(count):
            step = eye_ref[...] - changes[n][:, :HEAD_DIM]
            turn_ref[slot, n, 0], turn_ref[slot, n, 1] = split(step)
            source_ref[slot, n] = changes[n][:, HEAD_DIM:]
            yield

    def compose(it):
        slot = it % 2
        pair, part = it // parts, it % parts
        states_now = [x_ref[2 * pair + i] for i in range(2)]
        for n in range(count):
            h, blk = place(it, n)
            i = n % 2
            high, low = split(states_now[i])
            start_ref[h, blk, 0] = high[:, :HEAD_DIM]
            start_ref[h, blk, 1] = high[:, HEAD_DIM:]
            turn_h, turn_l = turn_ref[slot, n, 0], turn_ref[slot, n, 1]
            moved = dot(
                jnp.concatenate([turn_h, turn_l, turn_h], axis=1),
                jnp.concatenate([high, high, low], axis=0),
            )
            states_now[i] = jnp.concatenate(
                [moved[:, :HEAD_DIM], moved[:, HEAD_DIM:] + source_ref[slot, n]], axis=1
            )
            if n >= count - 2:
                x_ref[h] = states_now[i]
            yield

    def a_stream(it, first=0.0, last=1.0):
        return 7 * count // 4 + BASE, solve(it), first, last

    def b_stream(it, first=0.0, last=1.0):
        return 9 * count, transit(it), first, last

    def c_stream(it, first=0.0, last=1.0):
        return count, compose(it), first, last

    def owner_of(pair, i):
        side = lax.rem(pair + core, 2)
        return peers // 2 - 2 + side + i * (3 - 2 * side)

    def send_map(pair, i, source):
        h = 2 * pair + i
        return pltpu.make_async_remote_copy(
            src_ref=maps.at[h],
            dst_ref=held.at[pair, source],
            send_sem=map_send.at[h],
            recv_sem=map_recv.at[pair, source],
            device_id={seq_axis: owner_of(pair, i)},
            device_id_type=MESH,
        )

    def send_state(pair, i, target):
        h = 2 * pair + i
        return pltpu.make_async_remote_copy(
            src_ref=states.at[pair, target],
            dst_ref=s_ref.at[h],
            send_sem=back_send.at[pair, target],
            recv_sem=back_recv.at[h],
            device_id={seq_axis: target},
            device_id_type=MESH,
        )

    def post(pair):
        for i in range(2):
            h = 2 * pair + i
            maps[h, 0] = x_ref[h, :, :HEAD_DIM].astype(BF16)
            maps[h, 1] = x_ref[h, :, HEAD_DIM:].astype(BF16)

            @pl.when((seq != owner_of(pair, i)) & (seq != peers - 1))
            def _():
                send_map(pair, i, seq).start()

            @pl.when(seq == owner_of(pair, i))
            def _():
                held[pair, seq] = maps[h]

    def chain(pair):
        for i in range(2):

            @pl.when(seq == owner_of(pair, i))
            def _():
                carry_ref[...] = jnp.zeros((HEAD_DIM, HEAD_DIM), F32)
                for k in range(peers - 1):

                    @pl.when(seq != k)
                    def _():
                        send_map(pair, i, k).wait_recv()

                    high, low = split(carry_ref[...])
                    turn = held[pair, k, 0]
                    state = held[pair, k, 1].astype(F32) + dot(
                        jnp.concatenate([turn, turn], axis=1),
                        jnp.concatenate([high, low], axis=0),
                    )
                    carry_ref[...] = state
                    states[pair, k + 1] = state.astype(BF16)

                    @pl.when(seq != k + 1)
                    def _():
                        send_state(pair, i, k + 1).start()

                    @pl.when(seq == k + 1)
                    def _():
                        s_ref[2 * pair + i] = states[pair, k + 1]

    @pl.when(seq == 0)
    def _():
        s_ref[...] = jnp.zeros(s_ref.shape, BF16)

    def wait_kv(pair):
        for i in range(2):
            for copy in fetch_kv(2 * pair + i):
                copy.wait()

    steps = parts * pairs
    wait_kv(0)
    weave(a_stream(0))
    for n in range(4):
        load(n).start()
    for h in range(heads):
        fetch_g(h).start()
    weave(a_stream(1), b_stream(0))

    def step(it, _):
        @pl.when(it % parts == 0)
        def _():
            wait_kv(it // parts)

        weave(a_stream(it), b_stream(it - 1), c_stream(it - 2))

        @pl.when(it == parts + 1)
        def _():
            pl.semaphore_wait(barrier, peers + 1)

        @pl.when(it % parts == 1)
        def _():
            post(it // parts - 1)

        @pl.when(it == steps - 2)
        def _():
            chain(0)

        return 0

    lax.fori_loop(2, steps, step, 0)
    weave(
        b_stream(steps - 1, 0.0, 9.0),
        c_stream(steps - 2, 0.0, 6.0),
        c_stream(steps - 1, 8.1, 9.1),
    )
    post(pairs - 1)
    for h in range(heads):
        fetch_q(h).wait()

    def read(pair, _):
        causal = iota((span, 2 * span), 1) % span <= iota((span, 2 * span), 0)
        for i in range(2):
            h = 2 * pair + i
            scores = []
            for blk in range(blocks):
                found = jnp.where(causal, dot_t(q_ref[h, blk], key_of(h, blk)), 0.0).astype(BF16)
                scores.append(jnp.concatenate([found, found], axis=1))
            drawn = [dot(score, stack_of(h, blk)) for blk, score in enumerate(scores)]
            for blk in range(blocks):
                kept = (q_ref[h, blk].astype(F32) - drawn[blk][:, :HEAD_DIM]).astype(BF16)
                out = dot(kept, jnp.concatenate([start_ref[h, blk, 0], start_ref[h, blk, 1]], axis=1))
                m_ref[h, blk] = out[:, :HEAD_DIM].astype(BF16)
                o_ref[h, blk] = out[:, HEAD_DIM:] + drawn[blk][:, HEAD_DIM:]

        return 0

    chain(1)
    lax.fori_loop(0, pairs, read, 0)
    for h in range(heads):
        fetch_g(h).wait()

    def wait_state(pair):
        for i in range(2):

            @pl.when((seq != owner_of(pair, i)) & (seq != 0))
            def _():
                send_state(pair, i, seq).wait_recv()

    def blend(pair, t):
        for i in range(2):
            h = 2 * pair + i
            query = q_ref[h, t].astype(F32)
            unit = lax.rsqrt(jnp.sum(query * query, axis=1, keepdims=True) + 1e-06)
            seen = unit * (o_ref[h, t] + dot(m_ref[h, t], s_ref[h]))
            scale = lax.rsqrt(jnp.mean(seen * seen, axis=1, keepdims=True) + 1e-06)
            gate = g_ref[h, t].astype(F32)
            mixed[t, h] = (seen * scale * (gate / (1.0 + jnp.exp(-gate)))).astype(BF16)

    def blend_pair(pair):
        wait_state(pair)
        for blk in range(blocks):
            blend(pair, blk)

    def settle(pair, _):
        chain(pair + 2)
        blend_pair(pair)
        return 0

    lax.fori_loop(0, pairs - 2, settle, 0)
    blend_pair(pairs - 2)

    def send(source, target, send_sem, recv_sem, t, device):
        return pltpu.make_async_remote_copy(
            src_ref=source.at[t],
            dst_ref=target.at[t],
            send_sem=send_sem.at[t],
            recv_sem=recv_sem.at[t],
            device_id={axis: device},
            device_id_type=MESH,
        )

    def far(t):
        return send(far_out, far_in, far_send, far_recv, t, sibling)

    def near(t):
        return send(near_out, near_in, near_send, near_recv, t, sibling)

    def cross(t):
        return send(cross_out, cross_in, cross_send, cross_recv, t, across)

    def pass_on(t):
        far(t).wait()
        cross_out[t] = (total[t] + far_in[t].astype(F32)).astype(BF16)
        cross(t).start()

    share = blocks // PIECES

    def rows_of(t, first, last):
        return jnp.concatenate(
            [
                jnp.concatenate([mixed[t * share + b, h] for h in range(first, last)], axis=1)
                for b in range(share)
            ],
            axis=0,
        )

    def product(t, n):
        return dot(rows_of(t, 0, heads), weight[n])

    def finish_piece(t):
        for b in range(share):
            blend(pairs - 1, t * share + b)

    early = (heads - 2) * HEAD_DIM
    load(0).wait()
    total[0] = dot(rows_of(0, 0, heads - 2), weight[0, :early, :])
    wait_state(pairs - 1)
    finish_piece(0)
    far_out[0] = (total[0] + dot(rows_of(0, heads - 2, heads), weight[0, early:, :])).astype(BF16)
    far(0).start()
    load(1).wait()
    total[0] = product(0, 1)
    for t in range(1, PIECES):
        finish_piece(t)
        far_out[t] = product(t, 0).astype(BF16)
        far(t).start()
        if t > 1:
            total[t] = product(t, 1)
        pass_on(t - 1)
        if t == 1:
            total[t] = product(t, 1)
    load(2).wait()
    for t in range(PIECES):
        near_out[t] = product(t, 2).astype(BF16)
        near(t).start()
        if t == 0:
            pass_on(PIECES - 1)
    load(3).wait()
    for t in range(PIECES):
        total[t] = product(t, 3)

    def put(t):
        rows = y_ref.shape[1]
        return pltpu.make_async_copy(y_ref.at[t], y_hbm.at[pl.ds(t * rows, rows)], y_sem.at[t])

    for t in range(PIECES):
        near(t).wait()
        cross(t).wait()
        y_ref[t] = (total[t] + near_in[t].astype(F32) + cross_in[t].astype(F32)).astype(BF16)
        put(t).start()
    for pair in range(pairs):
        for i in range(2):

            @pl.when((seq != owner_of(pair, i)) & (seq != peers - 1))
            def _():
                send_map(pair, i, seq).wait_send()

            @pl.when(seq == owner_of(pair, i))
            def _():
                for k in range(1, peers):

                    @pl.when(seq != k)
                    def _():
                        send_state(pair, i, k).wait_send()

    for t in range(PIECES):
        put(t).wait()


def fused(queries, keys, values, betas, gate, out_weight, seq_axis, axis):
    tokens, depth = queries.shape
    heads = depth // HEAD_DIM
    peers = lax.axis_size(seq_axis)
    width = out_weight.shape[1] // lax.axis_size(axis)
    blocks = tokens // SPAN
    batch = blocks // 2
    vmem = pl.BlockSpec(memory_space=pltpu.VMEM)
    hbm = pl.BlockSpec(memory_space=pl.ANY)
    piece = (PIECES, tokens // PIECES, width)
    square = (HEAD_DIM, HEAD_DIM)
    wide = (HEAD_DIM, 2 * HEAD_DIM)
    two = (2,) + square
    pairs = heads // 2
    dma = pltpu.SemaphoreType.DMA
    per_head = (heads, blocks, SPAN, HEAD_DIM)
    both = (heads, 2, blocks, SPAN, HEAD_DIM)
    return pl.pallas_call(
        functools.partial(fused_kernel, seq_axis, peers, axis),
        in_specs=[hbm, hbm, hbm, vmem, hbm, hbm],
        out_specs=hbm,
        out_shape=jax.ShapeDtypeStruct((tokens, width), BF16),
        scratch_shapes=[
            pltpu.VMEM(per_head, BF16),
            pltpu.VMEM(both, BF16),
            pltpu.VMEM(both, BF16),
            pltpu.VMEM(per_head, BF16),
            pltpu.VMEM((blocks, heads, 2 * SPAN), F32),
            pltpu.VMEM((heads, blocks, 3) + square, BF16),
            pltpu.VMEM((2, 2 * batch) + two, BF16),
            pltpu.VMEM((2, 2 * batch) + square, F32),
            pltpu.VMEM((heads,) + wide, F32),
            pltpu.VMEM((heads, blocks) + two, BF16),
            pltpu.VMEM((2, 2 * batch) + two, BF16),
            pltpu.VMEM((2, 2 * batch, BASE, 2 * SPAN), F32),
            pltpu.VMEM((2, 2, 2 * batch, 2 * SPAN), F32),
            pltpu.VMEM(square, F32),
            pltpu.VMEM((heads,) + two, BF16),
            pltpu.VMEM((pairs, peers) + two, BF16),
            pltpu.VMEM(square, F32),
            pltpu.VMEM((pairs, peers) + square, BF16),
            pltpu.VMEM((heads,) + square, BF16),
            pltpu.VMEM(per_head, F32),
            pltpu.VMEM(per_head, BF16),
            pltpu.VMEM((blocks, heads, SPAN, HEAD_DIM), BF16),
            pltpu.VMEM((4, depth, width), BF16),
            pltpu.VMEM(piece, F32),
        ]
        + [pltpu.VMEM(piece, BF16)] * 6
        + [
            pltpu.VMEM(piece, BF16),
            dma((2, heads)),
            dma((heads,)),
            dma((heads,)),
            dma((4,)),
            dma((PIECES,)),
            dma((heads,)),
            dma((pairs, peers)),
            dma((pairs, peers)),
            dma((heads,)),
        ]
        + [dma((PIECES,))] * 6,
        compiler_params=pltpu.CompilerParams(
            collective_id=0, has_side_effects=True, vmem_limit_bytes=VMEM_LIMIT
        ),
    )(
        queries.reshape(blocks, SPAN, depth),
        keys.reshape(2, blocks, SPAN, depth),
        values.reshape(2, blocks, SPAN, depth),
        betas,
        gate.reshape(blocks, SPAN, depth),
        out_weight,
    )


def start_state(maps, axis):
    peers, index = lax.axis_size(axis), lax.axis_index(axis)
    heads = maps.shape[0]
    held = lax.all_gather(maps, axis, axis=0, tiled=True)
    states = pl.pallas_call(
        functools.partial(chain_kernel, peers),
        out_shape=jax.ShapeDtypeStruct((held.shape[0], HEAD_DIM, HEAD_DIM), BF16),
        compiler_params=pltpu.CompilerParams(vmem_limit_bytes=VMEM_LIMIT),
    )(held)
    return lax.dynamic_slice_in_dim(states, index * heads, heads, 0)


def out_kernel(o_ref, m_ref, s_ref, g_ref, w_ref, y_ref, mixed_ref):
    @pl.when(pl.program_id(0) == 0)
    def _():
        for h in range(s_ref.shape[0]):
            cols = slice(h * HEAD_DIM, (h + 1) * HEAD_DIM)
            seen = o_ref[:, cols] + dot(m_ref[:, cols], s_ref[h])
            scale = lax.rsqrt(jnp.mean(seen * seen, axis=1, keepdims=True) + 1e-06)
            gate = g_ref[:, cols].astype(F32)
            mixed_ref[:, cols] = (seen * scale * (gate / (1.0 + jnp.exp(-gate)))).astype(BF16)

    y_ref[...] = dot(mixed_ref[...], w_ref[...]).astype(BF16)


def project(local, reach, states, gate, out_weight):
    tokens, width = local.shape
    total = out_weight.shape[1]
    tile = 512
    whole = pl.BlockSpec((tokens, width), lambda n: (0, 0))
    return pl.pallas_call(
        out_kernel,
        grid=(total // tile,),
        in_specs=[
            whole,
            whole,
            pl.BlockSpec(states.shape, lambda n: (0, 0, 0)),
            whole,
            pl.BlockSpec((width, tile), lambda n: (0, n)),
        ],
        out_specs=pl.BlockSpec((tokens, tile), lambda n: (0, n)),
        out_shape=jax.ShapeDtypeStruct((tokens, total), BF16),
        scratch_shapes=[pltpu.VMEM((tokens, width), BF16)],
        compiler_params=pltpu.CompilerParams(
            dimension_semantics=("arbitrary",), vmem_limit_bytes=VMEM_LIMIT
        ),
    )(local, reach, states, gate, out_weight)


def per_device(queries, keys, values, betas, gate, out_weight):
    heads, _, tokens = betas.shape
    peers, index = lax.axis_size("ctx"), lax.axis_size("head")
    if index == 4 and peers >= 4 and peers % 2 == 0 and heads % 8 == 0 and tokens % (8 * SPAN) == 0:
        return fused(queries, keys, values, betas, gate, out_weight, "ctx", "head")
    beta_cols = betas.transpose(2, 1, 0).reshape(2 * tokens, heads)
    local, reach, maps = mix(queries, keys, values, beta_cols)
    states = start_state(maps, "ctx")
    partial_sum = project(local, reach, states, gate, out_weight)
    return lax.psum_scatter(partial_sum, "head", scatter_dimension=1, tiled=True)


def solution(mesh):
    return jax.shard_map(
        per_device,
        mesh=mesh,
        in_specs=(
            P("ctx", "head"),
            P(None, "ctx", "head"),
            P(None, "ctx", "head"),
            P("head", None, "ctx"),
            P("ctx", "head"),
            P("head", None),
        ),
        out_specs=P("ctx", "head"),
        check_vma=False,
    )
```

```python
import functools

import jax
import jax.numpy as jnp
from jax import lax
from jax.experimental import pallas as pl
from jax.experimental.pallas import tpu as pltpu
from jax.sharding import PartitionSpec as P

HEAD_DIM = 128
SPAN = 64
BASE = 16
F32 = jnp.float32
BF16 = jnp.bfloat16
VMEM_LIMIT = 60 * 1024 * 1024
MESH = pl.DeviceIdType.MESH
PIECES = 4


def iota(shape, dim):
    return lax.broadcasted_iota(jnp.int32, shape, dim)


def split(a):
    high = a.astype(BF16)
    return high, (a - high.astype(F32)).astype(BF16)


def dot(a, b):
    return jnp.dot(a, b, preferred_element_type=F32)


def dot3(a, b):
    ah, al = split(a)
    bh, bl = split(b)
    return dot(jnp.concatenate([ah, al, ah], axis=1), jnp.concatenate([bh, bh, bl], axis=0))


def inverse(lowers, order):
    lane = iota((BASE, order), 1)
    compact = []
    for low in lowers:
        total = jnp.zeros((BASE, order), F32)
        for blk in range(order // BASE):
            total = jnp.where(lane // BASE == blk, low[blk * BASE : (blk + 1) * BASE, :], total)
        compact.append(total)
    inv = [(iota((BASE, order), 0) == lane % BASE).astype(F32) for _ in lowers]
    for j in range(BASE - 1):
        pick = (lane // BASE) * BASE + j
        for n, low in enumerate(compact):
            column = jnp.take_along_axis(low, pick, axis=1, mode="promise_in_bounds")
            inv[n] = inv[n] - column * inv[n][j : j + 1, :]
    row = iota((order, order), 0)
    col = iota((order, order), 1)
    width = BASE
    while width < order:
        corner = (row // (2 * width) == col // (2 * width)) & (row // width != col // width)
        diagonal = row // width == col // width
        second = (iota((width, order), 1) // width) % 2 == 1
        half = [dot3(jnp.where(second, t, 0.0), jnp.where(corner, low, 0.0)) for t, low in zip(inv, lowers)]
        full = [
            jnp.where(diagonal, jnp.concatenate([t] * (order // width), axis=0), 0.0) for t in inv
        ]
        fill = [dot3(y, e) for y, e in zip(half, full)]
        inv = [
            jnp.concatenate([jnp.where(second, 0.0, t), jnp.where(second, t, 0.0) - r], axis=0)
            for t, r in zip(inv, fill)
        ]
        width *= 2
    return inv


def mix_kernel(q_ref, k_ref, v_ref, b_ref, o_ref, m_ref, x_out, x_ref):
    heads = q_ref.shape[1] // HEAD_DIM
    span = q_ref.shape[0]
    order = 2 * span
    step = pl.program_id(0)

    @pl.when(step == 0)
    def _():
        start = (iota((HEAD_DIM, 2 * HEAD_DIM), 0) == iota((HEAD_DIM, 2 * HEAD_DIM), 1)).astype(F32)
        for h in range(heads):
            x_ref[h] = start

    row = iota((order, order), 0)
    col = iota((order, order), 1)
    strict = col < row
    weave = (row == 2 * (col % span) + col // span).astype(BF16)
    causal = iota((span, order), 1) <= 2 * iota((span, order), 0) + 1
    data = []
    lowers = []
    for h in range(heads):
        cols = slice(h * HEAD_DIM, (h + 1) * HEAD_DIM)
        query = q_ref[:, cols]
        pair = jnp.concatenate(
            [
                jnp.concatenate([k_ref[0, :, cols], v_ref[0, :, cols]], axis=1),
                jnp.concatenate([k_ref[1, :, cols], v_ref[1, :, cols]], axis=1),
            ],
            axis=0,
        )
        woven = dot(weave, pair)
        key = woven[:, :HEAD_DIM]
        value = woven[:, HEAD_DIM:]
        key_b = key.astype(BF16)
        norm = lax.rsqrt(jnp.sum(key * key, axis=1, keepdims=True) + 1e-06)
        beta = b_ref[:, h : h + 1]
        both = jnp.concatenate([key_b, query], axis=0)
        gram = lax.dot_general(both, key_b, (((1,), (1,)), ((), ())), preferred_element_type=F32)
        weight = beta * norm * norm
        lowers.append(jnp.where(strict, weight * gram[:order], 0.0))
        scores = jnp.where(causal, gram[order:], 0.0).astype(BF16)
        qf = query.astype(F32)
        q_norm = lax.rsqrt(jnp.sum(qf * qf, axis=1, keepdims=True) + 1e-06)
        readers = jnp.concatenate([key.T.astype(BF16), scores], axis=0)
        data.append((both, readers, beta * norm * value, weight, q_norm))
    solved = inverse(lowers, order)
    seen = []
    for h in range(heads):
        both = data[h][0]
        high, low = split(x_ref[h])
        seen.append(
            dot(jnp.concatenate([both, both], axis=1), jnp.concatenate([high, low], axis=0))
        )
    writes = []
    for h in range(heads):
        _, _, scaled, weight, _ = data[h]
        gap = -weight * seen[h][:order]
        gap = jnp.concatenate([gap[:, :HEAD_DIM], gap[:, HEAD_DIM:] + scaled], axis=1)
        writes.append(dot3(solved[h], gap))
    for h in range(heads):
        cols = slice(h * HEAD_DIM, (h + 1) * HEAD_DIM)
        readers, q_norm = data[h][1], data[h][4]
        high, low = split(writes[h])
        change = dot(
            jnp.concatenate([readers, readers], axis=1), jnp.concatenate([high, low], axis=0)
        )
        x_ref[h] = x_ref[h] + change[:HEAD_DIM]
        out = q_norm * (seen[h][order:] + change[HEAD_DIM:])
        m_ref[:, cols] = out[:, :HEAD_DIM].astype(BF16)
        o_ref[:, cols] = out[:, HEAD_DIM:]

    @pl.when(step == pl.num_programs(0) - 1)
    def _():
        for h in range(heads):
            x_out[h] = x_ref[h].astype(BF16)


def mix(queries, keys, values, beta_cols):
    tokens, width = queries.shape
    heads = width // HEAD_DIM
    return pl.pallas_call(
        mix_kernel,
        grid=(tokens // SPAN,),
        in_specs=[
            pl.BlockSpec((SPAN, width), lambda c: (c, 0)),
            pl.BlockSpec((2, SPAN, width), lambda c: (0, c, 0)),
            pl.BlockSpec((2, SPAN, width), lambda c: (0, c, 0)),
            pl.BlockSpec((2 * SPAN, heads), lambda c: (c, 0)),
        ],
        out_specs=[
            pl.BlockSpec((SPAN, width), lambda c: (c, 0)),
            pl.BlockSpec((SPAN, width), lambda c: (c, 0)),
            pl.BlockSpec((heads, HEAD_DIM, 2 * HEAD_DIM), lambda c: (0, 0, 0)),
        ],
        out_shape=[
            jax.ShapeDtypeStruct((tokens, width), F32),
            jax.ShapeDtypeStruct((tokens, width), BF16),
            jax.ShapeDtypeStruct((heads, HEAD_DIM, 2 * HEAD_DIM), BF16),
        ],
        scratch_shapes=[pltpu.VMEM((heads, HEAD_DIM, 2 * HEAD_DIM), F32)],
        compiler_params=pltpu.CompilerParams(
            dimension_semantics=("arbitrary",), vmem_limit_bytes=VMEM_LIMIT
        ),
    )(queries, keys, values, beta_cols)


def chain_kernel(peers, x_ref, s_ref):
    heads = x_ref.shape[0] // peers
    for h in range(heads):
        state = jnp.zeros((HEAD_DIM, HEAD_DIM), F32)
        for k in range(peers):
            s_ref[k * heads + h] = state.astype(BF16)
            if k < peers - 1:
                maps = x_ref[k * heads + h]
                turn = maps[:, :HEAD_DIM]
                high, low = split(state)
                state = maps[:, HEAD_DIM:].astype(F32) + dot(
                    jnp.concatenate([turn, turn], axis=1), jnp.concatenate([high, low], axis=0)
                )


FUSED_LIMIT = 52 * 1024 * 1024


def dot_t(a, b):
    return lax.dot_general(a, b, (((1,), (1,)), ((), ())), preferred_element_type=F32)


def pair_dot(a, low, high_b, low_b):
    rows = a.shape[0]
    both = dot(jnp.concatenate([a, low], axis=0), jnp.concatenate([high_b, low_b], axis=1))
    width = high_b.shape[1]
    return both[:rows, :width] + both[rows:, :width] + both[:rows, width:]


def weave(*streams):
    order = []
    for n, (count, _, first, last) in enumerate(streams):
        order += [(first + (last - first) * (k + 0.5) / count, n) for k in range(count)]
    for _, n in sorted(order):
        next(streams[n][1], None)
    for _, stream, _, _ in streams:
        for _ in stream:
            pass


def base_solve(lowers, span):
    order = 2 * span
    base = BASE // 2
    lane = iota((base, order), 1)
    group = (lane % span) // base
    row16, lane16 = iota((BASE, order), 0), iota((BASE, order), 1)
    group16 = (lane16 % span) // base
    row_tok, lane_tok = row16 % base, lane16 % base
    before = (lane_tok < row_tok) | ((lane_tok == row_tok) & (lane16 // span < row16 // base))
    compact = []
    for n, low in enumerate(lowers):
        halves = []
        for j in range(2):
            total = jnp.zeros((base, order), F32)
            for blk in range(span // base):
                start = j * span + blk * base
                total = jnp.where(group == blk, low[start : start + base, :], total)
            halves.append(total)
        compact.append(jnp.where(before, jnp.concatenate(halves, axis=0), 0.0))
        if n % 2:
            yield
    own = (row16 % base == lane16 % base) & (row16 // base == lane16 // span)
    inv = [own.astype(F32) for _ in lowers]
    for s in range(BASE - 1):
        t, j = s // 2, s % 2
        pick = j * span + group16 * base + t
        for n, low in enumerate(compact):
            column = jnp.take_along_axis(low, pick, axis=1, mode="promise_in_bounds")
            inv[n] = inv[n] - column * inv[n][j * base + t : j * base + t + 1, :]
        yield
    return inv


def merge(inv, pieces, span):
    order = 2 * span
    tok_r = iota((order, order), 0) % span
    tok_c = iota((order, order), 1) % span
    width = BASE // 2
    zero = jnp.zeros((), BF16)
    while width < span:
        last = 2 * width == span
        diagonal = tok_r // width == tok_c // width
        corner = (tok_r // (2 * width) == tok_c // (2 * width)) & (tok_r // width != tok_c // width)
        second = ((iota((2 * width, order), 1) % span) // width) % 2 == 1
        odd, half, fill, wide, merged = [], [], [], [], []
        for n, t in enumerate(inv):
            odd.append(jnp.where(second, t, 0.0))
            th, tl = split(odd[n])
            high, low = pieces(n)
            if last:
                y = jnp.where(second, 0.0, pair_dot(th, tl, high, low))
            else:
                y = pair_dot(th, tl, jnp.where(corner, high, zero), jnp.where(corner, low, zero))
            half.append(y)
            parts = []
            for j in range(2):
                part = t[j * width : (j + 1) * width]
                if width < 16:
                    part = jnp.concatenate([part] * (16 // width), axis=0)
                parts.append((split(part), span // part.shape[0]))
            full = [
                jnp.concatenate([p[k] for p, count in parts for _ in range(count)], axis=0)
                for k in range(2)
            ]
            if not last:
                full = [jnp.where(diagonal, f, zero) for f in full]
            wide.append(full)
            yield
        for y, full in zip(half, wide):
            yh, yl = split(y)
            r = pair_dot(yh, yl, full[0], full[1])
            fill.append(jnp.where(second, 0.0, r) if last else r)
            yield
        for t, o, r in zip(inv, odd, fill):
            even, lower = t - o, o - r
            merged.append(
                jnp.concatenate(
                    [even[:width], lower[:width], even[width:], lower[width:]], axis=0
                )
            )
        inv = merged
        width *= 2
    return inv


def fused_kernel(
    seq_axis, peers, axis, q_hbm, k_hbm, v_hbm, b_hbm, g_hbm, w_hbm, y_ref,
    b_ref, q_ref, k_ref, v_ref, g_ref, beta_ref, stack_ref, turn_ref, source_ref, x_ref, start_ref,
    low_ref, inv_ref, weight_ref, eye_ref,
    maps, held, carry_ref, states, s_ref, o_ref, m_ref,
    mixed, weight, total, far_out, far_in, near_out, near_in, cross_out, cross_in,
    b_sem, kv_sem, q_sem, g_sem, load_sem, map_send, map_recv, back_send, back_recv,
    far_send, far_recv, near_send, near_recv, cross_send, cross_recv,
):
    heads, blocks, span = q_ref.shape[0], q_ref.shape[1], q_ref.shape[2]
    pairs = heads // 2
    parts = 2
    batch = blocks // parts
    seq = lax.axis_index(seq_axis)
    me = lax.axis_index(axis)
    chip, core = me // 2, me % 2
    sibling = 2 * chip + 1 - core
    across = 2 * (1 - chip) + core
    beyond = 2 * (1 - chip) + 1 - core
    width = y_ref.shape[2]

    def columns(h):
        return pl.ds(pl.multiple_of(h * HEAD_DIM, HEAD_DIM), HEAD_DIM)

    def fetch_kv(h):
        return (
            pltpu.make_async_copy(k_hbm.at[:, :, :, columns(h)], k_ref.at[h], kv_sem.at[0, h]),
            pltpu.make_async_copy(v_hbm.at[:, :, :, columns(h)], v_ref.at[h], kv_sem.at[1, h]),
        )

    def fetch_q(h):
        return pltpu.make_async_copy(q_hbm.at[:, :, columns(h)], q_ref.at[h], q_sem.at[h])

    def fetch_g(h):
        return pltpu.make_async_copy(g_hbm.at[:, :, columns(h)], g_ref.at[h], g_sem.at[h])

    def load(n):
        owner = (beyond, across, sibling, me)[n]
        return pltpu.make_async_copy(
            w_hbm.at[:, pl.ds(pl.multiple_of(owner * width, width), width)],
            weight.at[n],
            load_sem.at[n],
        )

    def start_kv(first, last):
        for h in range(first, last):
            for copy in fetch_kv(h):
                copy.start()

    fetch_b = pltpu.make_async_copy(b_hbm, b_ref, b_sem)
    fetch_b.start()
    start_kv(0, 2)
    barrier = pltpu.get_barrier_semaphore()
    for other in (sibling, across):
        pl.semaphore_signal(barrier, inc=1, device_id={axis: other}, device_id_type=MESH)
    for away in range(1, peers):
        pl.semaphore_signal(
            barrier,
            inc=1,
            device_id={seq_axis: lax.rem(seq + away, peers)},
            device_id_type=MESH,
        )

    begin = (iota((HEAD_DIM, 2 * HEAD_DIM), 0) == iota((HEAD_DIM, 2 * HEAD_DIM), 1)).astype(F32)
    for h in range(heads):
        x_ref[h] = begin
    eye_ref[...] = (iota(eye_ref.shape, 0) == iota(eye_ref.shape, 1)).astype(F32)
    fetch_b.wait()
    for blk in range(blocks):
        window = slice(blk * span, (blk + 1) * span)
        beta_ref[blk] = jnp.concatenate([b_ref[:, 0, window], b_ref[:, 1, window]], axis=1)

    def place(it, n):
        pair, part = it // parts, it % parts
        return 2 * pair + n % 2, part * batch + n // 2

    count = 2 * batch

    def key_of(h, blk):
        return jnp.concatenate([k_ref[h, 0, blk], k_ref[h, 1, blk]], axis=0)

    def stack_of(h, blk):
        none = jnp.zeros((HEAD_DIM, HEAD_DIM), BF16)
        return jnp.concatenate(
            [
                jnp.concatenate([stack_ref[h, blk, 0], stack_ref[h, blk, 2]], axis=1),
                jnp.concatenate([stack_ref[h, blk, 1], none], axis=1),
            ],
            axis=0,
        )

    def solve(it):
        slot = it % 2
        grams, squares = [], []
        for n in range(count):
            key = key_of(*place(it, n))
            grams.append(dot_t(key, key))
            if n % 2:
                yield
        for n, g in enumerate(grams):
            squares.append(jnp.sum(eye_ref[...] * g, axis=0, keepdims=True))
            if n % 4 == 3:
                yield
        beta = jnp.concatenate(
            [beta_ref[place(it, n)[1], pl.ds(place(it, n)[0], 1), :] for n in range(count)], axis=0
        )
        norm = lax.rsqrt(jnp.concatenate(squares, axis=0) + 1e-06)
        value_weight = beta * norm
        weight_rows = value_weight * norm
        weight_ref[slot, 0] = weight_rows
        weight_ref[slot, 1] = value_weight
        weight_cols = weight_rows.T
        yield
        lowers = []
        for n, g in enumerate(grams):
            low = weight_cols[:, n : n + 1] * g
            lowers.append(low)
            low_ref[slot, n, 0], low_ref[slot, n, 1] = split(low)
            if n % 2:
                yield
        inv = yield from base_solve(lowers, span)
        for n in range(count):
            inv_ref[slot, n] = inv[n]

    def transit(it):
        slot = it % 2

        def pieces(n):
            return low_ref[slot, n, 0], low_ref[slot, n, 1]

        solved = yield from merge([inv_ref[slot, n] for n in range(count)], pieces, span)
        turns, writes, changes = [], [], []
        for n in range(count):
            h, blk = place(it, n)
            th, tl = split(solved[n] * weight_ref[slot, 0, n : n + 1, :])
            tv = (solved[n] * weight_ref[slot, 1, n : n + 1, :]).astype(BF16)
            key = key_of(h, blk)
            value = jnp.concatenate([v_ref[h, 0, blk], v_ref[h, 1, blk]], axis=0)
            turns.append(
                dot(jnp.concatenate([th, tl], axis=1), jnp.concatenate([key, key], axis=0))
            )
            writes.append(dot(tv, value))
            yield
        for n in range(count):
            h, blk = place(it, n)
            turn_h, turn_l = split(turns[n])
            stack_ref[h, blk, 0], stack_ref[h, blk, 1] = turn_h, turn_l
            stack_ref[h, blk, 2] = writes[n].astype(BF16)
            stack = stack_of(h, blk)
            key_t = key_of(h, blk).T
            changes.append(dot(jnp.concatenate([key_t, key_t], axis=1), stack))
            yield
        for n in range(count):
            step = eye_ref[...] - changes[n][:, :HEAD_DIM]
            turn_ref[slot, n, 0], turn_ref[slot, n, 1] = split(step)
            source_ref[slot, n] = changes[n][:, HEAD_DIM:]
            yield

    def compose(it):
        slot = it % 2
        pair, part = it // parts, it % parts
        states_now = [x_ref[2 * pair + i] for i in range(2)]
        for n in range(count):
            h, blk = place(it, n)
            i = n % 2
            high, low = split(states_now[i])
            start_ref[h, blk, 0] = high[:, :HEAD_DIM]
            start_ref[h, blk, 1] = high[:, HEAD_DIM:]
            turn_h, turn_l = turn_ref[slot, n, 0], turn_ref[slot, n, 1]
            moved = dot(
                jnp.concatenate([turn_h, turn_l, turn_h], axis=1),
                jnp.concatenate([high, high, low], axis=0),
            )
            states_now[i] = jnp.concatenate(
                [moved[:, :HEAD_DIM], moved[:, HEAD_DIM:] + source_ref[slot, n]], axis=1
            )
            if n >= count - 2:
                x_ref[h] = states_now[i]
            yield

    def a_stream(it, first=0.0, last=1.0):
        return 7 * count // 4 + BASE, solve(it), first, last

    def b_stream(it, first=0.0, last=1.0):
        return 9 * count, transit(it), first, last

    def c_stream(it, first=0.0, last=1.0):
        return count, compose(it), first, last

    def owner_of(pair, i):
        side = lax.rem(pair + core, 2)
        return peers // 2 - 2 + side + i * (3 - 2 * side)

    def send_map(pair, i, source):
        h = 2 * pair + i
        return pltpu.make_async_remote_copy(
            src_ref=maps.at[h],
            dst_ref=held.at[pair, source],
            send_sem=map_send.at[h],
            recv_sem=map_recv.at[pair, source],
            device_id={seq_axis: owner_of(pair, i)},
            device_id_type=MESH,
        )

    def send_state(pair, i, target):
        h = 2 * pair + i
        return pltpu.make_async_remote_copy(
            src_ref=states.at[pair, target],
            dst_ref=s_ref.at[h],
            send_sem=back_send.at[pair, target],
            recv_sem=back_recv.at[h],
            device_id={seq_axis: target},
            device_id_type=MESH,
        )

    def post(pair):
        for i in range(2):
            h = 2 * pair + i
            maps[h, 0] = x_ref[h, :, :HEAD_DIM].astype(BF16)
            maps[h, 1] = x_ref[h, :, HEAD_DIM:].astype(BF16)

            @pl.when((seq != owner_of(pair, i)) & (seq != peers - 1))
            def _():
                send_map(pair, i, seq).start()

            @pl.when(seq == owner_of(pair, i))
            def _():
                held[pair, seq] = maps[h]

    def chain(pair):
        for i in range(2):

            @pl.when(seq == owner_of(pair, i))
            def _():
                carry_ref[...] = jnp.zeros((HEAD_DIM, HEAD_DIM), F32)
                for k in range(peers - 1):

                    @pl.when(seq != k)
                    def _():
                        send_map(pair, i, k).wait_recv()

                    high, low = split(carry_ref[...])
                    turn = held[pair, k, 0]
                    state = held[pair, k, 1].astype(F32) + dot(
                        jnp.concatenate([turn, turn], axis=1),
                        jnp.concatenate([high, low], axis=0),
                    )
                    carry_ref[...] = state
                    states[pair, k + 1] = state.astype(BF16)

                    @pl.when(seq != k + 1)
                    def _():
                        send_state(pair, i, k + 1).start()

                    @pl.when(seq == k + 1)
                    def _():
                        s_ref[2 * pair + i] = states[pair, k + 1]

    @pl.when(seq == 0)
    def _():
        s_ref[...] = jnp.zeros(s_ref.shape, BF16)

    def wait_kv(pair):
        for i in range(2):
            for copy in fetch_kv(2 * pair + i):
                copy.wait()

    steps = parts * pairs
    wait_kv(0)
    start_kv(2, heads)
    weave(a_stream(0))
    for h in range(heads):
        fetch_q(h).start()
    for n in range(4):
        load(n).start()
    for h in range(heads):
        fetch_g(h).start()
    weave(a_stream(1), b_stream(0))

    def step(it, _):
        @pl.when(it % parts == 0)
        def _():
            wait_kv(it // parts)

        weave(a_stream(it), b_stream(it - 1), c_stream(it - 2))

        @pl.when(it == parts + 1)
        def _():
            pl.semaphore_wait(barrier, peers + 1)

        @pl.when(it % parts == 1)
        def _():
            post(it // parts - 1)

        @pl.when(it == steps - 2)
        def _():
            chain(0)

        return 0

    lax.fori_loop(2, steps, step, 0)
    weave(
        b_stream(steps - 1, 0.0, 9.0),
        c_stream(steps - 2, 0.0, 6.0),
        c_stream(steps - 1, 8.1, 9.1),
    )
    post(pairs - 1)
    for h in range(heads):
        fetch_q(h).wait()

    def read(pair, _):
        causal = iota((span, 2 * span), 1) % span <= iota((span, 2 * span), 0)
        for i in range(2):
            h = 2 * pair + i
            scores = []
            for blk in range(blocks):
                found = jnp.where(causal, dot_t(q_ref[h, blk], key_of(h, blk)), 0.0).astype(BF16)
                scores.append(jnp.concatenate([found, found], axis=1))
            drawn = [dot(score, stack_of(h, blk)) for blk, score in enumerate(scores)]
            for blk in range(blocks):
                kept = (q_ref[h, blk].astype(F32) - drawn[blk][:, :HEAD_DIM]).astype(BF16)
                out = dot(kept, jnp.concatenate([start_ref[h, blk, 0], start_ref[h, blk, 1]], axis=1))
                m_ref[h, blk] = out[:, :HEAD_DIM].astype(BF16)
                o_ref[h, blk] = out[:, HEAD_DIM:] + drawn[blk][:, HEAD_DIM:]

        return 0

    chain(1)
    lax.fori_loop(0, pairs, read, 0)
    for h in range(heads):
        fetch_g(h).wait()

    def wait_state(pair):
        for i in range(2):

            @pl.when((seq != owner_of(pair, i)) & (seq != 0))
            def _():
                send_state(pair, i, seq).wait_recv()

    def blend(pair, t):
        for i in range(2):
            h = 2 * pair + i
            query = q_ref[h, t].astype(F32)
            unit = lax.rsqrt(jnp.sum(query * query, axis=1, keepdims=True) + 1e-06)
            seen = unit * (o_ref[h, t] + dot(m_ref[h, t], s_ref[h]))
            scale = lax.rsqrt(jnp.mean(seen * seen, axis=1, keepdims=True) + 1e-06)
            gate = g_ref[h, t].astype(F32)
            mixed[t, h] = (seen * scale * (gate / (1.0 + jnp.exp(-gate)))).astype(BF16)

    def blend_pair(pair):
        wait_state(pair)
        for blk in range(blocks):
            blend(pair, blk)

    def settle(pair, _):
        chain(pair + 2)
        blend_pair(pair)
        return 0

    lax.fori_loop(0, pairs - 2, settle, 0)
    blend_pair(pairs - 2)

    def send(source, target, send_sem, recv_sem, t, device):
        return pltpu.make_async_remote_copy(
            src_ref=source.at[t],
            dst_ref=target.at[t],
            send_sem=send_sem.at[t],
            recv_sem=recv_sem.at[t],
            device_id={axis: device},
            device_id_type=MESH,
        )

    def far(t):
        return send(far_out, far_in, far_send, far_recv, t, sibling)

    def near(t):
        return send(near_out, near_in, near_send, near_recv, t, sibling)

    def cross(t):
        return send(cross_out, cross_in, cross_send, cross_recv, t, across)

    def pass_on(t):
        far(t).wait()
        cross_out[t] = (total[t] + far_in[t].astype(F32)).astype(BF16)
        cross(t).start()

    share = blocks // PIECES

    def rows_of(t, first, last):
        return jnp.concatenate(
            [
                jnp.concatenate([mixed[t * share + b, h] for h in range(first, last)], axis=1)
                for b in range(share)
            ],
            axis=0,
        )

    def product(t, n):
        return dot(rows_of(t, 0, heads), weight[n])

    def finish_piece(t):
        for b in range(share):
            blend(pairs - 1, t * share + b)

    early = (heads - 2) * HEAD_DIM
    load(0).wait()
    total[0] = dot(rows_of(0, 0, heads - 2), weight[0, :early, :])
    wait_state(pairs - 1)
    finish_piece(0)
    far_out[0] = (total[0] + dot(rows_of(0, heads - 2, heads), weight[0, early:, :])).astype(BF16)
    far(0).start()
    load(1).wait()
    total[0] = product(0, 1)
    for t in range(1, PIECES):
        finish_piece(t)
        far_out[t] = product(t, 0).astype(BF16)
        far(t).start()
        if t > 1:
            total[t] = product(t, 1)
        pass_on(t - 1)
        if t == 1:
            total[t] = product(t, 1)
    load(2).wait()
    for t in range(PIECES):
        near_out[t] = product(t, 2).astype(BF16)
        near(t).start()
        if t == 0:
            pass_on(PIECES - 1)
    load(3).wait()
    for t in range(PIECES):
        total[t] = product(t, 3)

    for t in range(PIECES):
        near(t).wait()
        cross(t).wait()
        y_ref[t] = (total[t] + near_in[t].astype(F32) + cross_in[t].astype(F32)).astype(BF16)
    for pair in range(pairs):
        for i in range(2):

            @pl.when((seq != owner_of(pair, i)) & (seq != peers - 1))
            def _():
                send_map(pair, i, seq).wait_send()

            @pl.when(seq == owner_of(pair, i))
            def _():
                for k in range(1, peers):

                    @pl.when(seq != k)
                    def _():
                        send_state(pair, i, k).wait_send()


def fused(queries, keys, values, betas, gate, out_weight, seq_axis, axis):
    tokens, depth = queries.shape
    heads = depth // HEAD_DIM
    peers = lax.axis_size(seq_axis)
    width = out_weight.shape[1] // lax.axis_size(axis)
    blocks = tokens // SPAN
    batch = blocks // 2
    hbm = pl.BlockSpec(memory_space=pltpu.HBM)
    piece = (PIECES, tokens // PIECES, width)
    square = (HEAD_DIM, HEAD_DIM)
    wide = (HEAD_DIM, 2 * HEAD_DIM)
    two = (2,) + square
    pairs = heads // 2
    dma = pltpu.SemaphoreType.DMA
    per_head = (heads, blocks, SPAN, HEAD_DIM)
    both = (heads, 2, blocks, SPAN, HEAD_DIM)
    return pl.pallas_call(
        functools.partial(fused_kernel, seq_axis, peers, axis),
        in_specs=[hbm] * 6,
        out_specs=pl.BlockSpec(memory_space=pltpu.VMEM),
        out_shape=jax.ShapeDtypeStruct((PIECES, tokens // PIECES, width), BF16),
        scratch_shapes=[
            pltpu.VMEM(betas.shape, F32),
            pltpu.VMEM(per_head, BF16),
            pltpu.VMEM(both, BF16),
            pltpu.VMEM(both, BF16),
            pltpu.VMEM(per_head, BF16),
            pltpu.VMEM((blocks, heads, 2 * SPAN), F32),
            pltpu.VMEM((heads, blocks, 3) + square, BF16),
            pltpu.VMEM((2, 2 * batch) + two, BF16),
            pltpu.VMEM((2, 2 * batch) + square, F32),
            pltpu.VMEM((heads,) + wide, F32),
            pltpu.VMEM((heads, blocks) + two, BF16),
            pltpu.VMEM((2, 2 * batch) + two, BF16),
            pltpu.VMEM((2, 2 * batch, BASE, 2 * SPAN), F32),
            pltpu.VMEM((2, 2, 2 * batch, 2 * SPAN), F32),
            pltpu.VMEM(square, F32),
            pltpu.VMEM((heads,) + two, BF16),
            pltpu.VMEM((pairs, peers) + two, BF16),
            pltpu.VMEM(square, F32),
            pltpu.VMEM((pairs, peers) + square, BF16),
            pltpu.VMEM((heads,) + square, BF16),
            pltpu.VMEM(per_head, F32),
            pltpu.VMEM(per_head, BF16),
            pltpu.VMEM((blocks, heads, SPAN, HEAD_DIM), BF16),
            pltpu.VMEM((4, depth, width), BF16),
            pltpu.VMEM(piece, F32),
        ]
        + [pltpu.VMEM(piece, BF16)] * 6
        + [
            dma,
            dma((2, heads)),
            dma((heads,)),
            dma((heads,)),
            dma((4,)),
            dma((heads,)),
            dma((pairs, peers)),
            dma((pairs, peers)),
            dma((heads,)),
        ]
        + [dma((PIECES,))] * 6,
        compiler_params=pltpu.CompilerParams(
            collective_id=0, has_side_effects=True, vmem_limit_bytes=FUSED_LIMIT
        ),
    )(
        queries.reshape(blocks, SPAN, depth),
        keys.reshape(2, blocks, SPAN, depth),
        values.reshape(2, blocks, SPAN, depth),
        betas,
        gate.reshape(blocks, SPAN, depth),
        out_weight,
    ).reshape(tokens, width)


def start_state(maps, axis):
    peers, index = lax.axis_size(axis), lax.axis_index(axis)
    heads = maps.shape[0]
    held = lax.all_gather(maps, axis, axis=0, tiled=True)
    states = pl.pallas_call(
        functools.partial(chain_kernel, peers),
        out_shape=jax.ShapeDtypeStruct((held.shape[0], HEAD_DIM, HEAD_DIM), BF16),
        compiler_params=pltpu.CompilerParams(vmem_limit_bytes=VMEM_LIMIT),
    )(held)
    return lax.dynamic_slice_in_dim(states, index * heads, heads, 0)


def out_kernel(o_ref, m_ref, s_ref, g_ref, w_ref, y_ref, mixed_ref):
    @pl.when(pl.program_id(0) == 0)
    def _():
        for h in range(s_ref.shape[0]):
            cols = slice(h * HEAD_DIM, (h + 1) * HEAD_DIM)
            seen = o_ref[:, cols] + dot(m_ref[:, cols], s_ref[h])
            scale = lax.rsqrt(jnp.mean(seen * seen, axis=1, keepdims=True) + 1e-06)
            gate = g_ref[:, cols].astype(F32)
            mixed_ref[:, cols] = (seen * scale * (gate / (1.0 + jnp.exp(-gate)))).astype(BF16)

    y_ref[...] = dot(mixed_ref[...], w_ref[...]).astype(BF16)


def project(local, reach, states, gate, out_weight):
    tokens, width = local.shape
    total = out_weight.shape[1]
    tile = 512
    whole = pl.BlockSpec((tokens, width), lambda n: (0, 0))
    return pl.pallas_call(
        out_kernel,
        grid=(total // tile,),
        in_specs=[
            whole,
            whole,
            pl.BlockSpec(states.shape, lambda n: (0, 0, 0)),
            whole,
            pl.BlockSpec((width, tile), lambda n: (0, n)),
        ],
        out_specs=pl.BlockSpec((tokens, tile), lambda n: (0, n)),
        out_shape=jax.ShapeDtypeStruct((tokens, total), BF16),
        scratch_shapes=[pltpu.VMEM((tokens, width), BF16)],
        compiler_params=pltpu.CompilerParams(
            dimension_semantics=("arbitrary",), vmem_limit_bytes=VMEM_LIMIT
        ),
    )(local, reach, states, gate, out_weight)


def per_device(queries, keys, values, betas, gate, out_weight):
    heads, _, tokens = betas.shape
    peers, index = lax.axis_size("ctx"), lax.axis_size("head")
    if index == 4 and peers >= 4 and peers % 2 == 0 and heads % 8 == 0 and tokens % (8 * SPAN) == 0:
        return fused(queries, keys, values, betas, gate, out_weight, "ctx", "head")
    beta_cols = betas.transpose(2, 1, 0).reshape(2 * tokens, heads)
    local, reach, maps = mix(queries, keys, values, beta_cols)
    states = start_state(maps, "ctx")
    partial_sum = project(local, reach, states, gate, out_weight)
    return lax.psum_scatter(partial_sum, "head", scatter_dimension=1, tiled=True)


def solution(mesh):
    return jax.shard_map(
        per_device,
        mesh=mesh,
        in_specs=(
            P("ctx", "head"),
            P(None, "ctx", "head"),
            P(None, "ctx", "head"),
            P("head", None, "ctx"),
            P("ctx", "head"),
            P("head", None),
        ),
        out_specs=P("ctx", "head"),
        check_vma=False,
    )
```

```python
import functools

import jax
import jax.numpy as jnp
from jax import lax
from jax.experimental import pallas as pl
from jax.experimental.pallas import tpu as pltpu
from jax.sharding import PartitionSpec as P

HEAD_DIM = 128
SPAN = 64
BASE = 16
F32 = jnp.float32
BF16 = jnp.bfloat16
VMEM_LIMIT = 60 * 1024 * 1024
MESH = pl.DeviceIdType.MESH
PIECES = 4


def iota(shape, dim):
    return lax.broadcasted_iota(jnp.int32, shape, dim)


def split(a):
    high = a.astype(BF16)
    return high, (a - high.astype(F32)).astype(BF16)


def dot(a, b):
    return jnp.dot(a, b, preferred_element_type=F32)


def dot3(a, b):
    ah, al = split(a)
    bh, bl = split(b)
    return dot(jnp.concatenate([ah, al, ah], axis=1), jnp.concatenate([bh, bh, bl], axis=0))


def inverse(lowers, order):
    lane = iota((BASE, order), 1)
    compact = []
    for low in lowers:
        total = jnp.zeros((BASE, order), F32)
        for blk in range(order // BASE):
            total = jnp.where(lane // BASE == blk, low[blk * BASE : (blk + 1) * BASE, :], total)
        compact.append(total)
    inv = [(iota((BASE, order), 0) == lane % BASE).astype(F32) for _ in lowers]
    for j in range(BASE - 1):
        pick = (lane // BASE) * BASE + j
        for n, low in enumerate(compact):
            column = jnp.take_along_axis(low, pick, axis=1, mode="promise_in_bounds")
            inv[n] = inv[n] - column * inv[n][j : j + 1, :]
    row = iota((order, order), 0)
    col = iota((order, order), 1)
    width = BASE
    while width < order:
        corner = (row // (2 * width) == col // (2 * width)) & (row // width != col // width)
        diagonal = row // width == col // width
        second = (iota((width, order), 1) // width) % 2 == 1
        half = [dot3(jnp.where(second, t, 0.0), jnp.where(corner, low, 0.0)) for t, low in zip(inv, lowers)]
        full = [
            jnp.where(diagonal, jnp.concatenate([t] * (order // width), axis=0), 0.0) for t in inv
        ]
        fill = [dot3(y, e) for y, e in zip(half, full)]
        inv = [
            jnp.concatenate([jnp.where(second, 0.0, t), jnp.where(second, t, 0.0) - r], axis=0)
            for t, r in zip(inv, fill)
        ]
        width *= 2
    return inv


def mix_kernel(q_ref, k_ref, v_ref, b_ref, o_ref, m_ref, x_out, x_ref):
    heads = q_ref.shape[1] // HEAD_DIM
    span = q_ref.shape[0]
    order = 2 * span
    step = pl.program_id(0)

    @pl.when(step == 0)
    def _():
        start = (iota((HEAD_DIM, 2 * HEAD_DIM), 0) == iota((HEAD_DIM, 2 * HEAD_DIM), 1)).astype(F32)
        for h in range(heads):
            x_ref[h] = start

    row = iota((order, order), 0)
    col = iota((order, order), 1)
    strict = col < row
    weave = (row == 2 * (col % span) + col // span).astype(BF16)
    causal = iota((span, order), 1) <= 2 * iota((span, order), 0) + 1
    data = []
    lowers = []
    for h in range(heads):
        cols = slice(h * HEAD_DIM, (h + 1) * HEAD_DIM)
        query = q_ref[:, cols]
        pair = jnp.concatenate(
            [
                jnp.concatenate([k_ref[0, :, cols], v_ref[0, :, cols]], axis=1),
                jnp.concatenate([k_ref[1, :, cols], v_ref[1, :, cols]], axis=1),
            ],
            axis=0,
        )
        woven = dot(weave, pair)
        key = woven[:, :HEAD_DIM]
        value = woven[:, HEAD_DIM:]
        key_b = key.astype(BF16)
        norm = lax.rsqrt(jnp.sum(key * key, axis=1, keepdims=True) + 1e-06)
        beta = b_ref[:, h : h + 1]
        both = jnp.concatenate([key_b, query], axis=0)
        gram = lax.dot_general(both, key_b, (((1,), (1,)), ((), ())), preferred_element_type=F32)
        weight = beta * norm * norm
        lowers.append(jnp.where(strict, weight * gram[:order], 0.0))
        scores = jnp.where(causal, gram[order:], 0.0).astype(BF16)
        qf = query.astype(F32)
        q_norm = lax.rsqrt(jnp.sum(qf * qf, axis=1, keepdims=True) + 1e-06)
        readers = jnp.concatenate([key.T.astype(BF16), scores], axis=0)
        data.append((both, readers, beta * norm * value, weight, q_norm))
    solved = inverse(lowers, order)
    seen = []
    for h in range(heads):
        both = data[h][0]
        high, low = split(x_ref[h])
        seen.append(
            dot(jnp.concatenate([both, both], axis=1), jnp.concatenate([high, low], axis=0))
        )
    writes = []
    for h in range(heads):
        _, _, scaled, weight, _ = data[h]
        gap = -weight * seen[h][:order]
        gap = jnp.concatenate([gap[:, :HEAD_DIM], gap[:, HEAD_DIM:] + scaled], axis=1)
        writes.append(dot3(solved[h], gap))
    for h in range(heads):
        cols = slice(h * HEAD_DIM, (h + 1) * HEAD_DIM)
        readers, q_norm = data[h][1], data[h][4]
        high, low = split(writes[h])
        change = dot(
            jnp.concatenate([readers, readers], axis=1), jnp.concatenate([high, low], axis=0)
        )
        x_ref[h] = x_ref[h] + change[:HEAD_DIM]
        out = q_norm * (seen[h][order:] + change[HEAD_DIM:])
        m_ref[:, cols] = out[:, :HEAD_DIM].astype(BF16)
        o_ref[:, cols] = out[:, HEAD_DIM:]

    @pl.when(step == pl.num_programs(0) - 1)
    def _():
        for h in range(heads):
            x_out[h] = x_ref[h].astype(BF16)


def mix(queries, keys, values, beta_cols):
    tokens, width = queries.shape
    heads = width // HEAD_DIM
    return pl.pallas_call(
        mix_kernel,
        grid=(tokens // SPAN,),
        in_specs=[
            pl.BlockSpec((SPAN, width), lambda c: (c, 0)),
            pl.BlockSpec((2, SPAN, width), lambda c: (0, c, 0)),
            pl.BlockSpec((2, SPAN, width), lambda c: (0, c, 0)),
            pl.BlockSpec((2 * SPAN, heads), lambda c: (c, 0)),
        ],
        out_specs=[
            pl.BlockSpec((SPAN, width), lambda c: (c, 0)),
            pl.BlockSpec((SPAN, width), lambda c: (c, 0)),
            pl.BlockSpec((heads, HEAD_DIM, 2 * HEAD_DIM), lambda c: (0, 0, 0)),
        ],
        out_shape=[
            jax.ShapeDtypeStruct((tokens, width), F32),
            jax.ShapeDtypeStruct((tokens, width), BF16),
            jax.ShapeDtypeStruct((heads, HEAD_DIM, 2 * HEAD_DIM), BF16),
        ],
        scratch_shapes=[pltpu.VMEM((heads, HEAD_DIM, 2 * HEAD_DIM), F32)],
        compiler_params=pltpu.CompilerParams(
            dimension_semantics=("arbitrary",), vmem_limit_bytes=VMEM_LIMIT
        ),
    )(queries, keys, values, beta_cols)


def chain_kernel(peers, x_ref, s_ref):
    heads = x_ref.shape[0] // peers
    for h in range(heads):
        state = jnp.zeros((HEAD_DIM, HEAD_DIM), F32)
        for k in range(peers):
            s_ref[k * heads + h] = state.astype(BF16)
            if k < peers - 1:
                maps = x_ref[k * heads + h]
                turn = maps[:, :HEAD_DIM]
                high, low = split(state)
                state = maps[:, HEAD_DIM:].astype(F32) + dot(
                    jnp.concatenate([turn, turn], axis=1), jnp.concatenate([high, low], axis=0)
                )


FUSED_LIMIT = 52 * 1024 * 1024


def dot_t(a, b):
    return lax.dot_general(a, b, (((1,), (1,)), ((), ())), preferred_element_type=F32)


def pair_dot(a, low, high_b, low_b):
    rows = a.shape[0]
    both = dot(jnp.concatenate([a, low], axis=0), jnp.concatenate([high_b, low_b], axis=1))
    width = high_b.shape[1]
    return both[:rows, :width] + both[rows:, :width] + both[:rows, width:]


def weave(*streams):
    order = []
    for n, (count, _, first, last) in enumerate(streams):
        order += [(first + (last - first) * (k + 0.5) / count, n) for k in range(count)]
    for _, n in sorted(order):
        next(streams[n][1], None)
    for _, stream, _, _ in streams:
        for _ in stream:
            pass


def base_solve(lowers, span):
    order = 2 * span
    base = BASE // 2
    lane = iota((base, order), 1)
    group = (lane % span) // base
    row16, lane16 = iota((BASE, order), 0), iota((BASE, order), 1)
    group16 = (lane16 % span) // base
    row_tok, lane_tok = row16 % base, lane16 % base
    before = (lane_tok < row_tok) | ((lane_tok == row_tok) & (lane16 // span < row16 // base))
    compact = []
    for n, low in enumerate(lowers):
        halves = []
        for j in range(2):
            total = jnp.zeros((base, order), F32)
            for blk in range(span // base):
                start = j * span + blk * base
                total = jnp.where(group == blk, low[start : start + base, :], total)
            halves.append(total)
        compact.append(jnp.where(before, jnp.concatenate(halves, axis=0), 0.0))
        if n % 2:
            yield
    own = (row16 % base == lane16 % base) & (row16 // base == lane16 // span)
    inv = [own.astype(F32) for _ in lowers]
    for s in range(BASE - 1):
        t, j = s // 2, s % 2
        pick = j * span + group16 * base + t
        for n, low in enumerate(compact):
            column = jnp.take_along_axis(low, pick, axis=1, mode="promise_in_bounds")
            inv[n] = inv[n] - column * inv[n][j * base + t : j * base + t + 1, :]
        yield
    return inv


def merge(inv, pieces, span):
    order = 2 * span
    tok_r = iota((order, order), 0) % span
    tok_c = iota((order, order), 1) % span
    width = BASE // 2
    zero = jnp.zeros((), BF16)
    while width < span:
        last = 2 * width == span
        diagonal = tok_r // width == tok_c // width
        corner = (tok_r // (2 * width) == tok_c // (2 * width)) & (tok_r // width != tok_c // width)
        second = ((iota((2 * width, order), 1) % span) // width) % 2 == 1
        odd, half, fill, wide, merged = [], [], [], [], []
        for n, t in enumerate(inv):
            odd.append(jnp.where(second, t, 0.0))
            th, tl = split(odd[n])
            high, low = pieces(n)
            if last:
                y = jnp.where(second, 0.0, pair_dot(th, tl, high, low))
            else:
                y = pair_dot(th, tl, jnp.where(corner, high, zero), jnp.where(corner, low, zero))
            half.append(y)
            parts = []
            for j in range(2):
                part = t[j * width : (j + 1) * width]
                if width < 16:
                    part = jnp.concatenate([part] * (16 // width), axis=0)
                parts.append((split(part), span // part.shape[0]))
            full = [
                jnp.concatenate([p[k] for p, count in parts for _ in range(count)], axis=0)
                for k in range(2)
            ]
            if not last:
                full = [jnp.where(diagonal, f, zero) for f in full]
            wide.append(full)
            yield
        for y, full in zip(half, wide):
            yh, yl = split(y)
            r = pair_dot(yh, yl, full[0], full[1])
            fill.append(jnp.where(second, 0.0, r) if last else r)
            yield
        for t, o, r in zip(inv, odd, fill):
            even, lower = t - o, o - r
            merged.append(
                jnp.concatenate(
                    [even[:width], lower[:width], even[width:], lower[width:]], axis=0
                )
            )
        inv = merged
        width *= 2
    return inv


def fused_kernel(
    seq_axis, peers, axis, q_hbm, k_hbm, v_hbm, b_hbm, g_hbm, w_hbm, y_ref,
    b_ref, q_ref, k_ref, v_ref, g_ref, beta_ref, stack_ref, turn_ref, source_ref, x_ref, start_ref,
    low_ref, inv_ref, weight_ref, eye_ref,
    maps, held, carry_ref, states, s_ref, o_ref, m_ref,
    mixed, weight, total, far_out, far_in, near_out, near_in, cross_out, cross_in,
    b_sem, kv_sem, q_sem, g_sem, load_sem, map_send, map_recv, back_send, back_recv,
    far_send, far_recv, near_send, near_recv, cross_send, cross_recv,
):
    heads, blocks, span = q_ref.shape[0], q_ref.shape[1], q_ref.shape[2]
    pairs = heads // 2
    parts = 2
    batch = blocks // parts
    seq = lax.axis_index(seq_axis)
    me = lax.axis_index(axis)
    chip, core = me // 2, me % 2
    sibling = 2 * chip + 1 - core
    across = 2 * (1 - chip) + core
    beyond = 2 * (1 - chip) + 1 - core
    width = y_ref.shape[2]

    def columns(h):
        return pl.ds(pl.multiple_of(h * HEAD_DIM, HEAD_DIM), HEAD_DIM)

    def fetch_kv(h):
        return (
            pltpu.make_async_copy(k_hbm.at[:, :, :, columns(h)], k_ref.at[h], kv_sem.at[0, h]),
            pltpu.make_async_copy(v_hbm.at[:, :, :, columns(h)], v_ref.at[h], kv_sem.at[1, h]),
        )

    def fetch_q(h):
        return pltpu.make_async_copy(q_hbm.at[:, :, columns(h)], q_ref.at[h], q_sem.at[h])

    def fetch_g(h):
        return pltpu.make_async_copy(g_hbm.at[:, :, columns(h)], g_ref.at[h], g_sem.at[h])

    def load(n):
        owner = (beyond, across, sibling, me)[n]
        return pltpu.make_async_copy(
            w_hbm.at[:, pl.ds(pl.multiple_of(owner * width, width), width)],
            weight.at[n],
            load_sem.at[n],
        )

    def start_kv(first, last):
        for h in range(first, last):
            for copy in fetch_kv(h):
                copy.start()

    fetch_b = pltpu.make_async_copy(b_hbm, b_ref, b_sem)
    fetch_b.start()
    start_kv(0, 2)
    barrier = pltpu.get_barrier_semaphore()
    for other in (sibling, across):
        pl.semaphore_signal(barrier, inc=1, device_id={axis: other}, device_id_type=MESH)
    for away in range(1, peers):
        pl.semaphore_signal(
            barrier,
            inc=1,
            device_id={seq_axis: lax.rem(seq + away, peers)},
            device_id_type=MESH,
        )

    begin = (iota((HEAD_DIM, 2 * HEAD_DIM), 0) == iota((HEAD_DIM, 2 * HEAD_DIM), 1)).astype(F32)
    for h in range(heads):
        x_ref[h] = begin
    eye_ref[...] = (iota(eye_ref.shape, 0) == iota(eye_ref.shape, 1)).astype(F32)
    fetch_b.wait()
    for blk in range(blocks):
        window = slice(blk * span, (blk + 1) * span)
        beta_ref[blk] = jnp.concatenate([b_ref[:, 0, window], b_ref[:, 1, window]], axis=1)

    def place(it, n):
        pair, part = it
        return 2 * pair + n % 2, part * batch + n // 2

    count = 2 * batch

    def key_of(h, blk):
        return jnp.concatenate([k_ref[h, 0, blk], k_ref[h, 1, blk]], axis=0)

    def stack_of(h, blk):
        none = jnp.zeros((HEAD_DIM, HEAD_DIM), BF16)
        return jnp.concatenate(
            [
                jnp.concatenate([stack_ref[h, blk, 0], stack_ref[h, blk, 2]], axis=1),
                jnp.concatenate([stack_ref[h, blk, 1], none], axis=1),
            ],
            axis=0,
        )

    def solve(it):
        slot = it[1]
        grams, squares = [], []
        for n in range(count):
            key = key_of(*place(it, n))
            grams.append(dot_t(key, key))
            if n % 2:
                yield
        for n, g in enumerate(grams):
            squares.append(jnp.sum(eye_ref[...] * g, axis=0, keepdims=True))
            if n % 4 == 3:
                yield
        beta = jnp.concatenate(
            [beta_ref[place(it, n)[1], pl.ds(place(it, n)[0], 1), :] for n in range(count)], axis=0
        )
        norm = lax.rsqrt(jnp.concatenate(squares, axis=0) + 1e-06)
        value_weight = beta * norm
        weight_rows = value_weight * norm
        weight_ref[slot, 0] = weight_rows
        weight_ref[slot, 1] = value_weight
        weight_cols = weight_rows.T
        yield
        lowers = []
        for n, g in enumerate(grams):
            low = weight_cols[:, n : n + 1] * g
            lowers.append(low)
            low_ref[slot, n, 0], low_ref[slot, n, 1] = split(low)
            if n % 2:
                yield
        inv = yield from base_solve(lowers, span)
        for n in range(count):
            inv_ref[slot, n] = inv[n]

    def transit(it):
        slot = it[1]

        def pieces(n):
            return low_ref[slot, n, 0], low_ref[slot, n, 1]

        solved = yield from merge([inv_ref[slot, n] for n in range(count)], pieces, span)
        turns, writes, changes = [], [], []
        for n in range(count):
            h, blk = place(it, n)
            th, tl = split(solved[n] * weight_ref[slot, 0, n : n + 1, :])
            tv = (solved[n] * weight_ref[slot, 1, n : n + 1, :]).astype(BF16)
            key = key_of(h, blk)
            value = jnp.concatenate([v_ref[h, 0, blk], v_ref[h, 1, blk]], axis=0)
            turns.append(
                dot(jnp.concatenate([th, tl], axis=1), jnp.concatenate([key, key], axis=0))
            )
            writes.append(dot(tv, value))
            yield
        for n in range(count):
            h, blk = place(it, n)
            turn_h, turn_l = split(turns[n])
            stack_ref[h, blk, 0], stack_ref[h, blk, 1] = turn_h, turn_l
            stack_ref[h, blk, 2] = writes[n].astype(BF16)
            stack = stack_of(h, blk)
            key_t = key_of(h, blk).T
            changes.append(dot(jnp.concatenate([key_t, key_t], axis=1), stack))
            yield
        for n in range(count):
            step = eye_ref[...] - changes[n][:, :HEAD_DIM]
            turn_ref[slot, n, 0], turn_ref[slot, n, 1] = split(step)
            source_ref[slot, n] = changes[n][:, HEAD_DIM:]
            yield

    def compose(it):
        slot = it[1]
        pair, _ = it
        states_now = [x_ref[2 * pair + i] for i in range(2)]
        for n in range(count):
            h, blk = place(it, n)
            i = n % 2
            high, low = split(states_now[i])
            start_ref[h, blk, 0] = high[:, :HEAD_DIM]
            start_ref[h, blk, 1] = high[:, HEAD_DIM:]
            turn_h, turn_l = turn_ref[slot, n, 0], turn_ref[slot, n, 1]
            moved = dot(
                jnp.concatenate([turn_h, turn_l, turn_h], axis=1),
                jnp.concatenate([high, high, low], axis=0),
            )
            states_now[i] = jnp.concatenate(
                [moved[:, :HEAD_DIM], moved[:, HEAD_DIM:] + source_ref[slot, n]], axis=1
            )
            if n >= count - 2:
                x_ref[h] = states_now[i]
            yield

    def a_stream(it, first=0.0, last=1.0):
        return 7 * count // 4 + BASE + 1, solve(it), first, last

    def b_stream(it, first=0.0, last=1.0):
        return 9 * count, transit(it), first, last

    def c_stream(it, first=0.0, last=1.0):
        return count, compose(it), first, last

    def owner_of(pair, i):
        side = lax.rem(pair + core, 2)
        return peers // 2 - 2 + side + i * (3 - 2 * side)

    def send_map(pair, i, source):
        h = 2 * pair + i
        return pltpu.make_async_remote_copy(
            src_ref=maps.at[h],
            dst_ref=held.at[pair, source],
            send_sem=map_send.at[h],
            recv_sem=map_recv.at[pair, source],
            device_id={seq_axis: owner_of(pair, i)},
            device_id_type=MESH,
        )

    def send_state(pair, i, target):
        h = 2 * pair + i
        return pltpu.make_async_remote_copy(
            src_ref=states.at[pair, target],
            dst_ref=s_ref.at[h],
            send_sem=back_send.at[pair, target],
            recv_sem=back_recv.at[h],
            device_id={seq_axis: target},
            device_id_type=MESH,
        )

    def post(pair):
        for i in range(2):
            h = 2 * pair + i
            maps[h, 0] = x_ref[h, :, :HEAD_DIM].astype(BF16)
            maps[h, 1] = x_ref[h, :, HEAD_DIM:].astype(BF16)

            @pl.when((seq != owner_of(pair, i)) & (seq != peers - 1))
            def _():
                send_map(pair, i, seq).start()

            @pl.when(seq == owner_of(pair, i))
            def _():
                held[pair, seq] = maps[h]

    def chain(pair):
        for i in range(2):

            @pl.when(seq == owner_of(pair, i))
            def _():
                carry_ref[...] = jnp.zeros((HEAD_DIM, HEAD_DIM), F32)
                for k in range(peers - 1):

                    @pl.when(seq != k)
                    def _():
                        send_map(pair, i, k).wait_recv()

                    high, low = split(carry_ref[...])
                    turn = held[pair, k, 0]
                    state = held[pair, k, 1].astype(F32) + dot(
                        jnp.concatenate([turn, turn], axis=1),
                        jnp.concatenate([high, low], axis=0),
                    )
                    carry_ref[...] = state
                    states[pair, k + 1] = state.astype(BF16)

                    @pl.when(seq != k + 1)
                    def _():
                        send_state(pair, i, k + 1).start()

                    @pl.when(seq == k + 1)
                    def _():
                        s_ref[2 * pair + i] = states[pair, k + 1]

    @pl.when(seq == 0)
    def _():
        s_ref[...] = jnp.zeros(s_ref.shape, BF16)

    def wait_kv(pair):
        for i in range(2):
            for copy in fetch_kv(2 * pair + i):
                copy.wait()

    wait_kv(0)
    start_kv(2, heads)
    for h in range(heads):
        fetch_q(h).start()
    for n in range(4):
        load(n).start()
    for h in range(heads):
        fetch_g(h).start()
    weave(
        a_stream((0, 0), 0.0, 1.0),
        a_stream((0, 1), 0.5, 2.0),
        b_stream((0, 0), 1.1, 2.1),
    )

    def step(pair, _):
        wait_kv(pair)
        weave(
            a_stream((pair, 0), 0.0, 1.0),
            b_stream((pair - 1, 1), 0.0, 1.0),
            c_stream((pair - 1, 0), 0.0, 1.0),
            a_stream((pair, 1), 1.05, 2.0),
            b_stream((pair, 0), 1.05, 2.0),
            c_stream((pair - 1, 1), 1.05, 2.0),
        )

        @pl.when(pair == 1)
        def _():
            pl.semaphore_wait(barrier, peers + 1)

        post(pair - 1)
        return 0

    lax.fori_loop(1, pairs, step, 0)
    chain(0)
    weave(
        b_stream((pairs - 1, 1), 0.0, 9.0),
        c_stream((pairs - 1, 0), 0.0, 6.0),
        c_stream((pairs - 1, 1), 8.1, 9.1),
    )
    post(pairs - 1)
    for h in range(heads):
        fetch_q(h).wait()

    def read(pair, _):
        causal = iota((span, 2 * span), 1) % span <= iota((span, 2 * span), 0)
        for i in range(2):
            h = 2 * pair + i
            scores = []
            for blk in range(blocks):
                found = jnp.where(causal, dot_t(q_ref[h, blk], key_of(h, blk)), 0.0).astype(BF16)
                scores.append(jnp.concatenate([found, found], axis=1))
            drawn = [dot(score, stack_of(h, blk)) for blk, score in enumerate(scores)]
            for blk in range(blocks):
                kept = (q_ref[h, blk].astype(F32) - drawn[blk][:, :HEAD_DIM]).astype(BF16)
                out = dot(kept, jnp.concatenate([start_ref[h, blk, 0], start_ref[h, blk, 1]], axis=1))
                m_ref[h, blk] = out[:, :HEAD_DIM].astype(BF16)
                o_ref[h, blk] = out[:, HEAD_DIM:] + drawn[blk][:, HEAD_DIM:]

        return 0

    chain(1)
    lax.fori_loop(0, pairs, read, 0)
    for h in range(heads):
        fetch_g(h).wait()

    def wait_state(pair):
        for i in range(2):

            @pl.when((seq != owner_of(pair, i)) & (seq != 0))
            def _():
                send_state(pair, i, seq).wait_recv()

    def blend(pair, t):
        for i in range(2):
            h = 2 * pair + i
            query = q_ref[h, t].astype(F32)
            unit = lax.rsqrt(jnp.sum(query * query, axis=1, keepdims=True) + 1e-06)
            seen = unit * (o_ref[h, t] + dot(m_ref[h, t], s_ref[h]))
            scale = lax.rsqrt(jnp.mean(seen * seen, axis=1, keepdims=True) + 1e-06)
            gate = g_ref[h, t].astype(F32)
            mixed[t, h] = (seen * scale * (gate / (1.0 + jnp.exp(-gate)))).astype(BF16)

    def blend_pair(pair):
        wait_state(pair)
        for blk in range(blocks):
            blend(pair, blk)

    def settle(pair, _):
        chain(pair + 2)
        blend_pair(pair)
        return 0

    lax.fori_loop(0, pairs - 2, settle, 0)
    blend_pair(pairs - 2)

    def send(source, target, send_sem, recv_sem, t, device):
        return pltpu.make_async_remote_copy(
            src_ref=source.at[t],
            dst_ref=target.at[t],
            send_sem=send_sem.at[t],
            recv_sem=recv_sem.at[t],
            device_id={axis: device},
            device_id_type=MESH,
        )

    def far(t):
        return send(far_out, far_in, far_send, far_recv, t, sibling)

    def near(t):
        return send(near_out, near_in, near_send, near_recv, t, sibling)

    def cross(t):
        return send(cross_out, cross_in, cross_send, cross_recv, t, across)

    def pass_on(t):
        far(t).wait()
        cross_out[t] = (total[t] + far_in[t].astype(F32)).astype(BF16)
        cross(t).start()

    share = blocks // PIECES

    def rows_of(t, first, last):
        return jnp.concatenate(
            [
                jnp.concatenate([mixed[t * share + b, h] for h in range(first, last)], axis=1)
                for b in range(share)
            ],
            axis=0,
        )

    def product(t, n):
        return dot(rows_of(t, 0, heads), weight[n])

    def finish_piece(t):
        for b in range(share):
            blend(pairs - 1, t * share + b)

    early = (heads - 2) * HEAD_DIM
    load(0).wait()
    total[0] = dot(rows_of(0, 0, heads - 2), weight[0, :early, :])
    wait_state(pairs - 1)
    finish_piece(0)
    far_out[0] = (total[0] + dot(rows_of(0, heads - 2, heads), weight[0, early:, :])).astype(BF16)
    far(0).start()
    load(1).wait()
    total[0] = product(0, 1)
    for t in range(1, PIECES):
        finish_piece(t)
        far_out[t] = product(t, 0).astype(BF16)
        far(t).start()
        if t > 1:
            total[t] = product(t, 1)
        pass_on(t - 1)
        if t == 1:
            total[t] = product(t, 1)
    load(2).wait()
    for t in range(PIECES):
        near_out[t] = product(t, 2).astype(BF16)
        near(t).start()
        if t == 0:
            pass_on(PIECES - 1)
    load(3).wait()
    for t in range(PIECES):
        total[t] = product(t, 3)

    for t in range(PIECES):
        near(t).wait()
        cross(t).wait()
        y_ref[t] = (total[t] + near_in[t].astype(F32) + cross_in[t].astype(F32)).astype(BF16)
    for pair in range(pairs):
        for i in range(2):

            @pl.when((seq != owner_of(pair, i)) & (seq != peers - 1))
            def _():
                send_map(pair, i, seq).wait_send()

            @pl.when(seq == owner_of(pair, i))
            def _():
                for k in range(1, peers):

                    @pl.when(seq != k)
                    def _():
                        send_state(pair, i, k).wait_send()


def fused(queries, keys, values, betas, gate, out_weight, seq_axis, axis):
    tokens, depth = queries.shape
    heads = depth // HEAD_DIM
    peers = lax.axis_size(seq_axis)
    width = out_weight.shape[1] // lax.axis_size(axis)
    blocks = tokens // SPAN
    batch = blocks // 2
    hbm = pl.BlockSpec(memory_space=pltpu.HBM)
    piece = (PIECES, tokens // PIECES, width)
    square = (HEAD_DIM, HEAD_DIM)
    wide = (HEAD_DIM, 2 * HEAD_DIM)
    two = (2,) + square
    pairs = heads // 2
    dma = pltpu.SemaphoreType.DMA
    per_head = (heads, blocks, SPAN, HEAD_DIM)
    both = (heads, 2, blocks, SPAN, HEAD_DIM)
    return pl.pallas_call(
        functools.partial(fused_kernel, seq_axis, peers, axis),
        in_specs=[hbm] * 6,
        out_specs=pl.BlockSpec(memory_space=pltpu.VMEM),
        out_shape=jax.ShapeDtypeStruct(piece, BF16),
        scratch_shapes=[
            pltpu.VMEM(betas.shape, F32),
            pltpu.VMEM(per_head, BF16),
            pltpu.VMEM(both, BF16),
            pltpu.VMEM(both, BF16),
            pltpu.VMEM(per_head, BF16),
            pltpu.VMEM((blocks, heads, 2 * SPAN), F32),
            pltpu.VMEM((heads, blocks, 3) + square, BF16),
            pltpu.VMEM((2, 2 * batch) + two, BF16),
            pltpu.VMEM((2, 2 * batch) + square, F32),
            pltpu.VMEM((heads,) + wide, F32),
            pltpu.VMEM((heads, blocks) + two, BF16),
            pltpu.VMEM((2, 2 * batch) + two, BF16),
            pltpu.VMEM((2, 2 * batch, BASE, 2 * SPAN), F32),
            pltpu.VMEM((2, 2, 2 * batch, 2 * SPAN), F32),
            pltpu.VMEM(square, F32),
            pltpu.VMEM((heads,) + two, BF16),
            pltpu.VMEM((pairs, peers) + two, BF16),
            pltpu.VMEM(square, F32),
            pltpu.VMEM((pairs, peers) + square, BF16),
            pltpu.VMEM((heads,) + square, BF16),
            pltpu.VMEM(per_head, F32),
            pltpu.VMEM(per_head, BF16),
            pltpu.VMEM((blocks, heads, SPAN, HEAD_DIM), BF16),
            pltpu.VMEM((4, depth, width), BF16),
            pltpu.VMEM(piece, F32),
        ]
        + [pltpu.VMEM(piece, BF16)] * 6
        + [
            dma,
            dma((2, heads)),
            dma((heads,)),
            dma((heads,)),
            dma((4,)),
            dma((heads,)),
            dma((pairs, peers)),
            dma((pairs, peers)),
            dma((heads,)),
        ]
        + [dma((PIECES,))] * 6,
        compiler_params=pltpu.CompilerParams(
            collective_id=0, has_side_effects=True, vmem_limit_bytes=FUSED_LIMIT
        ),
    )(
        queries.reshape(blocks, SPAN, depth),
        keys.reshape(2, blocks, SPAN, depth),
        values.reshape(2, blocks, SPAN, depth),
        betas,
        gate.reshape(blocks, SPAN, depth),
        out_weight,
    ).reshape(tokens, width)


def start_state(maps, axis):
    peers, index = lax.axis_size(axis), lax.axis_index(axis)
    heads = maps.shape[0]
    held = lax.all_gather(maps, axis, axis=0, tiled=True)
    states = pl.pallas_call(
        functools.partial(chain_kernel, peers),
        out_shape=jax.ShapeDtypeStruct((held.shape[0], HEAD_DIM, HEAD_DIM), BF16),
        compiler_params=pltpu.CompilerParams(vmem_limit_bytes=VMEM_LIMIT),
    )(held)
    return lax.dynamic_slice_in_dim(states, index * heads, heads, 0)


def out_kernel(o_ref, m_ref, s_ref, g_ref, w_ref, y_ref, mixed_ref):
    @pl.when(pl.program_id(0) == 0)
    def _():
        for h in range(s_ref.shape[0]):
            cols = slice(h * HEAD_DIM, (h + 1) * HEAD_DIM)
            seen = o_ref[:, cols] + dot(m_ref[:, cols], s_ref[h])
            scale = lax.rsqrt(jnp.mean(seen * seen, axis=1, keepdims=True) + 1e-06)
            gate = g_ref[:, cols].astype(F32)
            mixed_ref[:, cols] = (seen * scale * (gate / (1.0 + jnp.exp(-gate)))).astype(BF16)

    y_ref[...] = dot(mixed_ref[...], w_ref[...]).astype(BF16)


def project(local, reach, states, gate, out_weight):
    tokens, width = local.shape
    total = out_weight.shape[1]
    tile = 512
    whole = pl.BlockSpec((tokens, width), lambda n: (0, 0))
    return pl.pallas_call(
        out_kernel,
        grid=(total // tile,),
        in_specs=[
            whole,
            whole,
            pl.BlockSpec(states.shape, lambda n: (0, 0, 0)),
            whole,
            pl.BlockSpec((width, tile), lambda n: (0, n)),
        ],
        out_specs=pl.BlockSpec((tokens, tile), lambda n: (0, n)),
        out_shape=jax.ShapeDtypeStruct((tokens, total), BF16),
        scratch_shapes=[pltpu.VMEM((tokens, width), BF16)],
        compiler_params=pltpu.CompilerParams(
            dimension_semantics=("arbitrary",), vmem_limit_bytes=VMEM_LIMIT
        ),
    )(local, reach, states, gate, out_weight)


def per_device(queries, keys, values, betas, gate, out_weight):
    heads, _, tokens = betas.shape
    peers, index = lax.axis_size("ctx"), lax.axis_size("head")
    if index == 4 and peers >= 4 and peers % 2 == 0 and heads % 8 == 0 and tokens % (8 * SPAN) == 0:
        return fused(queries, keys, values, betas, gate, out_weight, "ctx", "head")
    beta_cols = betas.transpose(2, 1, 0).reshape(2 * tokens, heads)
    local, reach, maps = mix(queries, keys, values, beta_cols)
    states = start_state(maps, "ctx")
    partial_sum = project(local, reach, states, gate, out_weight)
    return lax.psum_scatter(partial_sum, "head", scatter_dimension=1, tiled=True)


def solution(mesh):
    return jax.shard_map(
        per_device,
        mesh=mesh,
        in_specs=(
            P("ctx", "head"),
            P(None, "ctx", "head"),
            P(None, "ctx", "head"),
            P("head", None, "ctx"),
            P("ctx", "head"),
            P("head", None),
        ),
        out_specs=P("ctx", "head"),
        check_vma=False,
    )
```

```python
import functools

import jax
import jax.numpy as jnp
from jax import lax
from jax.experimental import pallas as pl
from jax.experimental.pallas import tpu as pltpu
from jax.sharding import PartitionSpec as P

HEAD_DIM = 128
SPAN = 64
BASE = 16
F32 = jnp.float32
BF16 = jnp.bfloat16
VMEM_LIMIT = 60 * 1024 * 1024
MESH = pl.DeviceIdType.MESH
PIECES = 4


def iota(shape, dim):
    return lax.broadcasted_iota(jnp.int32, shape, dim)


def split(a):
    high = a.astype(BF16)
    return high, (a - high.astype(F32)).astype(BF16)


def dot(a, b):
    return jnp.dot(a, b, preferred_element_type=F32)


def dot3(a, b):
    ah, al = split(a)
    bh, bl = split(b)
    return dot(jnp.concatenate([ah, al, ah], axis=1), jnp.concatenate([bh, bh, bl], axis=0))


def inverse(lowers, order):
    lane = iota((BASE, order), 1)
    compact = []
    for low in lowers:
        total = jnp.zeros((BASE, order), F32)
        for blk in range(order // BASE):
            total = jnp.where(lane // BASE == blk, low[blk * BASE : (blk + 1) * BASE, :], total)
        compact.append(total)
    inv = [(iota((BASE, order), 0) == lane % BASE).astype(F32) for _ in lowers]
    for j in range(BASE - 1):
        pick = (lane // BASE) * BASE + j
        for n, low in enumerate(compact):
            column = jnp.take_along_axis(low, pick, axis=1, mode="promise_in_bounds")
            inv[n] = inv[n] - column * inv[n][j : j + 1, :]
    row = iota((order, order), 0)
    col = iota((order, order), 1)
    width = BASE
    while width < order:
        corner = (row // (2 * width) == col // (2 * width)) & (row // width != col // width)
        diagonal = row // width == col // width
        second = (iota((width, order), 1) // width) % 2 == 1
        half = [dot3(jnp.where(second, t, 0.0), jnp.where(corner, low, 0.0)) for t, low in zip(inv, lowers)]
        full = [
            jnp.where(diagonal, jnp.concatenate([t] * (order // width), axis=0), 0.0) for t in inv
        ]
        fill = [dot3(y, e) for y, e in zip(half, full)]
        inv = [
            jnp.concatenate([jnp.where(second, 0.0, t), jnp.where(second, t, 0.0) - r], axis=0)
            for t, r in zip(inv, fill)
        ]
        width *= 2
    return inv


def mix_kernel(q_ref, k_ref, v_ref, b_ref, o_ref, m_ref, x_out, x_ref):
    heads = q_ref.shape[1] // HEAD_DIM
    span = q_ref.shape[0]
    order = 2 * span
    step = pl.program_id(0)

    @pl.when(step == 0)
    def _():
        start = (iota((HEAD_DIM, 2 * HEAD_DIM), 0) == iota((HEAD_DIM, 2 * HEAD_DIM), 1)).astype(F32)
        for h in range(heads):
            x_ref[h] = start

    row = iota((order, order), 0)
    col = iota((order, order), 1)
    strict = col < row
    weave = (row == 2 * (col % span) + col // span).astype(BF16)
    causal = iota((span, order), 1) <= 2 * iota((span, order), 0) + 1
    data = []
    lowers = []
    for h in range(heads):
        cols = slice(h * HEAD_DIM, (h + 1) * HEAD_DIM)
        query = q_ref[:, cols]
        pair = jnp.concatenate(
            [
                jnp.concatenate([k_ref[0, :, cols], v_ref[0, :, cols]], axis=1),
                jnp.concatenate([k_ref[1, :, cols], v_ref[1, :, cols]], axis=1),
            ],
            axis=0,
        )
        woven = dot(weave, pair)
        key = woven[:, :HEAD_DIM]
        value = woven[:, HEAD_DIM:]
        key_b = key.astype(BF16)
        norm = lax.rsqrt(jnp.sum(key * key, axis=1, keepdims=True) + 1e-06)
        beta = b_ref[:, h : h + 1]
        both = jnp.concatenate([key_b, query], axis=0)
        gram = lax.dot_general(both, key_b, (((1,), (1,)), ((), ())), preferred_element_type=F32)
        weight = beta * norm * norm
        lowers.append(jnp.where(strict, weight * gram[:order], 0.0))
        scores = jnp.where(causal, gram[order:], 0.0).astype(BF16)
        qf = query.astype(F32)
        q_norm = lax.rsqrt(jnp.sum(qf * qf, axis=1, keepdims=True) + 1e-06)
        readers = jnp.concatenate([key.T.astype(BF16), scores], axis=0)
        data.append((both, readers, beta * norm * value, weight, q_norm))
    solved = inverse(lowers, order)
    seen = []
    for h in range(heads):
        both = data[h][0]
        high, low = split(x_ref[h])
        seen.append(
            dot(jnp.concatenate([both, both], axis=1), jnp.concatenate([high, low], axis=0))
        )
    writes = []
    for h in range(heads):
        _, _, scaled, weight, _ = data[h]
        gap = -weight * seen[h][:order]
        gap = jnp.concatenate([gap[:, :HEAD_DIM], gap[:, HEAD_DIM:] + scaled], axis=1)
        writes.append(dot3(solved[h], gap))
    for h in range(heads):
        cols = slice(h * HEAD_DIM, (h + 1) * HEAD_DIM)
        readers, q_norm = data[h][1], data[h][4]
        high, low = split(writes[h])
        change = dot(
            jnp.concatenate([readers, readers], axis=1), jnp.concatenate([high, low], axis=0)
        )
        x_ref[h] = x_ref[h] + change[:HEAD_DIM]
        out = q_norm * (seen[h][order:] + change[HEAD_DIM:])
        m_ref[:, cols] = out[:, :HEAD_DIM].astype(BF16)
        o_ref[:, cols] = out[:, HEAD_DIM:]

    @pl.when(step == pl.num_programs(0) - 1)
    def _():
        for h in range(heads):
            x_out[h] = x_ref[h].astype(BF16)


def mix(queries, keys, values, beta_cols):
    tokens, width = queries.shape
    heads = width // HEAD_DIM
    return pl.pallas_call(
        mix_kernel,
        grid=(tokens // SPAN,),
        in_specs=[
            pl.BlockSpec((SPAN, width), lambda c: (c, 0)),
            pl.BlockSpec((2, SPAN, width), lambda c: (0, c, 0)),
            pl.BlockSpec((2, SPAN, width), lambda c: (0, c, 0)),
            pl.BlockSpec((2 * SPAN, heads), lambda c: (c, 0)),
        ],
        out_specs=[
            pl.BlockSpec((SPAN, width), lambda c: (c, 0)),
            pl.BlockSpec((SPAN, width), lambda c: (c, 0)),
            pl.BlockSpec((heads, HEAD_DIM, 2 * HEAD_DIM), lambda c: (0, 0, 0)),
        ],
        out_shape=[
            jax.ShapeDtypeStruct((tokens, width), F32),
            jax.ShapeDtypeStruct((tokens, width), BF16),
            jax.ShapeDtypeStruct((heads, HEAD_DIM, 2 * HEAD_DIM), BF16),
        ],
        scratch_shapes=[pltpu.VMEM((heads, HEAD_DIM, 2 * HEAD_DIM), F32)],
        compiler_params=pltpu.CompilerParams(
            dimension_semantics=("arbitrary",), vmem_limit_bytes=VMEM_LIMIT
        ),
    )(queries, keys, values, beta_cols)


def chain_kernel(peers, x_ref, s_ref):
    heads = x_ref.shape[0] // peers
    for h in range(heads):
        state = jnp.zeros((HEAD_DIM, HEAD_DIM), F32)
        for k in range(peers):
            s_ref[k * heads + h] = state.astype(BF16)
            if k < peers - 1:
                maps = x_ref[k * heads + h]
                turn = maps[:, :HEAD_DIM]
                high, low = split(state)
                state = maps[:, HEAD_DIM:].astype(F32) + dot(
                    jnp.concatenate([turn, turn], axis=1), jnp.concatenate([high, low], axis=0)
                )


FUSED_LIMIT = 52 * 1024 * 1024


def dot_t(a, b):
    return lax.dot_general(a, b, (((1,), (1,)), ((), ())), preferred_element_type=F32)


def pair_dot(a, low, high_b, low_b):
    rows = a.shape[0]
    both = dot(jnp.concatenate([a, low], axis=0), jnp.concatenate([high_b, low_b], axis=1))
    width = high_b.shape[1]
    return both[:rows, :width] + both[rows:, :width] + both[:rows, width:]


def weave(*streams):
    order = []
    for n, (count, _, first, last) in enumerate(streams):
        order += [(first + (last - first) * (k + 0.5) / count, n) for k in range(count)]
    for _, n in sorted(order):
        next(streams[n][1], None)
    for _, stream, _, _ in streams:
        for _ in stream:
            pass


def base_solve(lowers, span):
    order = 2 * span
    base = BASE // 2
    lane = iota((base, order), 1)
    group = (lane % span) // base
    row16, lane16 = iota((BASE, order), 0), iota((BASE, order), 1)
    group16 = (lane16 % span) // base
    row_tok, lane_tok = row16 % base, lane16 % base
    before = (lane_tok < row_tok) | ((lane_tok == row_tok) & (lane16 // span < row16 // base))
    compact = []
    for n, low in enumerate(lowers):
        halves = []
        for j in range(2):
            total = jnp.zeros((base, order), F32)
            for blk in range(span // base):
                start = j * span + blk * base
                total = jnp.where(group == blk, low[start : start + base, :], total)
            halves.append(total)
        compact.append(jnp.where(before, jnp.concatenate(halves, axis=0), 0.0))
        if n % 2:
            yield
    own = (row16 % base == lane16 % base) & (row16 // base == lane16 // span)
    inv = [own.astype(F32) for _ in lowers]
    for s in range(BASE - 1):
        t, j = s // 2, s % 2
        pick = j * span + group16 * base + t
        for n, low in enumerate(compact):
            column = jnp.take_along_axis(low, pick, axis=1, mode="promise_in_bounds")
            inv[n] = inv[n] - column * inv[n][j * base + t : j * base + t + 1, :]
        yield
    return inv


def merge(inv, pieces, span):
    order = 2 * span
    tok_r = iota((order, order), 0) % span
    tok_c = iota((order, order), 1) % span
    width = BASE // 2
    zero = jnp.zeros((), BF16)
    while width < span:
        last = 2 * width == span
        diagonal = tok_r // width == tok_c // width
        corner = (tok_r // (2 * width) == tok_c // (2 * width)) & (tok_r // width != tok_c // width)
        second = ((iota((2 * width, order), 1) % span) // width) % 2 == 1
        odd, half, fill, wide, merged = [], [], [], [], []
        for n, t in enumerate(inv):
            odd.append(jnp.where(second, t, 0.0))
            th, tl = split(odd[n])
            high, low = pieces(n)
            if last:
                y = jnp.where(second, 0.0, pair_dot(th, tl, high, low))
            else:
                y = pair_dot(th, tl, jnp.where(corner, high, zero), jnp.where(corner, low, zero))
            half.append(y)
            parts = []
            for j in range(2):
                part = t[j * width : (j + 1) * width]
                if width < 16:
                    part = jnp.concatenate([part] * (16 // width), axis=0)
                parts.append((split(part), span // part.shape[0]))
            full = [
                jnp.concatenate([p[k] for p, count in parts for _ in range(count)], axis=0)
                for k in range(2)
            ]
            if not last:
                full = [jnp.where(diagonal, f, zero) for f in full]
            wide.append(full)
            yield
        for y, full in zip(half, wide):
            yh, yl = split(y)
            r = pair_dot(yh, yl, full[0], full[1])
            fill.append(jnp.where(second, 0.0, r) if last else r)
            yield
        for t, o, r in zip(inv, odd, fill):
            even, lower = t - o, o - r
            merged.append(
                jnp.concatenate(
                    [even[:width], lower[:width], even[width:], lower[width:]], axis=0
                )
            )
        inv = merged
        width *= 2
    return inv


def fused_kernel(
    seq_axis, peers, axis, q_hbm, k_hbm, v_hbm, b_hbm, g_hbm, w_hbm, y_ref,
    b_ref, q_ref, k_ref, v_ref, g_ref, beta_ref, stack_ref, turn_ref, source_ref, x_ref, start_ref,
    low_ref, inv_ref, weight_ref, eye_ref,
    maps, held, carry_ref, states, s_ref, o_ref, m_ref,
    mixed, weight, total, far_out, far_in, near_out, near_in, cross_out, cross_in,
    b_sem, kv_sem, q_sem, g_sem, load_sem, map_send, map_recv, back_send, back_recv,
    far_send, far_recv, near_send, near_recv, cross_send, cross_recv,
):
    heads, blocks, span = q_ref.shape[0], q_ref.shape[1], q_ref.shape[2]
    pairs = heads // 2
    parts = 2
    batch = blocks // parts
    seq = lax.axis_index(seq_axis)
    me = lax.axis_index(axis)
    chip, core = me // 2, me % 2
    sibling = 2 * chip + 1 - core
    across = 2 * (1 - chip) + core
    beyond = 2 * (1 - chip) + 1 - core
    width = y_ref.shape[2]

    def columns(h):
        return pl.ds(pl.multiple_of(h * HEAD_DIM, HEAD_DIM), HEAD_DIM)

    def fetch_kv(h):
        return (
            pltpu.make_async_copy(k_hbm.at[:, :, :, columns(h)], k_ref.at[h], kv_sem.at[0, h]),
            pltpu.make_async_copy(v_hbm.at[:, :, :, columns(h)], v_ref.at[h], kv_sem.at[1, h]),
        )

    def fetch_q(h):
        return pltpu.make_async_copy(q_hbm.at[:, :, columns(h)], q_ref.at[h], q_sem.at[h])

    def fetch_g(h):
        return pltpu.make_async_copy(g_hbm.at[:, :, columns(h)], g_ref.at[h], g_sem.at[h])

    def load(n):
        owner = (beyond, across, sibling, me)[n]
        return pltpu.make_async_copy(
            w_hbm.at[:, pl.ds(pl.multiple_of(owner * width, width), width)],
            weight.at[n],
            load_sem.at[n],
        )

    def start_kv(first, last):
        for n in range(2):
            for h in range(first, last):
                fetch_kv(h)[n].start()

    fetch_b = pltpu.make_async_copy(b_hbm, b_ref, b_sem)
    fetch_b.start()
    start_kv(0, 2)
    barrier = pltpu.get_barrier_semaphore()
    for other in (sibling, across):
        pl.semaphore_signal(barrier, inc=1, device_id={axis: other}, device_id_type=MESH)
    for away in range(1, peers):
        pl.semaphore_signal(
            barrier,
            inc=1,
            device_id={seq_axis: lax.rem(seq + away, peers)},
            device_id_type=MESH,
        )

    eye_ref[...] = (iota(eye_ref.shape, 0) == iota(eye_ref.shape, 1)).astype(F32)
    fetch_b.wait()
    for blk in range(blocks):
        window = slice(blk * span, (blk + 1) * span)
        beta_ref[blk] = jnp.concatenate([b_ref[:, 0, window], b_ref[:, 1, window]], axis=1)

    def place(it, n):
        pair, part = it
        return 2 * pair + n % 2, part * batch + n // 2

    count = 2 * batch

    def key_of(h, blk):
        return jnp.concatenate([k_ref[h, 0, blk], k_ref[h, 1, blk]], axis=0)

    def stack_of(h, blk):
        none = jnp.zeros((HEAD_DIM, HEAD_DIM), BF16)
        return jnp.concatenate(
            [
                jnp.concatenate([stack_ref[h, blk, 0], stack_ref[h, blk, 2]], axis=1),
                jnp.concatenate([stack_ref[h, blk, 1], none], axis=1),
            ],
            axis=0,
        )

    def solve(it):
        slot = it[1]
        grams, squares = [], []
        for n in range(count):
            key = key_of(*place(it, n))
            grams.append(dot_t(key, key))
            if n % 2:
                yield
        for n, g in enumerate(grams):
            squares.append(jnp.sum(eye_ref[...] * g, axis=0, keepdims=True))
            if n % 4 == 3:
                yield
        beta = jnp.concatenate(
            [beta_ref[place(it, n)[1], pl.ds(place(it, n)[0], 1), :] for n in range(count)], axis=0
        )
        norm = lax.rsqrt(jnp.concatenate(squares, axis=0) + 1e-06)
        value_weight = beta * norm
        weight_rows = value_weight * norm
        weight_ref[slot, 0] = weight_rows
        weight_ref[slot, 1] = value_weight
        weight_cols = weight_rows.T
        yield
        lowers = []
        for n, g in enumerate(grams):
            low = weight_cols[:, n : n + 1] * g
            lowers.append(low)
            low_ref[slot, n, 0], low_ref[slot, n, 1] = split(low)
            if n % 2:
                yield
        inv = yield from base_solve(lowers, span)
        for n in range(count):
            inv_ref[slot, n] = inv[n]

    def transit(it):
        slot = it[1]

        def pieces(n):
            return low_ref[slot, n, 0], low_ref[slot, n, 1]

        solved = yield from merge([inv_ref[slot, n] for n in range(count)], pieces, span)
        turns, writes, changes = [], [], []
        for n in range(count):
            h, blk = place(it, n)
            th, tl = split(solved[n] * weight_ref[slot, 0, n : n + 1, :])
            tv = (solved[n] * weight_ref[slot, 1, n : n + 1, :]).astype(BF16)
            key = key_of(h, blk)
            value = jnp.concatenate([v_ref[h, 0, blk], v_ref[h, 1, blk]], axis=0)
            turns.append(
                dot(jnp.concatenate([th, tl], axis=1), jnp.concatenate([key, key], axis=0))
            )
            writes.append(dot(tv, value))
            yield
        for n in range(count):
            h, blk = place(it, n)
            turn_h, turn_l = split(turns[n])
            stack_ref[h, blk, 0], stack_ref[h, blk, 1] = turn_h, turn_l
            stack_ref[h, blk, 2] = writes[n].astype(BF16)
            stack = stack_of(h, blk)
            key_t = key_of(h, blk).T
            changes.append(dot(jnp.concatenate([key_t, key_t], axis=1), stack))
            yield
        for n in range(count):
            step = eye_ref[...] - changes[n][:, :HEAD_DIM]
            turn_ref[slot, n, 0], turn_ref[slot, n, 1] = split(step)
            source_ref[slot, n] = changes[n][:, HEAD_DIM:]
            yield

    def compose(it):
        slot = it[1]
        pair, _ = it
        states_now = [None if it[1] == 0 else x_ref[2 * pair + i] for i in range(2)]
        for n in range(count):
            h, blk = place(it, n)
            i = n % 2
            if blk == 0:
                turn_h, turn_l = turn_ref[slot, n, 0], turn_ref[slot, n, 1]
                states_now[i] = jnp.concatenate(
                    [turn_h.astype(F32) + turn_l.astype(F32), source_ref[slot, n]], axis=1
                )
                yield
                continue
            high, low = split(states_now[i])
            start_ref[h, blk, 0] = high[:, :HEAD_DIM]
            start_ref[h, blk, 1] = high[:, HEAD_DIM:]
            turn_h, turn_l = turn_ref[slot, n, 0], turn_ref[slot, n, 1]
            moved = dot(
                jnp.concatenate([turn_h, turn_l, turn_h], axis=1),
                jnp.concatenate([high, high, low], axis=0),
            )
            states_now[i] = jnp.concatenate(
                [moved[:, :HEAD_DIM], moved[:, HEAD_DIM:] + source_ref[slot, n]], axis=1
            )
            if n >= count - 2:
                x_ref[h] = states_now[i]
            yield

    def a_stream(it, first=0.0, last=1.0):
        return 7 * count // 4 + BASE + 1, solve(it), first, last

    def b_stream(it, first=0.0, last=1.0):
        return 9 * count, transit(it), first, last

    def c_stream(it, first=0.0, last=1.0):
        return count, compose(it), first, last

    def owner_of(pair, i):
        side = lax.rem(pair + core, 2)
        return peers // 2 - 2 + side + i * (3 - 2 * side)

    def send_map(pair, i, source):
        h = 2 * pair + i
        return pltpu.make_async_remote_copy(
            src_ref=maps.at[h],
            dst_ref=held.at[pair, source],
            send_sem=map_send.at[h],
            recv_sem=map_recv.at[pair, source],
            device_id={seq_axis: owner_of(pair, i)},
            device_id_type=MESH,
        )

    def send_state(pair, i, target):
        h = 2 * pair + i
        return pltpu.make_async_remote_copy(
            src_ref=states.at[pair, target],
            dst_ref=s_ref.at[h],
            send_sem=back_send.at[pair, target],
            recv_sem=back_recv.at[h],
            device_id={seq_axis: target},
            device_id_type=MESH,
        )

    def post(pair):
        for i in range(2):
            h = 2 * pair + i
            maps[h, 0] = x_ref[h, :, :HEAD_DIM].astype(BF16)
            maps[h, 1] = x_ref[h, :, HEAD_DIM:].astype(BF16)

            @pl.when((seq != owner_of(pair, i)) & (seq != peers - 1))
            def _():
                send_map(pair, i, seq).start()

            @pl.when(seq == owner_of(pair, i))
            def _():
                held[pair, seq] = maps[h]

    def chain(pair):
        for i in range(2):

            @pl.when(seq == owner_of(pair, i))
            def _():
                carry_ref[...] = jnp.zeros((HEAD_DIM, HEAD_DIM), F32)
                for k in range(peers - 1):

                    @pl.when(seq != k)
                    def _():
                        send_map(pair, i, k).wait_recv()

                    high, low = split(carry_ref[...])
                    turn = held[pair, k, 0]
                    state = held[pair, k, 1].astype(F32) + dot(
                        jnp.concatenate([turn, turn], axis=1),
                        jnp.concatenate([high, low], axis=0),
                    )
                    carry_ref[...] = state
                    states[pair, k + 1] = state.astype(BF16)

                    @pl.when(seq != k + 1)
                    def _():
                        send_state(pair, i, k + 1).start()

                    @pl.when(seq == k + 1)
                    def _():
                        s_ref[2 * pair + i] = states[pair, k + 1]

    @pl.when(seq == 0)
    def _():
        s_ref[...] = jnp.zeros(s_ref.shape, BF16)

    def wait_kv(pair):
        for i in range(2):
            for copy in fetch_kv(2 * pair + i):
                copy.wait()

    def after_values(pair, stream):
        for i in range(2):
            fetch_kv(2 * pair + i)[1].wait()
        yield from stream

    for h in range(2):
        fetch_kv(h)[0].wait()
    start_kv(2, heads)
    for h in range(heads):
        fetch_q(h).start()
    for n in range(4):
        load(n).start()
    for h in range(heads):
        fetch_g(h).start()
    weave(
        a_stream((0, 0), 0.0, 1.0),
        a_stream((0, 1), 0.5, 2.0),
        (9 * count, after_values(0, transit((0, 0))), 1.1, 2.1),
    )

    def step(pair, _):
        wait_kv(pair)
        weave(
            a_stream((pair, 0), 0.0, 1.0),
            b_stream((pair - 1, 1), 0.0, 1.0),
            c_stream((pair - 1, 0), 0.0, 1.0),
            a_stream((pair, 1), 1.05, 2.0),
            b_stream((pair, 0), 1.05, 2.0),
            c_stream((pair - 1, 1), 1.05, 2.0),
        )

        @pl.when(pair == 1)
        def _():
            pl.semaphore_wait(barrier, peers + 1)

        post(pair - 1)
        return 0

    lax.fori_loop(1, pairs, step, 0)
    chain(0)
    weave(
        b_stream((pairs - 1, 1), 0.0, 9.0),
        c_stream((pairs - 1, 0), 0.0, 6.0),
        c_stream((pairs - 1, 1), 8.1, 9.1),
    )
    post(pairs - 1)
    for h in range(heads):
        fetch_q(h).wait()

    def read(pair, _):
        causal = iota((span, 2 * span), 1) % span <= iota((span, 2 * span), 0)
        for i in range(2):
            h = 2 * pair + i
            scores = []
            for blk in range(blocks):
                found = jnp.where(causal, dot_t(q_ref[h, blk], key_of(h, blk)), 0.0).astype(BF16)
                scores.append(jnp.concatenate([found, found], axis=1))
            drawn = [dot(score, stack_of(h, blk)) for blk, score in enumerate(scores)]
            for blk in range(blocks):
                kept = (q_ref[h, blk].astype(F32) - drawn[blk][:, :HEAD_DIM]).astype(BF16)
                if blk == 0:
                    m_ref[h, blk] = kept
                    o_ref[h, blk] = drawn[blk][:, HEAD_DIM:]
                    continue
                out = dot(kept, jnp.concatenate([start_ref[h, blk, 0], start_ref[h, blk, 1]], axis=1))
                m_ref[h, blk] = out[:, :HEAD_DIM].astype(BF16)
                o_ref[h, blk] = out[:, HEAD_DIM:] + drawn[blk][:, HEAD_DIM:]

        return 0

    chain(1)
    lax.fori_loop(0, pairs, read, 0)
    for h in range(heads):
        fetch_g(h).wait()

    def wait_state(pair):
        for i in range(2):

            @pl.when((seq != owner_of(pair, i)) & (seq != 0))
            def _():
                send_state(pair, i, seq).wait_recv()

    def blend(pair, t):
        for i in range(2):
            h = 2 * pair + i
            query = q_ref[h, t].astype(F32)
            unit = lax.rsqrt(jnp.sum(query * query, axis=1, keepdims=True) + 1e-06)
            seen = unit * (o_ref[h, t] + dot(m_ref[h, t], s_ref[h]))
            scale = lax.rsqrt(jnp.mean(seen * seen, axis=1, keepdims=True) + 1e-06)
            gate = g_ref[h, t].astype(F32)
            mixed[t, h] = (seen * scale * (gate / (1.0 + jnp.exp(-gate)))).astype(BF16)

    def blend_pair(pair):
        wait_state(pair)
        for blk in range(blocks):
            blend(pair, blk)

    def settle(pair, _):
        blend_pair(pair)
        return 0

    def link(pair, _):
        chain(pair)
        return 0

    lax.fori_loop(2, pairs, link, 0)
    lax.fori_loop(0, pairs - 1, settle, 0)

    def send(source, target, send_sem, recv_sem, t, device):
        return pltpu.make_async_remote_copy(
            src_ref=source.at[t],
            dst_ref=target.at[t],
            send_sem=send_sem.at[t],
            recv_sem=recv_sem.at[t],
            device_id={axis: device},
            device_id_type=MESH,
        )

    def far(t):
        return send(far_out, far_in, far_send, far_recv, t, sibling)

    def near(t):
        return send(near_out, near_in, near_send, near_recv, t, sibling)

    def cross(t):
        return send(cross_out, cross_in, cross_send, cross_recv, t, across)

    def pass_on(t):
        far(t).wait()
        cross_out[t] = (total[t] + far_in[t].astype(F32)).astype(BF16)
        cross(t).start()

    share = blocks // PIECES

    def rows_of(t, first, last):
        return jnp.concatenate(
            [
                jnp.concatenate([mixed[t * share + b, h] for h in range(first, last)], axis=1)
                for b in range(share)
            ],
            axis=0,
        )

    def product(t, n):
        return dot(rows_of(t, 0, heads), weight[n])

    def finish_piece(t):
        for b in range(share):
            blend(pairs - 1, t * share + b)

    early = (heads - 2) * HEAD_DIM
    load(0).wait()
    total[0] = dot(rows_of(0, 0, heads - 2), weight[0, :early, :])
    wait_state(pairs - 1)
    finish_piece(0)
    far_out[0] = (total[0] + dot(rows_of(0, heads - 2, heads), weight[0, early:, :])).astype(BF16)
    far(0).start()
    load(1).wait()
    total[0] = product(0, 1)
    for t in range(1, PIECES):
        finish_piece(t)
        far_out[t] = product(t, 0).astype(BF16)
        far(t).start()
        if t > 1:
            total[t] = product(t, 1)
        pass_on(t - 1)
        if t == 1:
            total[t] = product(t, 1)
    load(2).wait()
    for t in range(PIECES):
        near_out[t] = product(t, 2).astype(BF16)
        near(t).start()
        if t == 0:
            pass_on(PIECES - 1)
    load(3).wait()
    for t in range(PIECES):
        total[t] = product(t, 3)

    for t in range(PIECES):
        near(t).wait()
        cross(t).wait()
        y_ref[t] = (total[t] + near_in[t].astype(F32) + cross_in[t].astype(F32)).astype(BF16)
    for pair in range(pairs):
        for i in range(2):

            @pl.when((seq != owner_of(pair, i)) & (seq != peers - 1))
            def _():
                send_map(pair, i, seq).wait_send()

            @pl.when(seq == owner_of(pair, i))
            def _():
                for k in range(1, peers):

                    @pl.when(seq != k)
                    def _():
                        send_state(pair, i, k).wait_send()


def fused(queries, keys, values, betas, gate, out_weight, seq_axis, axis):
    tokens, depth = queries.shape
    heads = depth // HEAD_DIM
    peers = lax.axis_size(seq_axis)
    width = out_weight.shape[1] // lax.axis_size(axis)
    blocks = tokens // SPAN
    batch = blocks // 2
    hbm = pl.BlockSpec(memory_space=pltpu.HBM)
    piece = (PIECES, tokens // PIECES, width)
    square = (HEAD_DIM, HEAD_DIM)
    wide = (HEAD_DIM, 2 * HEAD_DIM)
    two = (2,) + square
    pairs = heads // 2
    dma = pltpu.SemaphoreType.DMA
    per_head = (heads, blocks, SPAN, HEAD_DIM)
    both = (heads, 2, blocks, SPAN, HEAD_DIM)
    return pl.pallas_call(
        functools.partial(fused_kernel, seq_axis, peers, axis),
        in_specs=[hbm] * 6,
        out_specs=pl.BlockSpec(memory_space=pltpu.VMEM),
        out_shape=jax.ShapeDtypeStruct(piece, BF16),
        scratch_shapes=[
            pltpu.VMEM(betas.shape, F32),
            pltpu.VMEM(per_head, BF16),
            pltpu.VMEM(both, BF16),
            pltpu.VMEM(both, BF16),
            pltpu.VMEM(per_head, BF16),
            pltpu.VMEM((blocks, heads, 2 * SPAN), F32),
            pltpu.VMEM((heads, blocks, 3) + square, BF16),
            pltpu.VMEM((2, 2 * batch) + two, BF16),
            pltpu.VMEM((2, 2 * batch) + square, F32),
            pltpu.VMEM((heads,) + wide, F32),
            pltpu.VMEM((heads, blocks) + two, BF16),
            pltpu.VMEM((2, 2 * batch) + two, BF16),
            pltpu.VMEM((2, 2 * batch, BASE, 2 * SPAN), F32),
            pltpu.VMEM((2, 2, 2 * batch, 2 * SPAN), F32),
            pltpu.VMEM(square, F32),
            pltpu.VMEM((heads,) + two, BF16),
            pltpu.VMEM((pairs, peers) + two, BF16),
            pltpu.VMEM(square, F32),
            pltpu.VMEM((pairs, peers) + square, BF16),
            pltpu.VMEM((heads,) + square, BF16),
            pltpu.VMEM(per_head, F32),
            pltpu.VMEM(per_head, BF16),
            pltpu.VMEM((blocks, heads, SPAN, HEAD_DIM), BF16),
            pltpu.VMEM((4, depth, width), BF16),
            pltpu.VMEM(piece, F32),
        ]
        + [pltpu.VMEM(piece, BF16)] * 6
        + [
            dma,
            dma((2, heads)),
            dma((heads,)),
            dma((heads,)),
            dma((4,)),
            dma((heads,)),
            dma((pairs, peers)),
            dma((pairs, peers)),
            dma((heads,)),
        ]
        + [dma((PIECES,))] * 6,
        compiler_params=pltpu.CompilerParams(
            collective_id=0, has_side_effects=True, vmem_limit_bytes=FUSED_LIMIT
        ),
    )(
        queries.reshape(blocks, SPAN, depth),
        keys.reshape(2, blocks, SPAN, depth),
        values.reshape(2, blocks, SPAN, depth),
        pltpu.with_memory_space_constraint(betas, pltpu.HBM),
        gate.reshape(blocks, SPAN, depth),
        out_weight,
    ).reshape(tokens, width)


def start_state(maps, axis):
    peers, index = lax.axis_size(axis), lax.axis_index(axis)
    heads = maps.shape[0]
    held = lax.all_gather(maps, axis, axis=0, tiled=True)
    states = pl.pallas_call(
        functools.partial(chain_kernel, peers),
        out_shape=jax.ShapeDtypeStruct((held.shape[0], HEAD_DIM, HEAD_DIM), BF16),
        compiler_params=pltpu.CompilerParams(vmem_limit_bytes=VMEM_LIMIT),
    )(held)
    return lax.dynamic_slice_in_dim(states, index * heads, heads, 0)


def out_kernel(o_ref, m_ref, s_ref, g_ref, w_ref, y_ref, mixed_ref):
    @pl.when(pl.program_id(0) == 0)
    def _():
        for h in range(s_ref.shape[0]):
            cols = slice(h * HEAD_DIM, (h + 1) * HEAD_DIM)
            seen = o_ref[:, cols] + dot(m_ref[:, cols], s_ref[h])
            scale = lax.rsqrt(jnp.mean(seen * seen, axis=1, keepdims=True) + 1e-06)
            gate = g_ref[:, cols].astype(F32)
            mixed_ref[:, cols] = (seen * scale * (gate / (1.0 + jnp.exp(-gate)))).astype(BF16)

    y_ref[...] = dot(mixed_ref[...], w_ref[...]).astype(BF16)


def project(local, reach, states, gate, out_weight):
    tokens, width = local.shape
    total = out_weight.shape[1]
    tile = 512
    whole = pl.BlockSpec((tokens, width), lambda n: (0, 0))
    return pl.pallas_call(
        out_kernel,
        grid=(total // tile,),
        in_specs=[
            whole,
            whole,
            pl.BlockSpec(states.shape, lambda n: (0, 0, 0)),
            whole,
            pl.BlockSpec((width, tile), lambda n: (0, n)),
        ],
        out_specs=pl.BlockSpec((tokens, tile), lambda n: (0, n)),
        out_shape=jax.ShapeDtypeStruct((tokens, total), BF16),
        scratch_shapes=[pltpu.VMEM((tokens, width), BF16)],
        compiler_params=pltpu.CompilerParams(
            dimension_semantics=("arbitrary",), vmem_limit_bytes=VMEM_LIMIT
        ),
    )(local, reach, states, gate, out_weight)


def per_device(queries, keys, values, betas, gate, out_weight):
    heads, _, tokens = betas.shape
    peers, index = lax.axis_size("ctx"), lax.axis_size("head")
    if index == 4 and peers >= 4 and peers % 2 == 0 and heads % 8 == 0 and tokens % (8 * SPAN) == 0:
        return fused(queries, keys, values, betas, gate, out_weight, "ctx", "head")
    beta_cols = betas.transpose(2, 1, 0).reshape(2 * tokens, heads)
    local, reach, maps = mix(queries, keys, values, beta_cols)
    states = start_state(maps, "ctx")
    partial_sum = project(local, reach, states, gate, out_weight)
    return lax.psum_scatter(partial_sum, "head", scatter_dimension=1, tiled=True)


def solution(mesh):
    return jax.shard_map(
        per_device,
        mesh=mesh,
        in_specs=(
            P("ctx", "head"),
            P(None, "ctx", "head"),
            P(None, "ctx", "head"),
            P("head", None, "ctx"),
            P("ctx", "head"),
            P("head", None),
        ),
        out_specs=P("ctx", "head"),
        check_vma=False,
    )
```

```python
import functools

import jax
import jax.numpy as jnp
from jax import lax
from jax.experimental import pallas as pl
from jax.experimental.pallas import tpu as pltpu
from jax.sharding import PartitionSpec as P

HEAD_DIM = 128
SPAN = 64
BASE = 16
F32 = jnp.float32
BF16 = jnp.bfloat16
VMEM_LIMIT = 60 * 1024 * 1024
MESH = pl.DeviceIdType.MESH
PIECES = 4


def iota(shape, dim):
    return lax.broadcasted_iota(jnp.int32, shape, dim)


def split(a):
    high = a.astype(BF16)
    return high, (a - high.astype(F32)).astype(BF16)


def dot(a, b):
    return jnp.dot(a, b, preferred_element_type=F32)


def dot3(a, b):
    ah, al = split(a)
    bh, bl = split(b)
    return dot(jnp.concatenate([ah, al, ah], axis=1), jnp.concatenate([bh, bh, bl], axis=0))


def inverse(lowers, order):
    lane = iota((BASE, order), 1)
    compact = []
    for low in lowers:
        total = jnp.zeros((BASE, order), F32)
        for blk in range(order // BASE):
            total = jnp.where(lane // BASE == blk, low[blk * BASE : (blk + 1) * BASE, :], total)
        compact.append(total)
    inv = [(iota((BASE, order), 0) == lane % BASE).astype(F32) for _ in lowers]
    for j in range(BASE - 1):
        pick = (lane // BASE) * BASE + j
        for n, low in enumerate(compact):
            column = jnp.take_along_axis(low, pick, axis=1, mode="promise_in_bounds")
            inv[n] = inv[n] - column * inv[n][j : j + 1, :]
    row = iota((order, order), 0)
    col = iota((order, order), 1)
    width = BASE
    while width < order:
        corner = (row // (2 * width) == col // (2 * width)) & (row // width != col // width)
        diagonal = row // width == col // width
        second = (iota((width, order), 1) // width) % 2 == 1
        half = [dot3(jnp.where(second, t, 0.0), jnp.where(corner, low, 0.0)) for t, low in zip(inv, lowers)]
        full = [
            jnp.where(diagonal, jnp.concatenate([t] * (order // width), axis=0), 0.0) for t in inv
        ]
        fill = [dot3(y, e) for y, e in zip(half, full)]
        inv = [
            jnp.concatenate([jnp.where(second, 0.0, t), jnp.where(second, t, 0.0) - r], axis=0)
            for t, r in zip(inv, fill)
        ]
        width *= 2
    return inv


def mix_kernel(q_ref, k_ref, v_ref, b_ref, o_ref, m_ref, x_out, x_ref):
    heads = q_ref.shape[1] // HEAD_DIM
    span = q_ref.shape[0]
    order = 2 * span
    step = pl.program_id(0)

    @pl.when(step == 0)
    def _():
        start = (iota((HEAD_DIM, 2 * HEAD_DIM), 0) == iota((HEAD_DIM, 2 * HEAD_DIM), 1)).astype(F32)
        for h in range(heads):
            x_ref[h] = start

    row = iota((order, order), 0)
    col = iota((order, order), 1)
    strict = col < row
    weave = (row == 2 * (col % span) + col // span).astype(BF16)
    causal = iota((span, order), 1) <= 2 * iota((span, order), 0) + 1
    data = []
    lowers = []
    for h in range(heads):
        cols = slice(h * HEAD_DIM, (h + 1) * HEAD_DIM)
        query = q_ref[:, cols]
        pair = jnp.concatenate(
            [
                jnp.concatenate([k_ref[0, :, cols], v_ref[0, :, cols]], axis=1),
                jnp.concatenate([k_ref[1, :, cols], v_ref[1, :, cols]], axis=1),
            ],
            axis=0,
        )
        woven = dot(weave, pair)
        key = woven[:, :HEAD_DIM]
        value = woven[:, HEAD_DIM:]
        key_b = key.astype(BF16)
        norm = lax.rsqrt(jnp.sum(key * key, axis=1, keepdims=True) + 1e-06)
        beta = b_ref[:, h : h + 1]
        both = jnp.concatenate([key_b, query], axis=0)
        gram = lax.dot_general(both, key_b, (((1,), (1,)), ((), ())), preferred_element_type=F32)
        weight = beta * norm * norm
        lowers.append(jnp.where(strict, weight * gram[:order], 0.0))
        scores = jnp.where(causal, gram[order:], 0.0).astype(BF16)
        qf = query.astype(F32)
        q_norm = lax.rsqrt(jnp.sum(qf * qf, axis=1, keepdims=True) + 1e-06)
        readers = jnp.concatenate([key.T.astype(BF16), scores], axis=0)
        data.append((both, readers, beta * norm * value, weight, q_norm))
    solved = inverse(lowers, order)
    seen = []
    for h in range(heads):
        both = data[h][0]
        high, low = split(x_ref[h])
        seen.append(
            dot(jnp.concatenate([both, both], axis=1), jnp.concatenate([high, low], axis=0))
        )
    writes = []
    for h in range(heads):
        _, _, scaled, weight, _ = data[h]
        gap = -weight * seen[h][:order]
        gap = jnp.concatenate([gap[:, :HEAD_DIM], gap[:, HEAD_DIM:] + scaled], axis=1)
        writes.append(dot3(solved[h], gap))
    for h in range(heads):
        cols = slice(h * HEAD_DIM, (h + 1) * HEAD_DIM)
        readers, q_norm = data[h][1], data[h][4]
        high, low = split(writes[h])
        change = dot(
            jnp.concatenate([readers, readers], axis=1), jnp.concatenate([high, low], axis=0)
        )
        x_ref[h] = x_ref[h] + change[:HEAD_DIM]
        out = q_norm * (seen[h][order:] + change[HEAD_DIM:])
        m_ref[:, cols] = out[:, :HEAD_DIM].astype(BF16)
        o_ref[:, cols] = out[:, HEAD_DIM:]

    @pl.when(step == pl.num_programs(0) - 1)
    def _():
        for h in range(heads):
            x_out[h] = x_ref[h].astype(BF16)


def mix(queries, keys, values, beta_cols):
    tokens, width = queries.shape
    heads = width // HEAD_DIM
    return pl.pallas_call(
        mix_kernel,
        grid=(tokens // SPAN,),
        in_specs=[
            pl.BlockSpec((SPAN, width), lambda c: (c, 0)),
            pl.BlockSpec((2, SPAN, width), lambda c: (0, c, 0)),
            pl.BlockSpec((2, SPAN, width), lambda c: (0, c, 0)),
            pl.BlockSpec((2 * SPAN, heads), lambda c: (c, 0)),
        ],
        out_specs=[
            pl.BlockSpec((SPAN, width), lambda c: (c, 0)),
            pl.BlockSpec((SPAN, width), lambda c: (c, 0)),
            pl.BlockSpec((heads, HEAD_DIM, 2 * HEAD_DIM), lambda c: (0, 0, 0)),
        ],
        out_shape=[
            jax.ShapeDtypeStruct((tokens, width), F32),
            jax.ShapeDtypeStruct((tokens, width), BF16),
            jax.ShapeDtypeStruct((heads, HEAD_DIM, 2 * HEAD_DIM), BF16),
        ],
        scratch_shapes=[pltpu.VMEM((heads, HEAD_DIM, 2 * HEAD_DIM), F32)],
        compiler_params=pltpu.CompilerParams(
            dimension_semantics=("arbitrary",), vmem_limit_bytes=VMEM_LIMIT
        ),
    )(queries, keys, values, beta_cols)


def chain_kernel(peers, x_ref, s_ref):
    heads = x_ref.shape[0] // peers
    for h in range(heads):
        state = jnp.zeros((HEAD_DIM, HEAD_DIM), F32)
        for k in range(peers):
            s_ref[k * heads + h] = state.astype(BF16)
            if k < peers - 1:
                maps = x_ref[k * heads + h]
                turn = maps[:, :HEAD_DIM]
                high, low = split(state)
                state = maps[:, HEAD_DIM:].astype(F32) + dot(
                    jnp.concatenate([turn, turn], axis=1), jnp.concatenate([high, low], axis=0)
                )


FUSED_LIMIT = 52 * 1024 * 1024


def dot_t(a, b):
    return lax.dot_general(a, b, (((1,), (1,)), ((), ())), preferred_element_type=F32)


def pair_dot(a, low, high_b, low_b):
    rows = a.shape[0]
    both = dot(jnp.concatenate([a, low], axis=0), jnp.concatenate([high_b, low_b], axis=1))
    width = high_b.shape[1]
    return both[:rows, :width] + both[rows:, :width] + both[:rows, width:]


def weave(*streams):
    order = []
    for n, (count, _, first, last) in enumerate(streams):
        order += [(first + (last - first) * (k + 0.5) / count, n) for k in range(count)]
    for _, n in sorted(order):
        next(streams[n][1], None)
    for _, stream, _, _ in streams:
        for _ in stream:
            pass


def base_solve(lowers, span):
    order = 2 * span
    base = BASE // 2
    lane = iota((base, order), 1)
    group = (lane % span) // base
    row16, lane16 = iota((BASE, order), 0), iota((BASE, order), 1)
    group16 = (lane16 % span) // base
    row_tok, lane_tok = row16 % base, lane16 % base
    before = (lane_tok < row_tok) | ((lane_tok == row_tok) & (lane16 // span < row16 // base))
    compact = []
    for n, low in enumerate(lowers):
        halves = []
        for j in range(2):
            total = jnp.zeros((base, order), F32)
            for blk in range(span // base):
                start = j * span + blk * base
                total = jnp.where(group == blk, low[start : start + base, :], total)
            halves.append(total)
        compact.append(jnp.where(before, jnp.concatenate(halves, axis=0), 0.0))
        if n % 2:
            yield
    own = (row16 % base == lane16 % base) & (row16 // base == lane16 // span)
    inv = [own.astype(F32) for _ in lowers]
    for s in range(BASE - 1):
        t, j = s // 2, s % 2
        pick = j * span + group16 * base + t
        for n, low in enumerate(compact):
            column = jnp.take_along_axis(low, pick, axis=1, mode="promise_in_bounds")
            inv[n] = inv[n] - column * inv[n][j * base + t : j * base + t + 1, :]
        yield
    return inv


def merge(inv, pieces, span):
    order = 2 * span
    tok_r = iota((order, order), 0) % span
    tok_c = iota((order, order), 1) % span
    width = BASE // 2
    zero = jnp.zeros((), BF16)
    while width < span:
        last = 2 * width == span
        diagonal = tok_r // width == tok_c // width
        corner = (tok_r // (2 * width) == tok_c // (2 * width)) & (tok_r // width != tok_c // width)
        second = ((iota((2 * width, order), 1) % span) // width) % 2 == 1
        odd, half, fill, wide, merged = [], [], [], [], []
        for n, t in enumerate(inv):
            odd.append(jnp.where(second, t, 0.0))
            th, tl = split(odd[n])
            high, low = pieces(n)
            if last:
                y = jnp.where(second, 0.0, pair_dot(th, tl, high, low))
            else:
                y = pair_dot(th, tl, jnp.where(corner, high, zero), jnp.where(corner, low, zero))
            half.append(y)
            parts = []
            for j in range(2):
                part = t[j * width : (j + 1) * width]
                if width < 16:
                    part = jnp.concatenate([part] * (16 // width), axis=0)
                parts.append((split(part), span // part.shape[0]))
            full = [
                jnp.concatenate([p[k] for p, count in parts for _ in range(count)], axis=0)
                for k in range(2)
            ]
            if not last:
                full = [jnp.where(diagonal, f, zero) for f in full]
            wide.append(full)
            yield
        for y, full in zip(half, wide):
            yh, yl = split(y)
            r = pair_dot(yh, yl, full[0], full[1])
            fill.append(jnp.where(second, 0.0, r) if last else r)
            yield
        for t, o, r in zip(inv, odd, fill):
            even, lower = t - o, o - r
            merged.append(
                jnp.concatenate(
                    [even[:width], lower[:width], even[width:], lower[width:]], axis=0
                )
            )
        inv = merged
        width *= 2
    return inv


def fused_kernel(
    seq_axis, peers, axis, q_hbm, k_hbm, v_hbm, b_hbm, g_hbm, w_hbm, y_ref,
    b_ref, q_ref, k_ref, v_ref, g_ref, beta_ref, stack_ref, turn_ref, source_ref, x_ref, start_ref,
    low_ref, inv_ref, weight_ref, eye_ref,
    maps, held, carry_ref, states, s_ref, o_ref, m_ref,
    mixed, weight, total, far_out, far_in, near_out, near_in, cross_out, cross_in,
    b_sem, kv_sem, q_sem, g_sem, load_sem, map_send, map_recv, back_send, back_recv,
    far_send, far_recv, near_send, near_recv, cross_send, cross_recv,
):
    heads, blocks, span = q_ref.shape[0], q_ref.shape[1], q_ref.shape[2]
    pairs = heads // 2
    parts = 2
    batch = blocks // parts
    seq = lax.axis_index(seq_axis)
    me = lax.axis_index(axis)
    chip, core = me // 2, me % 2
    sibling = 2 * chip + 1 - core
    across = 2 * (1 - chip) + core
    beyond = 2 * (1 - chip) + 1 - core
    width = y_ref.shape[1]

    def columns(h):
        return pl.ds(pl.multiple_of(h * HEAD_DIM, HEAD_DIM), HEAD_DIM)

    def fetch_kv(h):
        return (
            pltpu.make_async_copy(k_hbm.at[:, :, :, columns(h)], k_ref.at[h], kv_sem.at[0, h]),
            pltpu.make_async_copy(v_hbm.at[:, :, :, columns(h)], v_ref.at[h], kv_sem.at[1, h]),
        )

    def fetch_q(h):
        return pltpu.make_async_copy(q_hbm.at[:, :, columns(h)], q_ref.at[h], q_sem.at[h])

    def fetch_g(h):
        return pltpu.make_async_copy(g_hbm.at[:, :, columns(h)], g_ref.at[h], g_sem.at[h])

    def load(n):
        owner = (beyond, across, sibling, me)[n]
        return pltpu.make_async_copy(
            w_hbm.at[:, pl.ds(pl.multiple_of(owner * width, width), width)],
            weight.at[n],
            load_sem.at[n],
        )

    def start_kv(first, last):
        for n in range(2):
            for h in range(first, last):
                fetch_kv(h)[n].start()

    fetch_b = pltpu.make_async_copy(b_hbm, b_ref, b_sem)
    fetch_b.start()
    start_kv(0, 2)
    barrier = pltpu.get_barrier_semaphore()
    for other in (sibling, across):
        pl.semaphore_signal(barrier, inc=1, device_id={axis: other}, device_id_type=MESH)
    for away in range(1, peers):
        pl.semaphore_signal(
            barrier,
            inc=1,
            device_id={seq_axis: lax.rem(seq + away, peers)},
            device_id_type=MESH,
        )

    eye_ref[...] = (iota(eye_ref.shape, 0) == iota(eye_ref.shape, 1)).astype(F32)
    fetch_b.wait()
    for blk in range(blocks):
        window = slice(blk * span, (blk + 1) * span)
        beta_ref[blk] = jnp.concatenate([b_ref[:, 0, window], b_ref[:, 1, window]], axis=1)

    def place(it, n):
        pair, part = it
        return 2 * pair + n % 2, part * batch + n // 2

    count = 2 * batch

    def key_of(h, blk):
        return jnp.concatenate([k_ref[h, 0, blk], k_ref[h, 1, blk]], axis=0)

    def stack_of(h, blk):
        none = jnp.zeros((HEAD_DIM, HEAD_DIM), BF16)
        return jnp.concatenate(
            [
                jnp.concatenate([stack_ref[h, blk, 0], stack_ref[h, blk, 2]], axis=1),
                jnp.concatenate([stack_ref[h, blk, 1], none], axis=1),
            ],
            axis=0,
        )

    def solve(it):
        slot = it[1]
        grams, squares = [], []
        for n in range(count):
            key = key_of(*place(it, n))
            grams.append(dot_t(key, key))
            if n % 2:
                yield
        for n, g in enumerate(grams):
            squares.append(jnp.sum(eye_ref[...] * g, axis=0, keepdims=True))
            if n % 4 == 3:
                yield
        beta = jnp.concatenate(
            [beta_ref[place(it, n)[1], pl.ds(place(it, n)[0], 1), :] for n in range(count)], axis=0
        )
        norm = lax.rsqrt(jnp.concatenate(squares, axis=0) + 1e-06)
        value_weight = beta * norm
        weight_rows = value_weight * norm
        weight_ref[slot, 0] = weight_rows
        weight_ref[slot, 1] = value_weight
        weight_cols = weight_rows.T
        yield
        lowers = []
        for n, g in enumerate(grams):
            low = weight_cols[:, n : n + 1] * g
            lowers.append(low)
            low_ref[slot, n, 0], low_ref[slot, n, 1] = split(low)
            if n % 2:
                yield
        inv = yield from base_solve(lowers, span)
        for n in range(count):
            inv_ref[slot, n] = inv[n]

    def transit(it):
        slot = it[1]

        def pieces(n):
            return low_ref[slot, n, 0], low_ref[slot, n, 1]

        solved = yield from merge([inv_ref[slot, n] for n in range(count)], pieces, span)
        turns, writes, changes = [], [], []
        for n in range(count):
            h, blk = place(it, n)
            th, tl = split(solved[n] * weight_ref[slot, 0, n : n + 1, :])
            tv = (solved[n] * weight_ref[slot, 1, n : n + 1, :]).astype(BF16)
            key = key_of(h, blk)
            value = jnp.concatenate([v_ref[h, 0, blk], v_ref[h, 1, blk]], axis=0)
            turns.append(
                dot(jnp.concatenate([th, tl], axis=1), jnp.concatenate([key, key], axis=0))
            )
            writes.append(dot(tv, value))
            yield
        for n in range(count):
            h, blk = place(it, n)
            turn_h, turn_l = split(turns[n])
            stack_ref[h, blk, 0], stack_ref[h, blk, 1] = turn_h, turn_l
            stack_ref[h, blk, 2] = writes[n].astype(BF16)
            stack = stack_of(h, blk)
            key_t = key_of(h, blk).T
            changes.append(dot(jnp.concatenate([key_t, key_t], axis=1), stack))
            yield
        for n in range(count):
            step = eye_ref[...] - changes[n][:, :HEAD_DIM]
            turn_ref[slot, n, 0], turn_ref[slot, n, 1] = split(step)
            source_ref[slot, n] = changes[n][:, HEAD_DIM:]
            yield

    def compose(it):
        slot = it[1]
        pair, _ = it
        states_now = [None if it[1] == 0 else x_ref[2 * pair + i] for i in range(2)]
        for n in range(count):
            h, blk = place(it, n)
            i = n % 2
            if blk == 0:
                turn_h, turn_l = turn_ref[slot, n, 0], turn_ref[slot, n, 1]
                states_now[i] = jnp.concatenate(
                    [turn_h.astype(F32) + turn_l.astype(F32), source_ref[slot, n]], axis=1
                )
                yield
                continue
            high, low = split(states_now[i])
            start_ref[h, blk, 0] = high[:, :HEAD_DIM]
            start_ref[h, blk, 1] = high[:, HEAD_DIM:]
            turn_h, turn_l = turn_ref[slot, n, 0], turn_ref[slot, n, 1]
            moved = dot(
                jnp.concatenate([turn_h, turn_l, turn_h], axis=1),
                jnp.concatenate([high, high, low], axis=0),
            )
            states_now[i] = jnp.concatenate(
                [moved[:, :HEAD_DIM], moved[:, HEAD_DIM:] + source_ref[slot, n]], axis=1
            )
            if n >= count - 2:
                x_ref[h] = states_now[i]
            yield

    def a_stream(it, first=0.0, last=1.0):
        return 7 * count // 4 + BASE + 1, solve(it), first, last

    def b_stream(it, first=0.0, last=1.0):
        return 9 * count, transit(it), first, last

    def c_stream(it, first=0.0, last=1.0):
        return count, compose(it), first, last

    def owner_of(pair, i):
        side = lax.rem(pair + core, 2)
        return peers // 2 - 2 + side + i * (3 - 2 * side)

    def send_map(pair, i, source):
        h = 2 * pair + i
        return pltpu.make_async_remote_copy(
            src_ref=maps.at[h],
            dst_ref=held.at[pair, source],
            send_sem=map_send.at[h],
            recv_sem=map_recv.at[pair, source],
            device_id={seq_axis: owner_of(pair, i)},
            device_id_type=MESH,
        )

    def send_state(pair, i, target):
        h = 2 * pair + i
        return pltpu.make_async_remote_copy(
            src_ref=states.at[pair, target],
            dst_ref=s_ref.at[h],
            send_sem=back_send.at[pair, target],
            recv_sem=back_recv.at[h],
            device_id={seq_axis: target},
            device_id_type=MESH,
        )

    def post(pair):
        for i in range(2):
            h = 2 * pair + i
            maps[h, 0] = x_ref[h, :, :HEAD_DIM].astype(BF16)
            maps[h, 1] = x_ref[h, :, HEAD_DIM:].astype(BF16)

            @pl.when((seq != owner_of(pair, i)) & (seq != peers - 1))
            def _():
                send_map(pair, i, seq).start()

            @pl.when(seq == owner_of(pair, i))
            def _():
                held[pair, seq] = maps[h]

    def chain(pair):
        for i in range(2):

            @pl.when(seq == owner_of(pair, i))
            def _():
                carry_ref[...] = jnp.zeros((HEAD_DIM, HEAD_DIM), F32)
                for k in range(peers - 1):

                    @pl.when(seq != k)
                    def _():
                        send_map(pair, i, k).wait_recv()

                    high, low = split(carry_ref[...])
                    turn = held[pair, k, 0]
                    state = held[pair, k, 1].astype(F32) + dot(
                        jnp.concatenate([turn, turn], axis=1),
                        jnp.concatenate([high, low], axis=0),
                    )
                    carry_ref[...] = state
                    states[pair, k + 1] = state.astype(BF16)

                    @pl.when(seq != k + 1)
                    def _():
                        send_state(pair, i, k + 1).start()

                    @pl.when(seq == k + 1)
                    def _():
                        s_ref[2 * pair + i] = states[pair, k + 1]

    @pl.when(seq == 0)
    def _():
        s_ref[...] = jnp.zeros(s_ref.shape, BF16)

    def wait_kv(pair):
        for i in range(2):
            for copy in fetch_kv(2 * pair + i):
                copy.wait()

    def after_values(pair, stream):
        for i in range(2):
            fetch_kv(2 * pair + i)[1].wait()
        yield from stream

    for h in range(2):
        fetch_kv(h)[0].wait()
    start_kv(2, heads)
    for h in range(heads):
        fetch_q(h).start()
    for n in range(4):
        load(n).start()
    for h in range(heads):
        fetch_g(h).start()
    weave(
        a_stream((0, 0), 0.0, 1.0),
        a_stream((0, 1), 0.5, 2.0),
        (9 * count, after_values(0, transit((0, 0))), 1.1, 2.1),
    )

    def step(pair, _):
        wait_kv(pair)
        weave(
            a_stream((pair, 0), 0.0, 1.0),
            b_stream((pair - 1, 1), 0.0, 1.0),
            c_stream((pair - 1, 0), 0.0, 1.0),
            a_stream((pair, 1), 1.05, 2.0),
            b_stream((pair, 0), 1.05, 2.0),
            c_stream((pair - 1, 1), 1.05, 2.0),
        )

        @pl.when(pair == 1)
        def _():
            pl.semaphore_wait(barrier, peers + 1)

        post(pair - 1)
        return 0

    lax.fori_loop(1, pairs, step, 0)
    weave(
        b_stream((pairs - 1, 1), 0.0, 9.0),
        c_stream((pairs - 1, 0), 0.0, 6.0),
        c_stream((pairs - 1, 1), 8.1, 9.1),
    )
    post(pairs - 1)
    for h in range(heads):
        fetch_q(h).wait()

    def read(pair, _):
        causal = iota((span, 2 * span), 1) % span <= iota((span, 2 * span), 0)
        for i in range(2):
            h = 2 * pair + i
            scores = []
            for blk in range(blocks):
                found = jnp.where(causal, dot_t(q_ref[h, blk], key_of(h, blk)), 0.0).astype(BF16)
                scores.append(jnp.concatenate([found, found], axis=1))
            drawn = [dot(score, stack_of(h, blk)) for blk, score in enumerate(scores)]
            for blk in range(blocks):
                kept = (q_ref[h, blk].astype(F32) - drawn[blk][:, :HEAD_DIM]).astype(BF16)
                if blk == 0:
                    m_ref[h, blk] = kept
                    o_ref[h, blk] = drawn[blk][:, HEAD_DIM:]
                    continue
                out = dot(kept, jnp.concatenate([start_ref[h, blk, 0], start_ref[h, blk, 1]], axis=1))
                m_ref[h, blk] = out[:, :HEAD_DIM].astype(BF16)
                o_ref[h, blk] = out[:, HEAD_DIM:] + drawn[blk][:, HEAD_DIM:]

        return 0

    def link(pair, _):
        chain(pair)
        return 0

    lax.fori_loop(0, 2, link, 0)
    lax.fori_loop(0, pairs, read, 0)
    for h in range(heads):
        fetch_g(h).wait()

    def wait_state(pair):
        for i in range(2):

            @pl.when((seq != owner_of(pair, i)) & (seq != 0))
            def _():
                send_state(pair, i, seq).wait_recv()

    def blend(pair, t):
        for i in range(2):
            h = 2 * pair + i
            query = q_ref[h, t].astype(F32)
            unit = lax.rsqrt(jnp.sum(query * query, axis=1, keepdims=True) + 1e-06)
            seen = unit * (o_ref[h, t] + dot(m_ref[h, t], s_ref[h]))
            scale = lax.rsqrt(jnp.mean(seen * seen, axis=1, keepdims=True) + 1e-06)
            gate = g_ref[h, t].astype(F32)
            mixed[t, h] = (seen * scale * (gate / (1.0 + jnp.exp(-gate)))).astype(BF16)

    def blend_pair(pair):
        wait_state(pair)
        for blk in range(blocks):
            blend(pair, blk)

    def settle(pair, _):
        blend_pair(pair)
        return 0

    lax.fori_loop(2, pairs, link, 0)
    lax.fori_loop(0, pairs - 1, settle, 0)

    sizes = [1, 1] + [2] * ((blocks - 4) // 2) + [1, 1]
    starts = [sum(sizes[:t]) for t in range(len(sizes))]

    def rows(t):
        return pl.ds(starts[t] * span, sizes[t] * span)

    def send(source, target, send_sem, recv_sem, t, device):
        return pltpu.make_async_remote_copy(
            src_ref=source.at[rows(t)],
            dst_ref=target.at[rows(t)],
            send_sem=send_sem.at[t],
            recv_sem=recv_sem.at[t],
            device_id={axis: device},
            device_id_type=MESH,
        )

    def far(t):
        return send(far_out, far_in, far_send, far_recv, t, sibling)

    def near(t):
        return send(near_out, near_in, near_send, near_recv, t, sibling)

    def cross(t):
        return send(cross_out, cross_in, cross_send, cross_recv, t, across)

    def pass_on(t):
        far(t).wait()
        cross_out[rows(t)] = (total[rows(t)] + far_in[rows(t)].astype(F32)).astype(BF16)
        cross(t).start()

    def mixed_of(t, first, last):
        return jnp.concatenate(
            [
                jnp.concatenate([mixed[starts[t] + b, h] for h in range(first, last)], axis=1)
                for b in range(sizes[t])
            ],
            axis=0,
        )

    def product(t, n):
        return dot(mixed_of(t, 0, heads), weight[n])

    def finish_piece(t):
        for b in range(sizes[t]):
            blend(pairs - 1, starts[t] + b)

    count_pieces = len(sizes)
    early = (heads - 2) * HEAD_DIM
    load(0).wait()
    total[rows(0)] = dot(mixed_of(0, 0, heads - 2), weight[0, :early, :])
    wait_state(pairs - 1)
    finish_piece(0)
    late = dot(mixed_of(0, heads - 2, heads), weight[0, early:, :])
    far_out[rows(0)] = (total[rows(0)] + late).astype(BF16)
    far(0).start()
    load(1).wait()
    finish_piece(1)
    total[rows(0)] = product(0, 1)
    for t in range(1, count_pieces):
        if t > 1:
            finish_piece(t)
        far_out[rows(t)] = product(t, 0).astype(BF16)
        far(t).start()
        pass_on(t - 1)
        total[rows(t)] = product(t, 1)
    load(2).wait()
    for t in range(count_pieces):
        near_out[rows(t)] = product(t, 2).astype(BF16)
        near(t).start()
        if t == 0:
            pass_on(count_pieces - 1)
    load(3).wait()
    for t in range(count_pieces):
        total[rows(t)] = product(t, 3)
    for t in range(count_pieces):
        near(t).wait()
        total[rows(t)] = total[rows(t)] + near_in[rows(t)].astype(F32)
    for t in range(count_pieces):
        cross(t).wait()
        y_ref[rows(t)] = (total[rows(t)] + cross_in[rows(t)].astype(F32)).astype(BF16)
    for pair in range(pairs):
        for i in range(2):

            @pl.when((seq != owner_of(pair, i)) & (seq != peers - 1))
            def _():
                send_map(pair, i, seq).wait_send()

            @pl.when(seq == owner_of(pair, i))
            def _():
                for k in range(1, peers):

                    @pl.when(seq != k)
                    def _():
                        send_state(pair, i, k).wait_send()


def fused(queries, keys, values, betas, gate, out_weight, seq_axis, axis):
    tokens, depth = queries.shape
    heads = depth // HEAD_DIM
    peers = lax.axis_size(seq_axis)
    width = out_weight.shape[1] // lax.axis_size(axis)
    blocks = tokens // SPAN
    batch = blocks // 2
    hbm = pl.BlockSpec(memory_space=pltpu.HBM)
    piece = (tokens, width)
    pieces = blocks // 2 + 2
    square = (HEAD_DIM, HEAD_DIM)
    wide = (HEAD_DIM, 2 * HEAD_DIM)
    two = (2,) + square
    pairs = heads // 2
    dma = pltpu.SemaphoreType.DMA
    per_head = (heads, blocks, SPAN, HEAD_DIM)
    both = (heads, 2, blocks, SPAN, HEAD_DIM)
    return pl.pallas_call(
        functools.partial(fused_kernel, seq_axis, peers, axis),
        in_specs=[hbm] * 6,
        out_specs=pl.BlockSpec(memory_space=pltpu.VMEM),
        out_shape=jax.ShapeDtypeStruct(piece, BF16),
        scratch_shapes=[
            pltpu.VMEM(betas.shape, F32),
            pltpu.VMEM(per_head, BF16),
            pltpu.VMEM(both, BF16),
            pltpu.VMEM(both, BF16),
            pltpu.VMEM(per_head, BF16),
            pltpu.VMEM((blocks, heads, 2 * SPAN), F32),
            pltpu.VMEM((heads, blocks, 3) + square, BF16),
            pltpu.VMEM((2, 2 * batch) + two, BF16),
            pltpu.VMEM((2, 2 * batch) + square, F32),
            pltpu.VMEM((heads,) + wide, F32),
            pltpu.VMEM((heads, blocks) + two, BF16),
            pltpu.VMEM((2, 2 * batch) + two, BF16),
            pltpu.VMEM((2, 2 * batch, BASE, 2 * SPAN), F32),
            pltpu.VMEM((2, 2, 2 * batch, 2 * SPAN), F32),
            pltpu.VMEM(square, F32),
            pltpu.VMEM((heads,) + two, BF16),
            pltpu.VMEM((pairs, peers) + two, BF16),
            pltpu.VMEM(square, F32),
            pltpu.VMEM((pairs, peers) + square, BF16),
            pltpu.VMEM((heads,) + square, BF16),
            pltpu.VMEM(per_head, F32),
            pltpu.VMEM(per_head, BF16),
            pltpu.VMEM((blocks, heads, SPAN, HEAD_DIM), BF16),
            pltpu.VMEM((4, depth, width), BF16),
            pltpu.VMEM(piece, F32),
        ]
        + [pltpu.VMEM(piece, BF16)] * 6
        + [
            dma,
            dma((2, heads)),
            dma((heads,)),
            dma((heads,)),
            dma((4,)),
            dma((heads,)),
            dma((pairs, peers)),
            dma((pairs, peers)),
            dma((heads,)),
        ]
        + [dma((pieces,))] * 6,
        compiler_params=pltpu.CompilerParams(
            collective_id=0, has_side_effects=True, vmem_limit_bytes=FUSED_LIMIT
        ),
    )(
        queries.reshape(blocks, SPAN, depth),
        keys.reshape(2, blocks, SPAN, depth),
        values.reshape(2, blocks, SPAN, depth),
        pltpu.with_memory_space_constraint(betas, pltpu.HBM),
        gate.reshape(blocks, SPAN, depth),
        out_weight,
    )


def start_state(maps, axis):
    peers, index = lax.axis_size(axis), lax.axis_index(axis)
    heads = maps.shape[0]
    held = lax.all_gather(maps, axis, axis=0, tiled=True)
    states = pl.pallas_call(
        functools.partial(chain_kernel, peers),
        out_shape=jax.ShapeDtypeStruct((held.shape[0], HEAD_DIM, HEAD_DIM), BF16),
        compiler_params=pltpu.CompilerParams(vmem_limit_bytes=VMEM_LIMIT),
    )(held)
    return lax.dynamic_slice_in_dim(states, index * heads, heads, 0)


def out_kernel(o_ref, m_ref, s_ref, g_ref, w_ref, y_ref, mixed_ref):
    @pl.when(pl.program_id(0) == 0)
    def _():
        for h in range(s_ref.shape[0]):
            cols = slice(h * HEAD_DIM, (h + 1) * HEAD_DIM)
            seen = o_ref[:, cols] + dot(m_ref[:, cols], s_ref[h])
            scale = lax.rsqrt(jnp.mean(seen * seen, axis=1, keepdims=True) + 1e-06)
            gate = g_ref[:, cols].astype(F32)
            mixed_ref[:, cols] = (seen * scale * (gate / (1.0 + jnp.exp(-gate)))).astype(BF16)

    y_ref[...] = dot(mixed_ref[...], w_ref[...]).astype(BF16)


def project(local, reach, states, gate, out_weight):
    tokens, width = local.shape
    total = out_weight.shape[1]
    tile = 512
    whole = pl.BlockSpec((tokens, width), lambda n: (0, 0))
    return pl.pallas_call(
        out_kernel,
        grid=(total // tile,),
        in_specs=[
            whole,
            whole,
            pl.BlockSpec(states.shape, lambda n: (0, 0, 0)),
            whole,
            pl.BlockSpec((width, tile), lambda n: (0, n)),
        ],
        out_specs=pl.BlockSpec((tokens, tile), lambda n: (0, n)),
        out_shape=jax.ShapeDtypeStruct((tokens, total), BF16),
        scratch_shapes=[pltpu.VMEM((tokens, width), BF16)],
        compiler_params=pltpu.CompilerParams(
            dimension_semantics=("arbitrary",), vmem_limit_bytes=VMEM_LIMIT
        ),
    )(local, reach, states, gate, out_weight)


def per_device(queries, keys, values, betas, gate, out_weight):
    heads, _, tokens = betas.shape
    peers, index = lax.axis_size("ctx"), lax.axis_size("head")
    if index == 4 and peers >= 4 and peers % 2 == 0 and heads % 8 == 0 and tokens % (8 * SPAN) == 0:
        return fused(queries, keys, values, betas, gate, out_weight, "ctx", "head")
    beta_cols = betas.transpose(2, 1, 0).reshape(2 * tokens, heads)
    local, reach, maps = mix(queries, keys, values, beta_cols)
    states = start_state(maps, "ctx")
    partial_sum = project(local, reach, states, gate, out_weight)
    return lax.psum_scatter(partial_sum, "head", scatter_dimension=1, tiled=True)


def solution(mesh):
    return jax.shard_map(
        per_device,
        mesh=mesh,
        in_specs=(
            P("ctx", "head"),
            P(None, "ctx", "head"),
            P(None, "ctx", "head"),
            P("head", None, "ctx"),
            P("ctx", "head"),
            P("head", None),
        ),
        out_specs=P("ctx", "head"),
        check_vma=False,
    )
```

```python
import functools

import jax
import jax.numpy as jnp
from jax import lax
from jax.experimental import pallas as pl
from jax.experimental.pallas import tpu as pltpu
from jax.sharding import PartitionSpec as P

HEAD_DIM = 128
SPAN = 64
BASE = 16
F32 = jnp.float32
BF16 = jnp.bfloat16
VMEM_LIMIT = 60 * 1024 * 1024
MESH = pl.DeviceIdType.MESH
PIECES = 4


def iota(shape, dim):
    return lax.broadcasted_iota(jnp.int32, shape, dim)


def split(a):
    high = a.astype(BF16)
    return high, (a - high.astype(F32)).astype(BF16)


def dot(a, b):
    return jnp.dot(a, b, preferred_element_type=F32)


def dot3(a, b):
    ah, al = split(a)
    bh, bl = split(b)
    return dot(jnp.concatenate([ah, al, ah], axis=1), jnp.concatenate([bh, bh, bl], axis=0))


def inverse(lowers, order):
    lane = iota((BASE, order), 1)
    compact = []
    for low in lowers:
        total = jnp.zeros((BASE, order), F32)
        for blk in range(order // BASE):
            total = jnp.where(lane // BASE == blk, low[blk * BASE : (blk + 1) * BASE, :], total)
        compact.append(total)
    inv = [(iota((BASE, order), 0) == lane % BASE).astype(F32) for _ in lowers]
    for j in range(BASE - 1):
        pick = (lane // BASE) * BASE + j
        for n, low in enumerate(compact):
            column = jnp.take_along_axis(low, pick, axis=1, mode="promise_in_bounds")
            inv[n] = inv[n] - column * inv[n][j : j + 1, :]
    row = iota((order, order), 0)
    col = iota((order, order), 1)
    width = BASE
    while width < order:
        corner = (row // (2 * width) == col // (2 * width)) & (row // width != col // width)
        diagonal = row // width == col // width
        second = (iota((width, order), 1) // width) % 2 == 1
        half = [dot3(jnp.where(second, t, 0.0), jnp.where(corner, low, 0.0)) for t, low in zip(inv, lowers)]
        full = [
            jnp.where(diagonal, jnp.concatenate([t] * (order // width), axis=0), 0.0) for t in inv
        ]
        fill = [dot3(y, e) for y, e in zip(half, full)]
        inv = [
            jnp.concatenate([jnp.where(second, 0.0, t), jnp.where(second, t, 0.0) - r], axis=0)
            for t, r in zip(inv, fill)
        ]
        width *= 2
    return inv


def mix_kernel(q_ref, k_ref, v_ref, b_ref, o_ref, m_ref, x_out, x_ref):
    heads = q_ref.shape[1] // HEAD_DIM
    span = q_ref.shape[0]
    order = 2 * span
    step = pl.program_id(0)

    @pl.when(step == 0)
    def _():
        start = (iota((HEAD_DIM, 2 * HEAD_DIM), 0) == iota((HEAD_DIM, 2 * HEAD_DIM), 1)).astype(F32)
        for h in range(heads):
            x_ref[h] = start

    row = iota((order, order), 0)
    col = iota((order, order), 1)
    strict = col < row
    weave = (row == 2 * (col % span) + col // span).astype(BF16)
    causal = iota((span, order), 1) <= 2 * iota((span, order), 0) + 1
    data = []
    lowers = []
    for h in range(heads):
        cols = slice(h * HEAD_DIM, (h + 1) * HEAD_DIM)
        query = q_ref[:, cols]
        pair = jnp.concatenate(
            [
                jnp.concatenate([k_ref[0, :, cols], v_ref[0, :, cols]], axis=1),
                jnp.concatenate([k_ref[1, :, cols], v_ref[1, :, cols]], axis=1),
            ],
            axis=0,
        )
        woven = dot(weave, pair)
        key = woven[:, :HEAD_DIM]
        value = woven[:, HEAD_DIM:]
        key_b = key.astype(BF16)
        norm = lax.rsqrt(jnp.sum(key * key, axis=1, keepdims=True) + 1e-06)
        beta = b_ref[:, h : h + 1]
        both = jnp.concatenate([key_b, query], axis=0)
        gram = lax.dot_general(both, key_b, (((1,), (1,)), ((), ())), preferred_element_type=F32)
        weight = beta * norm * norm
        lowers.append(jnp.where(strict, weight * gram[:order], 0.0))
        scores = jnp.where(causal, gram[order:], 0.0).astype(BF16)
        qf = query.astype(F32)
        q_norm = lax.rsqrt(jnp.sum(qf * qf, axis=1, keepdims=True) + 1e-06)
        readers = jnp.concatenate([key.T.astype(BF16), scores], axis=0)
        data.append((both, readers, beta * norm * value, weight, q_norm))
    solved = inverse(lowers, order)
    seen = []
    for h in range(heads):
        both = data[h][0]
        high, low = split(x_ref[h])
        seen.append(
            dot(jnp.concatenate([both, both], axis=1), jnp.concatenate([high, low], axis=0))
        )
    writes = []
    for h in range(heads):
        _, _, scaled, weight, _ = data[h]
        gap = -weight * seen[h][:order]
        gap = jnp.concatenate([gap[:, :HEAD_DIM], gap[:, HEAD_DIM:] + scaled], axis=1)
        writes.append(dot3(solved[h], gap))
    for h in range(heads):
        cols = slice(h * HEAD_DIM, (h + 1) * HEAD_DIM)
        readers, q_norm = data[h][1], data[h][4]
        high, low = split(writes[h])
        change = dot(
            jnp.concatenate([readers, readers], axis=1), jnp.concatenate([high, low], axis=0)
        )
        x_ref[h] = x_ref[h] + change[:HEAD_DIM]
        out = q_norm * (seen[h][order:] + change[HEAD_DIM:])
        m_ref[:, cols] = out[:, :HEAD_DIM].astype(BF16)
        o_ref[:, cols] = out[:, HEAD_DIM:]

    @pl.when(step == pl.num_programs(0) - 1)
    def _():
        for h in range(heads):
            x_out[h] = x_ref[h].astype(BF16)


def mix(queries, keys, values, beta_cols):
    tokens, width = queries.shape
    heads = width // HEAD_DIM
    return pl.pallas_call(
        mix_kernel,
        grid=(tokens // SPAN,),
        in_specs=[
            pl.BlockSpec((SPAN, width), lambda c: (c, 0)),
            pl.BlockSpec((2, SPAN, width), lambda c: (0, c, 0)),
            pl.BlockSpec((2, SPAN, width), lambda c: (0, c, 0)),
            pl.BlockSpec((2 * SPAN, heads), lambda c: (c, 0)),
        ],
        out_specs=[
            pl.BlockSpec((SPAN, width), lambda c: (c, 0)),
            pl.BlockSpec((SPAN, width), lambda c: (c, 0)),
            pl.BlockSpec((heads, HEAD_DIM, 2 * HEAD_DIM), lambda c: (0, 0, 0)),
        ],
        out_shape=[
            jax.ShapeDtypeStruct((tokens, width), F32),
            jax.ShapeDtypeStruct((tokens, width), BF16),
            jax.ShapeDtypeStruct((heads, HEAD_DIM, 2 * HEAD_DIM), BF16),
        ],
        scratch_shapes=[pltpu.VMEM((heads, HEAD_DIM, 2 * HEAD_DIM), F32)],
        compiler_params=pltpu.CompilerParams(
            dimension_semantics=("arbitrary",), vmem_limit_bytes=VMEM_LIMIT
        ),
    )(queries, keys, values, beta_cols)


def chain_kernel(peers, x_ref, s_ref):
    heads = x_ref.shape[0] // peers
    for h in range(heads):
        state = jnp.zeros((HEAD_DIM, HEAD_DIM), F32)
        for k in range(peers):
            s_ref[k * heads + h] = state.astype(BF16)
            if k < peers - 1:
                maps = x_ref[k * heads + h]
                turn = maps[:, :HEAD_DIM]
                high, low = split(state)
                state = maps[:, HEAD_DIM:].astype(F32) + dot(
                    jnp.concatenate([turn, turn], axis=1), jnp.concatenate([high, low], axis=0)
                )


FUSED_LIMIT = 52 * 1024 * 1024


def dot_t(a, b):
    return lax.dot_general(a, b, (((1,), (1,)), ((), ())), preferred_element_type=F32)


def pair_dot(a, low, high_b, low_b):
    rows = a.shape[0]
    both = dot(jnp.concatenate([a, low], axis=0), jnp.concatenate([high_b, low_b], axis=1))
    width = high_b.shape[1]
    return both[:rows, :width] + both[rows:, :width] + both[:rows, width:]


def weave(*streams):
    order = []
    for n, (count, _, first, last) in enumerate(streams):
        order += [(first + (last - first) * (k + 0.5) / count, n) for k in range(count)]
    for _, n in sorted(order):
        next(streams[n][1], None)
    for _, stream, _, _ in streams:
        for _ in stream:
            pass


def base_solve(lowers, span):
    order = 2 * span
    base = BASE // 2
    lane = iota((base, order), 1)
    group = (lane % span) // base
    row16, lane16 = iota((BASE, order), 0), iota((BASE, order), 1)
    group16 = (lane16 % span) // base
    row_tok, lane_tok = row16 % base, lane16 % base
    before = (lane_tok < row_tok) | ((lane_tok == row_tok) & (lane16 // span < row16 // base))
    compact = []
    for n, low in enumerate(lowers):
        halves = []
        for j in range(2):
            total = jnp.zeros((base, order), F32)
            for blk in range(span // base):
                start = j * span + blk * base
                total = jnp.where(group == blk, low[start : start + base, :], total)
            halves.append(total)
        compact.append(jnp.where(before, jnp.concatenate(halves, axis=0), 0.0))
        if n % 2:
            yield
    own = (row16 % base == lane16 % base) & (row16 // base == lane16 // span)
    inv = [own.astype(F32) for _ in lowers]
    for s in range(BASE - 1):
        t, j = s // 2, s % 2
        pick = j * span + group16 * base + t
        for n, low in enumerate(compact):
            column = jnp.take_along_axis(low, pick, axis=1, mode="promise_in_bounds")
            inv[n] = inv[n] - column * inv[n][j * base + t : j * base + t + 1, :]
        yield
    return inv


def merge(inv, pieces, span):
    order = 2 * span
    tok_r = iota((order, order), 0) % span
    tok_c = iota((order, order), 1) % span
    width = BASE // 2
    zero = jnp.zeros((), BF16)
    while width < span:
        last = 2 * width == span
        diagonal = tok_r // width == tok_c // width
        corner = (tok_r // (2 * width) == tok_c // (2 * width)) & (tok_r // width != tok_c // width)
        second = ((iota((2 * width, order), 1) % span) // width) % 2 == 1
        odd, half, fill, wide, merged = [], [], [], [], []
        for n, t in enumerate(inv):
            odd.append(jnp.where(second, t, 0.0))
            th, tl = split(odd[n])
            high, low = pieces(n)
            if last:
                y = jnp.where(second, 0.0, pair_dot(th, tl, high, low))
            else:
                y = pair_dot(th, tl, jnp.where(corner, high, zero), jnp.where(corner, low, zero))
            half.append(y)
            parts = []
            for j in range(2):
                part = t[j * width : (j + 1) * width]
                if width < 16:
                    part = jnp.concatenate([part] * (16 // width), axis=0)
                parts.append((split(part), span // part.shape[0]))
            full = [
                jnp.concatenate([p[k] for p, count in parts for _ in range(count)], axis=0)
                for k in range(2)
            ]
            if not last:
                full = [jnp.where(diagonal, f, zero) for f in full]
            wide.append(full)
            yield
        for y, full in zip(half, wide):
            yh, yl = split(y)
            r = pair_dot(yh, yl, full[0], full[1])
            fill.append(jnp.where(second, 0.0, r) if last else r)
            yield
        for t, o, r in zip(inv, odd, fill):
            even, lower = t - o, o - r
            merged.append(
                jnp.concatenate(
                    [even[:width], lower[:width], even[width:], lower[width:]], axis=0
                )
            )
        inv = merged
        width *= 2
    return inv


def fused_kernel(
    seq_axis, peers, axis, q_hbm, k_hbm, v_hbm, b_hbm, g_hbm, w_hbm, y_ref,
    b_ref, q_ref, k_ref, v_ref, g_ref, beta_ref, stack_ref, turn_ref, source_ref, x_ref, start_ref,
    low_ref, inv_ref, weight_ref, eye_ref,
    maps, held, carry_ref, states, s_ref, o_ref, m_ref,
    mixed, weight, total, far_out, far_in, near_out, near_in, cross_out, cross_in,
    b_sem, kv_sem, q_sem, g_sem, load_sem, map_send, map_recv, back_send, back_recv,
    far_send, far_recv, near_send, near_recv, cross_send, cross_recv,
):
    heads, blocks, span = q_ref.shape[0], q_ref.shape[1], q_ref.shape[2]
    pairs = heads // 2
    parts = 2
    batch = blocks // parts
    seq = lax.axis_index(seq_axis)
    me = lax.axis_index(axis)
    chip, core = me // 2, me % 2
    sibling = 2 * chip + 1 - core
    across = 2 * (1 - chip) + core
    beyond = 2 * (1 - chip) + 1 - core
    width = y_ref.shape[1]

    def columns(h):
        return pl.ds(pl.multiple_of(h * HEAD_DIM, HEAD_DIM), HEAD_DIM)

    def fetch_kv(h):
        return (
            pltpu.make_async_copy(k_hbm.at[:, :, :, columns(h)], k_ref.at[h], kv_sem.at[0, h]),
            pltpu.make_async_copy(v_hbm.at[:, :, :, columns(h)], v_ref.at[h], kv_sem.at[1, h]),
        )

    def fetch_q(h):
        return pltpu.make_async_copy(q_hbm.at[:, :, columns(h)], q_ref.at[h], q_sem.at[h])

    def fetch_g(h):
        return pltpu.make_async_copy(g_hbm.at[:, :, columns(h)], g_ref.at[h], g_sem.at[h])

    def load(n):
        owner = (beyond, across, sibling, me)[n]
        return pltpu.make_async_copy(
            w_hbm.at[:, pl.ds(pl.multiple_of(owner * width, width), width)],
            weight.at[n],
            load_sem.at[n],
        )

    def start_kv(first, last):
        for n in range(2):
            for h in range(first, last):
                fetch_kv(h)[n].start()

    fetch_b = pltpu.make_async_copy(b_hbm, b_ref, b_sem)
    fetch_b.start()
    start_kv(0, 2)
    barrier = pltpu.get_barrier_semaphore()
    for other in (sibling, across):
        pl.semaphore_signal(barrier, inc=1, device_id={axis: other}, device_id_type=MESH)
    for away in range(1, peers):
        pl.semaphore_signal(
            barrier,
            inc=1,
            device_id={seq_axis: lax.rem(seq + away, peers)},
            device_id_type=MESH,
        )

    eye_ref[...] = (iota(eye_ref.shape, 0) == iota(eye_ref.shape, 1)).astype(F32)
    fetch_b.wait()
    for blk in range(blocks):
        window = slice(blk * span, (blk + 1) * span)
        beta_ref[blk] = jnp.concatenate([b_ref[:, 0, window], b_ref[:, 1, window]], axis=1)

    def place(it, n):
        pair, part = it
        return 2 * pair + n % 2, part * batch + n // 2

    count = 2 * batch

    def key_of(h, blk):
        return jnp.concatenate([k_ref[h, 0, blk], k_ref[h, 1, blk]], axis=0)

    def stack_of(h, blk):
        none = jnp.zeros((HEAD_DIM, HEAD_DIM), BF16)
        return jnp.concatenate(
            [
                jnp.concatenate([stack_ref[h, blk, 0], stack_ref[h, blk, 2]], axis=1),
                jnp.concatenate([stack_ref[h, blk, 1], none], axis=1),
            ],
            axis=0,
        )

    def solve(it):
        slot = it[1]
        grams, squares = [], []
        for n in range(count):
            key = key_of(*place(it, n))
            grams.append(dot_t(key, key))
            if n % 2:
                yield
        for n, g in enumerate(grams):
            squares.append(jnp.sum(eye_ref[...] * g, axis=0, keepdims=True))
            if n % 4 == 3:
                yield
        beta = jnp.concatenate(
            [beta_ref[place(it, n)[1], pl.ds(place(it, n)[0], 1), :] for n in range(count)], axis=0
        )
        norm = lax.rsqrt(jnp.concatenate(squares, axis=0) + 1e-06)
        value_weight = beta * norm
        weight_rows = value_weight * norm
        weight_ref[slot, 0] = weight_rows
        weight_ref[slot, 1] = value_weight
        weight_cols = weight_rows.T
        yield
        lowers = []
        for n, g in enumerate(grams):
            low = weight_cols[:, n : n + 1] * g
            lowers.append(low)
            low_ref[slot, n, 0], low_ref[slot, n, 1] = split(low)
            if n % 2:
                yield
        inv = yield from base_solve(lowers, span)
        for n in range(count):
            inv_ref[slot, n] = inv[n]

    def transit(it):
        slot = it[1]

        def pieces(n):
            return low_ref[slot, n, 0], low_ref[slot, n, 1]

        solved = yield from merge([inv_ref[slot, n] for n in range(count)], pieces, span)
        turns, writes, changes = [], [], []
        for n in range(count):
            h, blk = place(it, n)
            th, tl = split(solved[n] * weight_ref[slot, 0, n : n + 1, :])
            tv = (solved[n] * weight_ref[slot, 1, n : n + 1, :]).astype(BF16)
            key = key_of(h, blk)
            value = jnp.concatenate([v_ref[h, 0, blk], v_ref[h, 1, blk]], axis=0)
            turns.append(
                dot(jnp.concatenate([th, tl], axis=1), jnp.concatenate([key, key], axis=0))
            )
            writes.append(dot(tv, value))
            yield
        for n in range(count):
            h, blk = place(it, n)
            turn_h, turn_l = split(turns[n])
            stack_ref[h, blk, 0], stack_ref[h, blk, 1] = turn_h, turn_l
            stack_ref[h, blk, 2] = writes[n].astype(BF16)
            stack = stack_of(h, blk)
            key_t = key_of(h, blk).T
            changes.append(dot(jnp.concatenate([key_t, key_t], axis=1), stack))
            yield
        for n in range(count):
            step = eye_ref[...] - changes[n][:, :HEAD_DIM]
            turn_ref[slot, n, 0], turn_ref[slot, n, 1] = split(step)
            source_ref[slot, n] = changes[n][:, HEAD_DIM:]
            yield

    def compose(it):
        slot = it[1]
        pair, _ = it
        states_now = [None if it[1] == 0 else x_ref[2 * pair + i] for i in range(2)]
        for n in range(count):
            h, blk = place(it, n)
            i = n % 2
            if blk == 0:
                turn_h, turn_l = turn_ref[slot, n, 0], turn_ref[slot, n, 1]
                states_now[i] = jnp.concatenate(
                    [turn_h.astype(F32) + turn_l.astype(F32), source_ref[slot, n]], axis=1
                )
                yield
                continue
            high, low = split(states_now[i])
            start_ref[h, blk, 0] = high[:, :HEAD_DIM]
            start_ref[h, blk, 1] = high[:, HEAD_DIM:]
            turn_h, turn_l = turn_ref[slot, n, 0], turn_ref[slot, n, 1]
            moved = dot(
                jnp.concatenate([turn_h, turn_l, turn_h], axis=1),
                jnp.concatenate([high, high, low], axis=0),
            )
            states_now[i] = jnp.concatenate(
                [moved[:, :HEAD_DIM], moved[:, HEAD_DIM:] + source_ref[slot, n]], axis=1
            )
            if n >= count - 2:
                x_ref[h] = states_now[i]
            yield

    def a_stream(it, first=0.0, last=1.0):
        return 7 * count // 4 + BASE + 1, solve(it), first, last

    def b_stream(it, first=0.0, last=1.0):
        return 9 * count, transit(it), first, last

    def c_stream(it, first=0.0, last=1.0):
        return count, compose(it), first, last

    def owner_of(pair, i):
        side = lax.rem(pair + core, 2)
        return peers // 2 - 2 + side + i * (3 - 2 * side)

    def send_map(pair, i, source):
        h = 2 * pair + i
        return pltpu.make_async_remote_copy(
            src_ref=maps.at[h],
            dst_ref=held.at[pair, source],
            send_sem=map_send.at[h],
            recv_sem=map_recv.at[pair, source],
            device_id={seq_axis: owner_of(pair, i)},
            device_id_type=MESH,
        )

    def send_state(pair, i, target):
        h = 2 * pair + i
        return pltpu.make_async_remote_copy(
            src_ref=states.at[pair, target],
            dst_ref=s_ref.at[h],
            send_sem=back_send.at[pair, target],
            recv_sem=back_recv.at[h],
            device_id={seq_axis: target},
            device_id_type=MESH,
        )

    def post(pair):
        for i in range(2):
            h = 2 * pair + i
            maps[h, 0] = x_ref[h, :, :HEAD_DIM].astype(BF16)
            maps[h, 1] = x_ref[h, :, HEAD_DIM:].astype(BF16)

            @pl.when((seq != owner_of(pair, i)) & (seq != peers - 1))
            def _():
                send_map(pair, i, seq).start()

            @pl.when(seq == owner_of(pair, i))
            def _():
                held[pair, seq] = maps[h]

    def chain(pair):
        for i in range(2):

            @pl.when(seq == owner_of(pair, i))
            def _():
                carry_ref[...] = jnp.zeros((HEAD_DIM, HEAD_DIM), F32)
                for k in range(peers - 1):

                    @pl.when(seq != k)
                    def _():
                        send_map(pair, i, k).wait_recv()

                    high, low = split(carry_ref[...])
                    turn = held[pair, k, 0]
                    state = held[pair, k, 1].astype(F32) + dot(
                        jnp.concatenate([turn, turn], axis=1),
                        jnp.concatenate([high, low], axis=0),
                    )
                    carry_ref[...] = state
                    states[pair, k + 1] = state.astype(BF16)

                    @pl.when(seq != k + 1)
                    def _():
                        send_state(pair, i, k + 1).start()

                    @pl.when(seq == k + 1)
                    def _():
                        s_ref[2 * pair + i] = states[pair, k + 1]

    @pl.when(seq == 0)
    def _():
        s_ref[...] = jnp.zeros(s_ref.shape, BF16)

    def wait_kv(pair):
        for i in range(2):
            for copy in fetch_kv(2 * pair + i):
                copy.wait()

    def after_values(pair, stream):
        for i in range(2):
            fetch_kv(2 * pair + i)[1].wait()
        yield from stream

    for h in range(2):
        fetch_kv(h)[0].wait()
    start_kv(2, heads)
    for h in range(heads):
        fetch_q(h).start()
    for n in range(4):
        load(n).start()
    for h in range(heads):
        fetch_g(h).start()
    weave(
        a_stream((0, 0), 0.0, 1.0),
        a_stream((0, 1), 0.8, 2.0),
        (9 * count, after_values(0, transit((0, 0))), 1.0, 2.1),
    )

    def step(pair, _):
        wait_kv(pair)
        weave(
            a_stream((pair, 0), 0.0, 1.0),
            b_stream((pair - 1, 1), 0.0, 1.0),
            c_stream((pair - 1, 0), 0.0, 1.0),
            a_stream((pair, 1), 1.05, 2.0),
            b_stream((pair, 0), 1.05, 2.0),
            c_stream((pair - 1, 1), 1.05, 2.0),
        )

        @pl.when(pair == 1)
        def _():
            pl.semaphore_wait(barrier, peers + 1)

        post(pair - 1)
        return 0

    lax.fori_loop(1, pairs, step, 0)
    weave(
        b_stream((pairs - 1, 1), 0.0, 9.0),
        c_stream((pairs - 1, 0), 0.0, 6.0),
        c_stream((pairs - 1, 1), 8.1, 9.1),
    )
    post(pairs - 1)
    for h in range(heads):
        fetch_q(h).wait()

    def read(pair, _):
        causal = iota((span, 2 * span), 1) % span <= iota((span, 2 * span), 0)
        for i in range(2):
            h = 2 * pair + i
            scores = []
            for blk in range(blocks):
                found = jnp.where(causal, dot_t(q_ref[h, blk], key_of(h, blk)), 0.0).astype(BF16)
                scores.append(jnp.concatenate([found, found], axis=1))
            drawn = [dot(score, stack_of(h, blk)) for blk, score in enumerate(scores)]
            for blk in range(blocks):
                kept = (q_ref[h, blk].astype(F32) - drawn[blk][:, :HEAD_DIM]).astype(BF16)
                if blk == 0:
                    m_ref[h, blk] = kept
                    o_ref[h, blk] = drawn[blk][:, HEAD_DIM:]
                    continue
                out = dot(kept, jnp.concatenate([start_ref[h, blk, 0], start_ref[h, blk, 1]], axis=1))
                m_ref[h, blk] = out[:, :HEAD_DIM].astype(BF16)
                o_ref[h, blk] = out[:, HEAD_DIM:] + drawn[blk][:, HEAD_DIM:]

        return 0

    def link(pair, _):
        chain(pair)
        return 0

    lax.fori_loop(0, 2, link, 0)
    lax.fori_loop(0, pairs - 1, read, 0)
    lax.fori_loop(2, pairs, link, 0)
    read(pairs - 1, 0)
    for h in range(heads):
        fetch_g(h).wait()

    def wait_state(pair):
        for i in range(2):

            @pl.when((seq != owner_of(pair, i)) & (seq != 0))
            def _():
                send_state(pair, i, seq).wait_recv()

    def blend(pair, t):
        for i in range(2):
            h = 2 * pair + i
            query = q_ref[h, t].astype(F32)
            unit = lax.rsqrt(jnp.sum(query * query, axis=1, keepdims=True) + 1e-06)
            seen = unit * (o_ref[h, t] + dot(m_ref[h, t], s_ref[h]))
            scale = lax.rsqrt(jnp.mean(seen * seen, axis=1, keepdims=True) + 1e-06)
            gate = g_ref[h, t].astype(F32)
            mixed[t, h] = (seen * scale * (gate / (1.0 + jnp.exp(-gate)))).astype(BF16)

    def blend_pair(pair):
        wait_state(pair)
        for blk in range(blocks):
            blend(pair, blk)

    def settle(pair, _):
        blend_pair(pair)
        return 0

    lax.fori_loop(0, pairs - 1, settle, 0)

    sizes = [1, 1] + [2] * ((blocks - 4) // 2) + [1, 1]
    starts = [sum(sizes[:t]) for t in range(len(sizes))]

    def rows(t):
        return pl.ds(starts[t] * span, sizes[t] * span)

    def send(source, target, send_sem, recv_sem, t, device):
        return pltpu.make_async_remote_copy(
            src_ref=source.at[rows(t)],
            dst_ref=target.at[rows(t)],
            send_sem=send_sem.at[t],
            recv_sem=recv_sem.at[t],
            device_id={axis: device},
            device_id_type=MESH,
        )

    def far(t):
        return send(far_out, far_in, far_send, far_recv, t, sibling)

    def near(t):
        return send(near_out, near_in, near_send, near_recv, t, sibling)

    def cross(t):
        return send(cross_out, cross_in, cross_send, cross_recv, t, across)

    def pass_on(t):
        far(t).wait()
        cross_out[rows(t)] = (total[rows(t)] + far_in[rows(t)].astype(F32)).astype(BF16)
        cross(t).start()

    def mixed_of(t, first, last):
        return jnp.concatenate(
            [
                jnp.concatenate([mixed[starts[t] + b, h] for h in range(first, last)], axis=1)
                for b in range(sizes[t])
            ],
            axis=0,
        )

    def product(t, n):
        return dot(mixed_of(t, 0, heads), weight[n])

    def finish_piece(t):
        for b in range(sizes[t]):
            blend(pairs - 1, starts[t] + b)

    count_pieces = len(sizes)
    early = (heads - 2) * HEAD_DIM
    load(0).wait()
    total[rows(0)] = dot(mixed_of(0, 0, heads - 2), weight[0, :early, :])
    wait_state(pairs - 1)
    finish_piece(0)
    late = dot(mixed_of(0, heads - 2, heads), weight[0, early:, :])
    far_out[rows(0)] = (total[rows(0)] + late).astype(BF16)
    far(0).start()
    load(1).wait()
    finish_piece(1)
    total[rows(0)] = product(0, 1)
    for t in range(1, count_pieces):
        if t > 1:
            finish_piece(t)
        far_out[rows(t)] = product(t, 0).astype(BF16)
        far(t).start()
        pass_on(t - 1)
        total[rows(t)] = product(t, 1)
    load(2).wait()
    for t in range(count_pieces):
        near_out[rows(t)] = product(t, 2).astype(BF16)
        near(t).start()
        if t == 0:
            pass_on(count_pieces - 1)
    load(3).wait()
    for t in range(count_pieces):
        total[rows(t)] = product(t, 3)
    for t in range(count_pieces):
        near(t).wait()
        total[rows(t)] = total[rows(t)] + near_in[rows(t)].astype(F32)
    for t in range(count_pieces):
        cross(t).wait()
        y_ref[rows(t)] = (total[rows(t)] + cross_in[rows(t)].astype(F32)).astype(BF16)
    for pair in range(pairs):
        for i in range(2):

            @pl.when((seq != owner_of(pair, i)) & (seq != peers - 1))
            def _():
                send_map(pair, i, seq).wait_send()

            @pl.when(seq == owner_of(pair, i))
            def _():
                for k in range(1, peers):

                    @pl.when(seq != k)
                    def _():
                        send_state(pair, i, k).wait_send()


def fused(queries, keys, values, betas, gate, out_weight, seq_axis, axis):
    tokens, depth = queries.shape
    heads = depth // HEAD_DIM
    peers = lax.axis_size(seq_axis)
    width = out_weight.shape[1] // lax.axis_size(axis)
    blocks = tokens // SPAN
    batch = blocks // 2
    hbm = pl.BlockSpec(memory_space=pltpu.HBM)
    piece = (tokens, width)
    pieces = blocks // 2 + 2
    square = (HEAD_DIM, HEAD_DIM)
    wide = (HEAD_DIM, 2 * HEAD_DIM)
    two = (2,) + square
    pairs = heads // 2
    dma = pltpu.SemaphoreType.DMA
    per_head = (heads, blocks, SPAN, HEAD_DIM)
    both = (heads, 2, blocks, SPAN, HEAD_DIM)
    return pl.pallas_call(
        functools.partial(fused_kernel, seq_axis, peers, axis),
        in_specs=[hbm] * 6,
        out_specs=pl.BlockSpec(memory_space=pltpu.VMEM),
        out_shape=jax.ShapeDtypeStruct(piece, BF16),
        scratch_shapes=[
            pltpu.VMEM(betas.shape, F32),
            pltpu.VMEM(per_head, BF16),
            pltpu.VMEM(both, BF16),
            pltpu.VMEM(both, BF16),
            pltpu.VMEM(per_head, BF16),
            pltpu.VMEM((blocks, heads, 2 * SPAN), F32),
            pltpu.VMEM((heads, blocks, 3) + square, BF16),
            pltpu.VMEM((2, 2 * batch) + two, BF16),
            pltpu.VMEM((2, 2 * batch) + square, F32),
            pltpu.VMEM((heads,) + wide, F32),
            pltpu.VMEM((heads, blocks) + two, BF16),
            pltpu.VMEM((2, 2 * batch) + two, BF16),
            pltpu.VMEM((2, 2 * batch, BASE, 2 * SPAN), F32),
            pltpu.VMEM((2, 2, 2 * batch, 2 * SPAN), F32),
            pltpu.VMEM(square, F32),
            pltpu.VMEM((heads,) + two, BF16),
            pltpu.VMEM((pairs, peers) + two, BF16),
            pltpu.VMEM(square, F32),
            pltpu.VMEM((pairs, peers) + square, BF16),
            pltpu.VMEM((heads,) + square, BF16),
            pltpu.VMEM(per_head, F32),
            pltpu.VMEM(per_head, BF16),
            pltpu.VMEM((blocks, heads, SPAN, HEAD_DIM), BF16),
            pltpu.VMEM((4, depth, width), BF16),
            pltpu.VMEM(piece, F32),
        ]
        + [pltpu.VMEM(piece, BF16)] * 6
        + [
            dma,
            dma((2, heads)),
            dma((heads,)),
            dma((heads,)),
            dma((4,)),
            dma((heads,)),
            dma((pairs, peers)),
            dma((pairs, peers)),
            dma((heads,)),
        ]
        + [dma((pieces,))] * 6,
        compiler_params=pltpu.CompilerParams(
            collective_id=0, has_side_effects=True, vmem_limit_bytes=FUSED_LIMIT
        ),
    )(
        queries.reshape(blocks, SPAN, depth),
        keys.reshape(2, blocks, SPAN, depth),
        values.reshape(2, blocks, SPAN, depth),
        pltpu.with_memory_space_constraint(betas, pltpu.HBM),
        gate.reshape(blocks, SPAN, depth),
        out_weight,
    )


def start_state(maps, axis):
    peers, index = lax.axis_size(axis), lax.axis_index(axis)
    heads = maps.shape[0]
    held = lax.all_gather(maps, axis, axis=0, tiled=True)
    states = pl.pallas_call(
        functools.partial(chain_kernel, peers),
        out_shape=jax.ShapeDtypeStruct((held.shape[0], HEAD_DIM, HEAD_DIM), BF16),
        compiler_params=pltpu.CompilerParams(vmem_limit_bytes=VMEM_LIMIT),
    )(held)
    return lax.dynamic_slice_in_dim(states, index * heads, heads, 0)


def out_kernel(o_ref, m_ref, s_ref, g_ref, w_ref, y_ref, mixed_ref):
    @pl.when(pl.program_id(0) == 0)
    def _():
        for h in range(s_ref.shape[0]):
            cols = slice(h * HEAD_DIM, (h + 1) * HEAD_DIM)
            seen = o_ref[:, cols] + dot(m_ref[:, cols], s_ref[h])
            scale = lax.rsqrt(jnp.mean(seen * seen, axis=1, keepdims=True) + 1e-06)
            gate = g_ref[:, cols].astype(F32)
            mixed_ref[:, cols] = (seen * scale * (gate / (1.0 + jnp.exp(-gate)))).astype(BF16)

    y_ref[...] = dot(mixed_ref[...], w_ref[...]).astype(BF16)


def project(local, reach, states, gate, out_weight):
    tokens, width = local.shape
    total = out_weight.shape[1]
    tile = 512
    whole = pl.BlockSpec((tokens, width), lambda n: (0, 0))
    return pl.pallas_call(
        out_kernel,
        grid=(total // tile,),
        in_specs=[
            whole,
            whole,
            pl.BlockSpec(states.shape, lambda n: (0, 0, 0)),
            whole,
            pl.BlockSpec((width, tile), lambda n: (0, n)),
        ],
        out_specs=pl.BlockSpec((tokens, tile), lambda n: (0, n)),
        out_shape=jax.ShapeDtypeStruct((tokens, total), BF16),
        scratch_shapes=[pltpu.VMEM((tokens, width), BF16)],
        compiler_params=pltpu.CompilerParams(
            dimension_semantics=("arbitrary",), vmem_limit_bytes=VMEM_LIMIT
        ),
    )(local, reach, states, gate, out_weight)


def per_device(queries, keys, values, betas, gate, out_weight):
    heads, _, tokens = betas.shape
    peers, index = lax.axis_size("ctx"), lax.axis_size("head")
    if index == 4 and peers >= 4 and peers % 2 == 0 and heads % 8 == 0 and tokens % (8 * SPAN) == 0:
        return fused(queries, keys, values, betas, gate, out_weight, "ctx", "head")
    beta_cols = betas.transpose(2, 1, 0).reshape(2 * tokens, heads)
    local, reach, maps = mix(queries, keys, values, beta_cols)
    states = start_state(maps, "ctx")
    partial_sum = project(local, reach, states, gate, out_weight)
    return lax.psum_scatter(partial_sum, "head", scatter_dimension=1, tiled=True)


def solution(mesh):
    return jax.shard_map(
        per_device,
        mesh=mesh,
        in_specs=(
            P("ctx", "head"),
            P(None, "ctx", "head"),
            P(None, "ctx", "head"),
            P("head", None, "ctx"),
            P("ctx", "head"),
            P("head", None),
        ),
        out_specs=P("ctx", "head"),
        check_vma=False,
    )
```

```python
import functools

import jax
import jax.numpy as jnp
from jax import lax
from jax.experimental import pallas as pl
from jax.experimental.pallas import tpu as pltpu
from jax.sharding import PartitionSpec as P

HEAD_DIM = 128
SPAN = 64
BASE = 16
F32 = jnp.float32
BF16 = jnp.bfloat16
VMEM_LIMIT = 60 * 1024 * 1024
MESH = pl.DeviceIdType.MESH
PIECES = 4


def iota(shape, dim):
    return lax.broadcasted_iota(jnp.int32, shape, dim)


def split(a):
    high = a.astype(BF16)
    return high, (a - high.astype(F32)).astype(BF16)


def dot(a, b):
    return jnp.dot(a, b, preferred_element_type=F32)


def dot3(a, b):
    ah, al = split(a)
    bh, bl = split(b)
    return dot(jnp.concatenate([ah, al, ah], axis=1), jnp.concatenate([bh, bh, bl], axis=0))


def inverse(lowers, order):
    lane = iota((BASE, order), 1)
    compact = []
    for low in lowers:
        total = jnp.zeros((BASE, order), F32)
        for blk in range(order // BASE):
            total = jnp.where(lane // BASE == blk, low[blk * BASE : (blk + 1) * BASE, :], total)
        compact.append(total)
    inv = [(iota((BASE, order), 0) == lane % BASE).astype(F32) for _ in lowers]
    for j in range(BASE - 1):
        pick = (lane // BASE) * BASE + j
        for n, low in enumerate(compact):
            column = jnp.take_along_axis(low, pick, axis=1, mode="promise_in_bounds")
            inv[n] = inv[n] - column * inv[n][j : j + 1, :]
    row = iota((order, order), 0)
    col = iota((order, order), 1)
    width = BASE
    while width < order:
        corner = (row // (2 * width) == col // (2 * width)) & (row // width != col // width)
        diagonal = row // width == col // width
        second = (iota((width, order), 1) // width) % 2 == 1
        half = [dot3(jnp.where(second, t, 0.0), jnp.where(corner, low, 0.0)) for t, low in zip(inv, lowers)]
        full = [
            jnp.where(diagonal, jnp.concatenate([t] * (order // width), axis=0), 0.0) for t in inv
        ]
        fill = [dot3(y, e) for y, e in zip(half, full)]
        inv = [
            jnp.concatenate([jnp.where(second, 0.0, t), jnp.where(second, t, 0.0) - r], axis=0)
            for t, r in zip(inv, fill)
        ]
        width *= 2
    return inv


def mix_kernel(q_ref, k_ref, v_ref, b_ref, o_ref, m_ref, x_out, x_ref):
    heads = q_ref.shape[1] // HEAD_DIM
    span = q_ref.shape[0]
    order = 2 * span
    step = pl.program_id(0)

    @pl.when(step == 0)
    def _():
        start = (iota((HEAD_DIM, 2 * HEAD_DIM), 0) == iota((HEAD_DIM, 2 * HEAD_DIM), 1)).astype(F32)
        for h in range(heads):
            x_ref[h] = start

    row = iota((order, order), 0)
    col = iota((order, order), 1)
    strict = col < row
    weave = (row == 2 * (col % span) + col // span).astype(BF16)
    causal = iota((span, order), 1) <= 2 * iota((span, order), 0) + 1
    data = []
    lowers = []
    for h in range(heads):
        cols = slice(h * HEAD_DIM, (h + 1) * HEAD_DIM)
        query = q_ref[:, cols]
        pair = jnp.concatenate(
            [
                jnp.concatenate([k_ref[0, :, cols], v_ref[0, :, cols]], axis=1),
                jnp.concatenate([k_ref[1, :, cols], v_ref[1, :, cols]], axis=1),
            ],
            axis=0,
        )
        woven = dot(weave, pair)
        key = woven[:, :HEAD_DIM]
        value = woven[:, HEAD_DIM:]
        key_b = key.astype(BF16)
        norm = lax.rsqrt(jnp.sum(key * key, axis=1, keepdims=True) + 1e-06)
        beta = b_ref[:, h : h + 1]
        both = jnp.concatenate([key_b, query], axis=0)
        gram = lax.dot_general(both, key_b, (((1,), (1,)), ((), ())), preferred_element_type=F32)
        weight = beta * norm * norm
        lowers.append(jnp.where(strict, weight * gram[:order], 0.0))
        scores = jnp.where(causal, gram[order:], 0.0).astype(BF16)
        qf = query.astype(F32)
        q_norm = lax.rsqrt(jnp.sum(qf * qf, axis=1, keepdims=True) + 1e-06)
        readers = jnp.concatenate([key.T.astype(BF16), scores], axis=0)
        data.append((both, readers, beta * norm * value, weight, q_norm))
    solved = inverse(lowers, order)
    seen = []
    for h in range(heads):
        both = data[h][0]
        high, low = split(x_ref[h])
        seen.append(
            dot(jnp.concatenate([both, both], axis=1), jnp.concatenate([high, low], axis=0))
        )
    writes = []
    for h in range(heads):
        _, _, scaled, weight, _ = data[h]
        gap = -weight * seen[h][:order]
        gap = jnp.concatenate([gap[:, :HEAD_DIM], gap[:, HEAD_DIM:] + scaled], axis=1)
        writes.append(dot3(solved[h], gap))
    for h in range(heads):
        cols = slice(h * HEAD_DIM, (h + 1) * HEAD_DIM)
        readers, q_norm = data[h][1], data[h][4]
        high, low = split(writes[h])
        change = dot(
            jnp.concatenate([readers, readers], axis=1), jnp.concatenate([high, low], axis=0)
        )
        x_ref[h] = x_ref[h] + change[:HEAD_DIM]
        out = q_norm * (seen[h][order:] + change[HEAD_DIM:])
        m_ref[:, cols] = out[:, :HEAD_DIM].astype(BF16)
        o_ref[:, cols] = out[:, HEAD_DIM:]

    @pl.when(step == pl.num_programs(0) - 1)
    def _():
        for h in range(heads):
            x_out[h] = x_ref[h].astype(BF16)


def mix(queries, keys, values, beta_cols):
    tokens, width = queries.shape
    heads = width // HEAD_DIM
    return pl.pallas_call(
        mix_kernel,
        grid=(tokens // SPAN,),
        in_specs=[
            pl.BlockSpec((SPAN, width), lambda c: (c, 0)),
            pl.BlockSpec((2, SPAN, width), lambda c: (0, c, 0)),
            pl.BlockSpec((2, SPAN, width), lambda c: (0, c, 0)),
            pl.BlockSpec((2 * SPAN, heads), lambda c: (c, 0)),
        ],
        out_specs=[
            pl.BlockSpec((SPAN, width), lambda c: (c, 0)),
            pl.BlockSpec((SPAN, width), lambda c: (c, 0)),
            pl.BlockSpec((heads, HEAD_DIM, 2 * HEAD_DIM), lambda c: (0, 0, 0)),
        ],
        out_shape=[
            jax.ShapeDtypeStruct((tokens, width), F32),
            jax.ShapeDtypeStruct((tokens, width), BF16),
            jax.ShapeDtypeStruct((heads, HEAD_DIM, 2 * HEAD_DIM), BF16),
        ],
        scratch_shapes=[pltpu.VMEM((heads, HEAD_DIM, 2 * HEAD_DIM), F32)],
        compiler_params=pltpu.CompilerParams(
            dimension_semantics=("arbitrary",), vmem_limit_bytes=VMEM_LIMIT
        ),
    )(queries, keys, values, beta_cols)


def chain_kernel(peers, x_ref, s_ref):
    heads = x_ref.shape[0] // peers
    for h in range(heads):
        state = jnp.zeros((HEAD_DIM, HEAD_DIM), F32)
        for k in range(peers):
            s_ref[k * heads + h] = state.astype(BF16)
            if k < peers - 1:
                maps = x_ref[k * heads + h]
                turn = maps[:, :HEAD_DIM]
                high, low = split(state)
                state = maps[:, HEAD_DIM:].astype(F32) + dot(
                    jnp.concatenate([turn, turn], axis=1), jnp.concatenate([high, low], axis=0)
                )


FUSED_LIMIT = 52 * 1024 * 1024


def dot_t(a, b):
    return lax.dot_general(a, b, (((1,), (1,)), ((), ())), preferred_element_type=F32)


def pair_dot(a, low, high_b, low_b):
    rows = a.shape[0]
    both = dot(jnp.concatenate([a, low], axis=0), jnp.concatenate([high_b, low_b], axis=1))
    width = high_b.shape[1]
    return both[:rows, :width] + both[rows:, :width] + both[:rows, width:]


def weave(*streams):
    order = []
    for n, (count, _, first, last) in enumerate(streams):
        order += [(first + (last - first) * (k + 0.5) / count, n) for k in range(count)]
    for _, n in sorted(order):
        next(streams[n][1], None)
    for _, stream, _, _ in streams:
        for _ in stream:
            pass


def base_solve(lowers, span):
    order = 2 * span
    base = BASE // 2
    lane = iota((base, order), 1)
    group = (lane % span) // base
    row16, lane16 = iota((BASE, order), 0), iota((BASE, order), 1)
    group16 = (lane16 % span) // base
    row_tok, lane_tok = row16 % base, lane16 % base
    before = (lane_tok < row_tok) | ((lane_tok == row_tok) & (lane16 // span < row16 // base))
    compact = []
    for n, low in enumerate(lowers):
        halves = []
        for j in range(2):
            total = jnp.zeros((base, order), F32)
            for blk in range(span // base):
                start = j * span + blk * base
                total = jnp.where(group == blk, low[start : start + base, :], total)
            halves.append(total)
        compact.append(jnp.where(before, jnp.concatenate(halves, axis=0), 0.0))
        if n % 2:
            yield
    own = (row16 % base == lane16 % base) & (row16 // base == lane16 // span)
    inv = [own.astype(F32) for _ in lowers]
    for s in range(BASE - 1):
        t, j = s // 2, s % 2
        pick = j * span + group16 * base + t
        for n, low in enumerate(compact):
            column = jnp.take_along_axis(low, pick, axis=1, mode="promise_in_bounds")
            inv[n] = inv[n] - column * inv[n][j * base + t : j * base + t + 1, :]
        yield
    return inv


def merge(inv, pieces, span):
    order = 2 * span
    tok_r = iota((order, order), 0) % span
    tok_c = iota((order, order), 1) % span
    width = BASE // 2
    zero = jnp.zeros((), BF16)
    while width < span:
        last = 2 * width == span
        diagonal = tok_r // width == tok_c // width
        corner = (tok_r // (2 * width) == tok_c // (2 * width)) & (tok_r // width != tok_c // width)
        second = ((iota((2 * width, order), 1) % span) // width) % 2 == 1
        odd, half, fill, wide, merged = [], [], [], [], []
        for n, t in enumerate(inv):
            odd.append(jnp.where(second, t, 0.0))
            th, tl = split(odd[n])
            high, low = pieces(n)
            if last:
                y = jnp.where(second, 0.0, pair_dot(th, tl, high, low))
            else:
                y = pair_dot(th, tl, jnp.where(corner, high, zero), jnp.where(corner, low, zero))
            half.append(y)
            parts = []
            for j in range(2):
                part = t[j * width : (j + 1) * width]
                if width < 16:
                    part = jnp.concatenate([part] * (16 // width), axis=0)
                parts.append((split(part), span // part.shape[0]))
            full = [
                jnp.concatenate([p[k] for p, count in parts for _ in range(count)], axis=0)
                for k in range(2)
            ]
            if not last:
                full = [jnp.where(diagonal, f, zero) for f in full]
            wide.append(full)
            yield
        for y, full in zip(half, wide):
            yh, yl = split(y)
            r = pair_dot(yh, yl, full[0], full[1])
            fill.append(jnp.where(second, 0.0, r) if last else r)
            yield
        for t, o, r in zip(inv, odd, fill):
            even, lower = t - o, o - r
            merged.append(
                jnp.concatenate(
                    [even[:width], lower[:width], even[width:], lower[width:]], axis=0
                )
            )
        inv = merged
        width *= 2
    return inv


def fused_kernel(
    seq_axis, peers, axis, q_hbm, k_hbm, v_hbm, b_hbm, g_hbm, w_hbm, y_ref,
    b_ref, q_ref, k_ref, v_ref, g_ref, beta_ref, stack_ref, turn_ref, source_ref, x_ref, start_ref,
    low_ref, inv_ref, weight_ref, eye_ref,
    maps, held, carry_ref, states, s_ref, o_ref, m_ref,
    mixed, weight, total, far_out, far_in, near_out, near_in, cross_out, cross_in,
    b_sem, kv_sem, q_sem, g_sem, load_sem, map_send, map_recv, back_send, back_recv,
    far_send, far_recv, near_send, near_recv, cross_send, cross_recv,
):
    heads, blocks, span = q_ref.shape[0], q_ref.shape[1], q_ref.shape[2]
    pairs = heads // 2
    parts = 2
    batch = blocks // parts
    seq = lax.axis_index(seq_axis)
    me = lax.axis_index(axis)
    chip, core = me // 2, me % 2
    sibling = 2 * chip + 1 - core
    across = 2 * (1 - chip) + core
    beyond = 2 * (1 - chip) + 1 - core
    width = y_ref.shape[1]

    def columns(h):
        return pl.ds(pl.multiple_of(h * HEAD_DIM, HEAD_DIM), HEAD_DIM)

    def fetch_kv(h):
        return (
            pltpu.make_async_copy(k_hbm.at[:, :, :, columns(h)], k_ref.at[h], kv_sem.at[0, h]),
            pltpu.make_async_copy(v_hbm.at[:, :, :, columns(h)], v_ref.at[h], kv_sem.at[1, h]),
        )

    def fetch_q(h):
        return pltpu.make_async_copy(q_hbm.at[:, :, columns(h)], q_ref.at[h], q_sem.at[h])

    def fetch_g(h):
        return pltpu.make_async_copy(g_hbm.at[:, :, columns(h)], g_ref.at[h], g_sem.at[h])

    def load(n):
        owner = (beyond, across, sibling, me)[n]
        return pltpu.make_async_copy(
            w_hbm.at[:, pl.ds(pl.multiple_of(owner * width, width), width)],
            weight.at[n],
            load_sem.at[n],
        )

    def start_kv(first, last):
        for n in range(2):
            for h in range(first, last):
                fetch_kv(h)[n].start()

    fetch_b = pltpu.make_async_copy(b_hbm, b_ref, b_sem)
    fetch_b.start()
    start_kv(0, 2)
    barrier = pltpu.get_barrier_semaphore()
    for other in (sibling, across):
        pl.semaphore_signal(barrier, inc=1, device_id={axis: other}, device_id_type=MESH)
    for away in range(1, peers):
        pl.semaphore_signal(
            barrier,
            inc=1,
            device_id={seq_axis: lax.rem(seq + away, peers)},
            device_id_type=MESH,
        )

    eye_ref[...] = (iota(eye_ref.shape, 0) == iota(eye_ref.shape, 1)).astype(F32)
    fetch_b.wait()
    for blk in range(blocks):
        window = slice(blk * span, (blk + 1) * span)
        beta_ref[blk] = jnp.concatenate([b_ref[:, 0, window], b_ref[:, 1, window]], axis=1)

    def place(it, n):
        pair, part = it
        return 2 * pair + n % 2, part * batch + n // 2

    count = 2 * batch

    def key_of(h, blk):
        return jnp.concatenate([k_ref[h, 0, blk], k_ref[h, 1, blk]], axis=0)

    def stack_of(h, blk):
        none = jnp.zeros((HEAD_DIM, HEAD_DIM), BF16)
        return jnp.concatenate(
            [
                jnp.concatenate([stack_ref[h, blk, 0], stack_ref[h, blk, 2]], axis=1),
                jnp.concatenate([stack_ref[h, blk, 1], none], axis=1),
            ],
            axis=0,
        )

    def solve(it):
        slot = it[1]
        grams, squares = [], []
        for n in range(count):
            key = key_of(*place(it, n))
            grams.append(dot_t(key, key))
            if n % 2:
                yield
        for n, g in enumerate(grams):
            squares.append(jnp.sum(eye_ref[...] * g, axis=0, keepdims=True))
            if n % 4 == 3:
                yield
        beta = jnp.concatenate(
            [beta_ref[place(it, n)[1], pl.ds(place(it, n)[0], 1), :] for n in range(count)], axis=0
        )
        norm = lax.rsqrt(jnp.concatenate(squares, axis=0) + 1e-06)
        value_weight = beta * norm
        weight_rows = value_weight * norm
        weight_ref[slot, 0] = weight_rows
        weight_ref[slot, 1] = value_weight
        weight_cols = weight_rows.T
        yield
        lowers = []
        for n, g in enumerate(grams):
            low = weight_cols[:, n : n + 1] * g
            lowers.append(low)
            low_ref[slot, n, 0], low_ref[slot, n, 1] = split(low)
            if n % 2:
                yield
        inv = yield from base_solve(lowers, span)
        for n in range(count):
            inv_ref[slot, n] = inv[n]

    def transit(it):
        slot = it[1]

        def pieces(n):
            return low_ref[slot, n, 0], low_ref[slot, n, 1]

        solved = yield from merge([inv_ref[slot, n] for n in range(count)], pieces, span)
        turns, writes, changes = [], [], []
        for n in range(count):
            h, blk = place(it, n)
            th, tl = split(solved[n] * weight_ref[slot, 0, n : n + 1, :])
            tv = (solved[n] * weight_ref[slot, 1, n : n + 1, :]).astype(BF16)
            key = key_of(h, blk)
            value = jnp.concatenate([v_ref[h, 0, blk], v_ref[h, 1, blk]], axis=0)
            turns.append(
                dot(jnp.concatenate([th, tl], axis=1), jnp.concatenate([key, key], axis=0))
            )
            writes.append(dot(tv, value))
            yield
        for n in range(count):
            h, blk = place(it, n)
            turn_h, turn_l = split(turns[n])
            stack_ref[h, blk, 0], stack_ref[h, blk, 1] = turn_h, turn_l
            stack_ref[h, blk, 2] = writes[n].astype(BF16)
            stack = stack_of(h, blk)
            key_t = key_of(h, blk).T
            changes.append(dot(jnp.concatenate([key_t, key_t], axis=1), stack))
            yield
        for n in range(count):
            step = eye_ref[...] - changes[n][:, :HEAD_DIM]
            turn_ref[slot, n, 0], turn_ref[slot, n, 1] = split(step)
            source_ref[slot, n] = changes[n][:, HEAD_DIM:]
            yield

    def compose(it):
        slot = it[1]
        pair, _ = it
        states_now = [None if it[1] == 0 else x_ref[2 * pair + i] for i in range(2)]
        for n in range(count):
            h, blk = place(it, n)
            i = n % 2
            if blk == 0:
                turn_h, turn_l = turn_ref[slot, n, 0], turn_ref[slot, n, 1]
                states_now[i] = jnp.concatenate(
                    [turn_h.astype(F32) + turn_l.astype(F32), source_ref[slot, n]], axis=1
                )
                yield
                continue
            high, low = split(states_now[i])
            start_ref[h, blk, 0] = high[:, :HEAD_DIM]
            start_ref[h, blk, 1] = high[:, HEAD_DIM:]
            turn_h, turn_l = turn_ref[slot, n, 0], turn_ref[slot, n, 1]
            moved = dot(
                jnp.concatenate([turn_h, turn_l, turn_h], axis=1),
                jnp.concatenate([high, high, low], axis=0),
            )
            states_now[i] = jnp.concatenate(
                [moved[:, :HEAD_DIM], moved[:, HEAD_DIM:] + source_ref[slot, n]], axis=1
            )
            if n >= count - 2:
                x_ref[h] = states_now[i]
            yield

    def a_stream(it, first=0.0, last=1.0):
        return 7 * count // 4 + BASE + 1, solve(it), first, last

    def b_stream(it, first=0.0, last=1.0):
        return 9 * count, transit(it), first, last

    def c_stream(it, first=0.0, last=1.0):
        return count, compose(it), first, last

    def owner_of(pair, i):
        side = lax.rem(pair + core, 2)
        return peers // 2 - 2 + side + i * (3 - 2 * side)

    def send_map(pair, i, source):
        h = 2 * pair + i
        return pltpu.make_async_remote_copy(
            src_ref=maps.at[h],
            dst_ref=held.at[pair, source],
            send_sem=map_send.at[h],
            recv_sem=map_recv.at[pair, source],
            device_id={seq_axis: owner_of(pair, i)},
            device_id_type=MESH,
        )

    def send_state(pair, i, target):
        h = 2 * pair + i
        return pltpu.make_async_remote_copy(
            src_ref=states.at[pair, target],
            dst_ref=s_ref.at[h],
            send_sem=back_send.at[pair, target],
            recv_sem=back_recv.at[h],
            device_id={seq_axis: target},
            device_id_type=MESH,
        )

    def post(pair):
        for i in range(2):
            h = 2 * pair + i
            maps[h, 0] = x_ref[h, :, :HEAD_DIM].astype(BF16)
            maps[h, 1] = x_ref[h, :, HEAD_DIM:].astype(BF16)

            @pl.when((seq != owner_of(pair, i)) & (seq != peers - 1))
            def _():
                send_map(pair, i, seq).start()

            @pl.when(seq == owner_of(pair, i))
            def _():
                held[pair, seq] = maps[h]

    def chain(pair):
        for i in range(2):

            @pl.when(seq == owner_of(pair, i))
            def _():
                carry_ref[...] = jnp.zeros((HEAD_DIM, HEAD_DIM), F32)
                for k in range(peers - 1):

                    @pl.when(seq != k)
                    def _():
                        send_map(pair, i, k).wait_recv()

                    high, low = split(carry_ref[...])
                    turn = held[pair, k, 0]
                    state = held[pair, k, 1].astype(F32) + dot(
                        jnp.concatenate([turn, turn], axis=1),
                        jnp.concatenate([high, low], axis=0),
                    )
                    carry_ref[...] = state
                    states[pair, k + 1] = state.astype(BF16)

                    @pl.when(seq != k + 1)
                    def _():
                        send_state(pair, i, k + 1).start()

                    @pl.when(seq == k + 1)
                    def _():
                        s_ref[2 * pair + i] = states[pair, k + 1]

    @pl.when(seq == 0)
    def _():
        s_ref[...] = jnp.zeros(s_ref.shape, BF16)

    def wait_kv(pair):
        for i in range(2):
            for copy in fetch_kv(2 * pair + i):
                copy.wait()

    def after_values(pair, stream):
        for i in range(2):
            fetch_kv(2 * pair + i)[1].wait()
        yield from stream

    for h in range(2):
        fetch_kv(h)[0].wait()
    start_kv(2, heads)
    for h in range(heads):
        fetch_q(h).start()
    for n in range(4):
        load(n).start()
    for h in range(heads):
        fetch_g(h).start()
    weave(
        a_stream((0, 0), 0.0, 1.0),
        a_stream((0, 1), 0.8, 2.0),
        (9 * count, after_values(0, transit((0, 0))), 1.0, 2.1),
    )

    def step(pair, _):
        wait_kv(pair)
        weave(
            a_stream((pair, 0), 0.0, 1.0),
            b_stream((pair - 1, 1), 0.0, 1.0),
            c_stream((pair - 1, 0), 0.0, 1.0),
            a_stream((pair, 1), 1.05, 2.0),
            b_stream((pair, 0), 1.05, 2.0),
            c_stream((pair - 1, 1), 1.05, 2.0),
        )

        @pl.when(pair == 1)
        def _():
            pl.semaphore_wait(barrier, peers + 1)

        post(pair - 1)
        return 0

    lax.fori_loop(1, pairs, step, 0)
    weave(
        b_stream((pairs - 1, 1), 0.0, 9.0),
        c_stream((pairs - 1, 0), 0.0, 6.0),
        c_stream((pairs - 1, 1), 8.1, 9.1),
    )
    post(pairs - 1)
    for h in range(heads):
        fetch_q(h).wait()

    def read(pair, _):
        causal = iota((span, 2 * span), 1) % span <= iota((span, 2 * span), 0)
        for i in range(2):
            h = 2 * pair + i
            scores = []
            for blk in range(blocks):
                found = jnp.where(causal, dot_t(q_ref[h, blk], key_of(h, blk)), 0.0).astype(BF16)
                scores.append(jnp.concatenate([found, found], axis=1))
            drawn = [dot(score, stack_of(h, blk)) for blk, score in enumerate(scores)]
            for blk in range(blocks):
                kept = (q_ref[h, blk].astype(F32) - drawn[blk][:, :HEAD_DIM]).astype(BF16)
                if blk == 0:
                    m_ref[h, blk] = kept
                    o_ref[h, blk] = drawn[blk][:, HEAD_DIM:]
                    continue
                out = dot(kept, jnp.concatenate([start_ref[h, blk, 0], start_ref[h, blk, 1]], axis=1))
                m_ref[h, blk] = out[:, :HEAD_DIM].astype(BF16)
                o_ref[h, blk] = out[:, HEAD_DIM:] + drawn[blk][:, HEAD_DIM:]

        return 0

    def link(pair, _):
        chain(pair)
        return 0

    lax.fori_loop(0, 2, link, 0)
    lax.fori_loop(0, pairs // 2, read, 0)
    lax.fori_loop(2, pairs, link, 0)
    lax.fori_loop(pairs // 2, pairs, read, 0)
    for h in range(heads):
        fetch_g(h).wait()

    def wait_state(pair):
        for i in range(2):

            @pl.when((seq != owner_of(pair, i)) & (seq != 0))
            def _():
                send_state(pair, i, seq).wait_recv()

    def blend(pair, t):
        for i in range(2):
            h = 2 * pair + i
            query = q_ref[h, t].astype(F32)
            unit = lax.rsqrt(jnp.sum(query * query, axis=1, keepdims=True) + 1e-06)
            seen = unit * (o_ref[h, t] + dot(m_ref[h, t], s_ref[h]))
            scale = lax.rsqrt(jnp.mean(seen * seen, axis=1, keepdims=True) + 1e-06)
            gate = g_ref[h, t].astype(F32)
            mixed[t, h] = (seen * scale * (gate / (1.0 + jnp.exp(-gate)))).astype(BF16)

    def blend_pair(pair):
        wait_state(pair)
        for blk in range(blocks):
            blend(pair, blk)

    def settle(pair, _):
        blend_pair(pair)
        return 0

    lax.fori_loop(0, pairs - 1, settle, 0)

    sizes = [1, 1] + [2] * ((blocks - 4) // 2) + [1, 1]
    starts = [sum(sizes[:t]) for t in range(len(sizes))]

    def rows(t):
        return pl.ds(starts[t] * span, sizes[t] * span)

    def send(source, target, send_sem, recv_sem, t, device):
        return pltpu.make_async_remote_copy(
            src_ref=source.at[rows(t)],
            dst_ref=target.at[rows(t)],
            send_sem=send_sem.at[t],
            recv_sem=recv_sem.at[t],
            device_id={axis: device},
            device_id_type=MESH,
        )

    def far(t):
        return send(far_out, far_in, far_send, far_recv, t, sibling)

    def near(t):
        return send(near_out, near_in, near_send, near_recv, t, sibling)

    def cross(t):
        return send(cross_out, cross_in, cross_send, cross_recv, t, across)

    def pass_on(t):
        far(t).wait()
        cross_out[rows(t)] = (total[rows(t)] + far_in[rows(t)].astype(F32)).astype(BF16)
        cross(t).start()

    def mixed_of(t, first, last):
        return jnp.concatenate(
            [
                jnp.concatenate([mixed[starts[t] + b, h] for h in range(first, last)], axis=1)
                for b in range(sizes[t])
            ],
            axis=0,
        )

    def product(t, n):
        return dot(mixed_of(t, 0, heads), weight[n])

    def finish_piece(t):
        for b in range(sizes[t]):
            blend(pairs - 1, starts[t] + b)

    count_pieces = len(sizes)
    early = (heads - 2) * HEAD_DIM
    load(0).wait()
    total[rows(0)] = dot(mixed_of(0, 0, heads - 2), weight[0, :early, :])
    wait_state(pairs - 1)
    finish_piece(0)
    late = dot(mixed_of(0, heads - 2, heads), weight[0, early:, :])
    far_out[rows(0)] = (total[rows(0)] + late).astype(BF16)
    far(0).start()
    load(1).wait()
    finish_piece(1)
    total[rows(0)] = product(0, 1)
    for t in range(1, count_pieces):
        if t > 1:
            finish_piece(t)
        far_out[rows(t)] = product(t, 0).astype(BF16)
        far(t).start()
        pass_on(t - 1)
        total[rows(t)] = product(t, 1)
    load(2).wait()
    for t in range(count_pieces):
        near_out[rows(t)] = product(t, 2).astype(BF16)
        near(t).start()
        if t == 0:
            pass_on(count_pieces - 1)
    load(3).wait()
    for t in range(count_pieces):
        total[rows(t)] = product(t, 3)
    for t in range(count_pieces):
        near(t).wait()
        total[rows(t)] = total[rows(t)] + near_in[rows(t)].astype(F32)
    for t in range(count_pieces):
        cross(t).wait()
        y_ref[rows(t)] = (total[rows(t)] + cross_in[rows(t)].astype(F32)).astype(BF16)
    for pair in range(pairs):
        for i in range(2):

            @pl.when((seq != owner_of(pair, i)) & (seq != peers - 1))
            def _():
                send_map(pair, i, seq).wait_send()

            @pl.when(seq == owner_of(pair, i))
            def _():
                for k in range(1, peers):

                    @pl.when(seq != k)
                    def _():
                        send_state(pair, i, k).wait_send()


def fused(queries, keys, values, betas, gate, out_weight, seq_axis, axis):
    tokens, depth = queries.shape
    heads = depth // HEAD_DIM
    peers = lax.axis_size(seq_axis)
    width = out_weight.shape[1] // lax.axis_size(axis)
    blocks = tokens // SPAN
    batch = blocks // 2
    hbm = pl.BlockSpec(memory_space=pltpu.HBM)
    piece = (tokens, width)
    pieces = blocks // 2 + 2
    square = (HEAD_DIM, HEAD_DIM)
    wide = (HEAD_DIM, 2 * HEAD_DIM)
    two = (2,) + square
    pairs = heads // 2
    dma = pltpu.SemaphoreType.DMA
    per_head = (heads, blocks, SPAN, HEAD_DIM)
    both = (heads, 2, blocks, SPAN, HEAD_DIM)
    return pl.pallas_call(
        functools.partial(fused_kernel, seq_axis, peers, axis),
        in_specs=[hbm] * 6,
        out_specs=pl.BlockSpec(memory_space=pltpu.VMEM),
        out_shape=jax.ShapeDtypeStruct(piece, BF16),
        scratch_shapes=[
            pltpu.VMEM(betas.shape, F32),
            pltpu.VMEM(per_head, BF16),
            pltpu.VMEM(both, BF16),
            pltpu.VMEM(both, BF16),
            pltpu.VMEM(per_head, BF16),
            pltpu.VMEM((blocks, heads, 2 * SPAN), F32),
            pltpu.VMEM((heads, blocks, 3) + square, BF16),
            pltpu.VMEM((2, 2 * batch) + two, BF16),
            pltpu.VMEM((2, 2 * batch) + square, F32),
            pltpu.VMEM((heads,) + wide, F32),
            pltpu.VMEM((heads, blocks) + two, BF16),
            pltpu.VMEM((2, 2 * batch) + two, BF16),
            pltpu.VMEM((2, 2 * batch, BASE, 2 * SPAN), F32),
            pltpu.VMEM((2, 2, 2 * batch, 2 * SPAN), F32),
            pltpu.VMEM(square, F32),
            pltpu.VMEM((heads,) + two, BF16),
            pltpu.VMEM((pairs, peers) + two, BF16),
            pltpu.VMEM(square, F32),
            pltpu.VMEM((pairs, peers) + square, BF16),
            pltpu.VMEM((heads,) + square, BF16),
            pltpu.VMEM(per_head, F32),
            pltpu.VMEM(per_head, BF16),
            pltpu.VMEM((blocks, heads, SPAN, HEAD_DIM), BF16),
            pltpu.VMEM((4, depth, width), BF16),
            pltpu.VMEM(piece, F32),
        ]
        + [pltpu.VMEM(piece, BF16)] * 6
        + [
            dma,
            dma((2, heads)),
            dma((heads,)),
            dma((heads,)),
            dma((4,)),
            dma((heads,)),
            dma((pairs, peers)),
            dma((pairs, peers)),
            dma((heads,)),
        ]
        + [dma((pieces,))] * 6,
        compiler_params=pltpu.CompilerParams(
            collective_id=0, has_side_effects=True, vmem_limit_bytes=FUSED_LIMIT
        ),
    )(
        queries.reshape(blocks, SPAN, depth),
        keys.reshape(2, blocks, SPAN, depth),
        values.reshape(2, blocks, SPAN, depth),
        pltpu.with_memory_space_constraint(betas, pltpu.HBM),
        gate.reshape(blocks, SPAN, depth),
        out_weight,
    )


def start_state(maps, axis):
    peers, index = lax.axis_size(axis), lax.axis_index(axis)
    heads = maps.shape[0]
    held = lax.all_gather(maps, axis, axis=0, tiled=True)
    states = pl.pallas_call(
        functools.partial(chain_kernel, peers),
        out_shape=jax.ShapeDtypeStruct((held.shape[0], HEAD_DIM, HEAD_DIM), BF16),
        compiler_params=pltpu.CompilerParams(vmem_limit_bytes=VMEM_LIMIT),
    )(held)
    return lax.dynamic_slice_in_dim(states, index * heads, heads, 0)


def out_kernel(o_ref, m_ref, s_ref, g_ref, w_ref, y_ref, mixed_ref):
    @pl.when(pl.program_id(0) == 0)
    def _():
        for h in range(s_ref.shape[0]):
            cols = slice(h * HEAD_DIM, (h + 1) * HEAD_DIM)
            seen = o_ref[:, cols] + dot(m_ref[:, cols], s_ref[h])
            scale = lax.rsqrt(jnp.mean(seen * seen, axis=1, keepdims=True) + 1e-06)
            gate = g_ref[:, cols].astype(F32)
            mixed_ref[:, cols] = (seen * scale * (gate / (1.0 + jnp.exp(-gate)))).astype(BF16)

    y_ref[...] = dot(mixed_ref[...], w_ref[...]).astype(BF16)


def project(local, reach, states, gate, out_weight):
    tokens, width = local.shape
    total = out_weight.shape[1]
    tile = 512
    whole = pl.BlockSpec((tokens, width), lambda n: (0, 0))
    return pl.pallas_call(
        out_kernel,
        grid=(total // tile,),
        in_specs=[
            whole,
            whole,
            pl.BlockSpec(states.shape, lambda n: (0, 0, 0)),
            whole,
            pl.BlockSpec((width, tile), lambda n: (0, n)),
        ],
        out_specs=pl.BlockSpec((tokens, tile), lambda n: (0, n)),
        out_shape=jax.ShapeDtypeStruct((tokens, total), BF16),
        scratch_shapes=[pltpu.VMEM((tokens, width), BF16)],
        compiler_params=pltpu.CompilerParams(
            dimension_semantics=("arbitrary",), vmem_limit_bytes=VMEM_LIMIT
        ),
    )(local, reach, states, gate, out_weight)


def per_device(queries, keys, values, betas, gate, out_weight):
    heads, _, tokens = betas.shape
    peers, index = lax.axis_size("ctx"), lax.axis_size("head")
    if index == 4 and peers >= 4 and peers % 2 == 0 and heads % 8 == 0 and tokens % (8 * SPAN) == 0:
        return fused(queries, keys, values, betas, gate, out_weight, "ctx", "head")
    beta_cols = betas.transpose(2, 1, 0).reshape(2 * tokens, heads)
    local, reach, maps = mix(queries, keys, values, beta_cols)
    states = start_state(maps, "ctx")
    partial_sum = project(local, reach, states, gate, out_weight)
    return lax.psum_scatter(partial_sum, "head", scatter_dimension=1, tiled=True)


def solution(mesh):
    return jax.shard_map(
        per_device,
        mesh=mesh,
        in_specs=(
            P("ctx", "head"),
            P(None, "ctx", "head"),
            P(None, "ctx", "head"),
            P("head", None, "ctx"),
            P("ctx", "head"),
            P("head", None),
        ),
        out_specs=P("ctx", "head"),
        check_vma=False,
    )
```

```python
import functools

import jax
import jax.numpy as jnp
from jax import lax
from jax.experimental import pallas as pl
from jax.experimental.pallas import tpu as pltpu
from jax.sharding import PartitionSpec as P

HEAD_DIM = 128
SPAN = 64
BASE = 16
F32 = jnp.float32
BF16 = jnp.bfloat16
VMEM_LIMIT = 60 * 1024 * 1024
MESH = pl.DeviceIdType.MESH
PIECES = 4


def iota(shape, dim):
    return lax.broadcasted_iota(jnp.int32, shape, dim)


def split(a):
    high = a.astype(BF16)
    return high, (a - high.astype(F32)).astype(BF16)


def dot(a, b):
    return jnp.dot(a, b, preferred_element_type=F32)


def dot3(a, b):
    ah, al = split(a)
    bh, bl = split(b)
    return dot(jnp.concatenate([ah, al, ah], axis=1), jnp.concatenate([bh, bh, bl], axis=0))


def inverse(lowers, order):
    lane = iota((BASE, order), 1)
    compact = []
    for low in lowers:
        total = jnp.zeros((BASE, order), F32)
        for blk in range(order // BASE):
            total = jnp.where(lane // BASE == blk, low[blk * BASE : (blk + 1) * BASE, :], total)
        compact.append(total)
    inv = [(iota((BASE, order), 0) == lane % BASE).astype(F32) for _ in lowers]
    for j in range(BASE - 1):
        pick = (lane // BASE) * BASE + j
        for n, low in enumerate(compact):
            column = jnp.take_along_axis(low, pick, axis=1, mode="promise_in_bounds")
            inv[n] = inv[n] - column * inv[n][j : j + 1, :]
    row = iota((order, order), 0)
    col = iota((order, order), 1)
    width = BASE
    while width < order:
        corner = (row // (2 * width) == col // (2 * width)) & (row // width != col // width)
        diagonal = row // width == col // width
        second = (iota((width, order), 1) // width) % 2 == 1
        half = [dot3(jnp.where(second, t, 0.0), jnp.where(corner, low, 0.0)) for t, low in zip(inv, lowers)]
        full = [
            jnp.where(diagonal, jnp.concatenate([t] * (order // width), axis=0), 0.0) for t in inv
        ]
        fill = [dot3(y, e) for y, e in zip(half, full)]
        inv = [
            jnp.concatenate([jnp.where(second, 0.0, t), jnp.where(second, t, 0.0) - r], axis=0)
            for t, r in zip(inv, fill)
        ]
        width *= 2
    return inv


def mix_kernel(q_ref, k_ref, v_ref, b_ref, o_ref, m_ref, x_out, x_ref):
    heads = q_ref.shape[1] // HEAD_DIM
    span = q_ref.shape[0]
    order = 2 * span
    step = pl.program_id(0)

    @pl.when(step == 0)
    def _():
        start = (iota((HEAD_DIM, 2 * HEAD_DIM), 0) == iota((HEAD_DIM, 2 * HEAD_DIM), 1)).astype(F32)
        for h in range(heads):
            x_ref[h] = start

    row = iota((order, order), 0)
    col = iota((order, order), 1)
    strict = col < row
    weave = (row == 2 * (col % span) + col // span).astype(BF16)
    causal = iota((span, order), 1) <= 2 * iota((span, order), 0) + 1
    data = []
    lowers = []
    for h in range(heads):
        cols = slice(h * HEAD_DIM, (h + 1) * HEAD_DIM)
        query = q_ref[:, cols]
        pair = jnp.concatenate(
            [
                jnp.concatenate([k_ref[0, :, cols], v_ref[0, :, cols]], axis=1),
                jnp.concatenate([k_ref[1, :, cols], v_ref[1, :, cols]], axis=1),
            ],
            axis=0,
        )
        woven = dot(weave, pair)
        key = woven[:, :HEAD_DIM]
        value = woven[:, HEAD_DIM:]
        key_b = key.astype(BF16)
        norm = lax.rsqrt(jnp.sum(key * key, axis=1, keepdims=True) + 1e-06)
        beta = b_ref[:, h : h + 1]
        both = jnp.concatenate([key_b, query], axis=0)
        gram = lax.dot_general(both, key_b, (((1,), (1,)), ((), ())), preferred_element_type=F32)
        weight = beta * norm * norm
        lowers.append(jnp.where(strict, weight * gram[:order], 0.0))
        scores = jnp.where(causal, gram[order:], 0.0).astype(BF16)
        qf = query.astype(F32)
        q_norm = lax.rsqrt(jnp.sum(qf * qf, axis=1, keepdims=True) + 1e-06)
        readers = jnp.concatenate([key.T.astype(BF16), scores], axis=0)
        data.append((both, readers, beta * norm * value, weight, q_norm))
    solved = inverse(lowers, order)
    seen = []
    for h in range(heads):
        both = data[h][0]
        high, low = split(x_ref[h])
        seen.append(
            dot(jnp.concatenate([both, both], axis=1), jnp.concatenate([high, low], axis=0))
        )
    writes = []
    for h in range(heads):
        _, _, scaled, weight, _ = data[h]
        gap = -weight * seen[h][:order]
        gap = jnp.concatenate([gap[:, :HEAD_DIM], gap[:, HEAD_DIM:] + scaled], axis=1)
        writes.append(dot3(solved[h], gap))
    for h in range(heads):
        cols = slice(h * HEAD_DIM, (h + 1) * HEAD_DIM)
        readers, q_norm = data[h][1], data[h][4]
        high, low = split(writes[h])
        change = dot(
            jnp.concatenate([readers, readers], axis=1), jnp.concatenate([high, low], axis=0)
        )
        x_ref[h] = x_ref[h] + change[:HEAD_DIM]
        out = q_norm * (seen[h][order:] + change[HEAD_DIM:])
        m_ref[:, cols] = out[:, :HEAD_DIM].astype(BF16)
        o_ref[:, cols] = out[:, HEAD_DIM:]

    @pl.when(step == pl.num_programs(0) - 1)
    def _():
        for h in range(heads):
            x_out[h] = x_ref[h].astype(BF16)


def mix(queries, keys, values, beta_cols):
    tokens, width = queries.shape
    heads = width // HEAD_DIM
    return pl.pallas_call(
        mix_kernel,
        grid=(tokens // SPAN,),
        in_specs=[
            pl.BlockSpec((SPAN, width), lambda c: (c, 0)),
            pl.BlockSpec((2, SPAN, width), lambda c: (0, c, 0)),
            pl.BlockSpec((2, SPAN, width), lambda c: (0, c, 0)),
            pl.BlockSpec((2 * SPAN, heads), lambda c: (c, 0)),
        ],
        out_specs=[
            pl.BlockSpec((SPAN, width), lambda c: (c, 0)),
            pl.BlockSpec((SPAN, width), lambda c: (c, 0)),
            pl.BlockSpec((heads, HEAD_DIM, 2 * HEAD_DIM), lambda c: (0, 0, 0)),
        ],
        out_shape=[
            jax.ShapeDtypeStruct((tokens, width), F32),
            jax.ShapeDtypeStruct((tokens, width), BF16),
            jax.ShapeDtypeStruct((heads, HEAD_DIM, 2 * HEAD_DIM), BF16),
        ],
        scratch_shapes=[pltpu.VMEM((heads, HEAD_DIM, 2 * HEAD_DIM), F32)],
        compiler_params=pltpu.CompilerParams(
            dimension_semantics=("arbitrary",), vmem_limit_bytes=VMEM_LIMIT
        ),
    )(queries, keys, values, beta_cols)


def chain_kernel(peers, x_ref, s_ref):
    heads = x_ref.shape[0] // peers
    for h in range(heads):
        state = jnp.zeros((HEAD_DIM, HEAD_DIM), F32)
        for k in range(peers):
            s_ref[k * heads + h] = state.astype(BF16)
            if k < peers - 1:
                maps = x_ref[k * heads + h]
                turn = maps[:, :HEAD_DIM]
                high, low = split(state)
                state = maps[:, HEAD_DIM:].astype(F32) + dot(
                    jnp.concatenate([turn, turn], axis=1), jnp.concatenate([high, low], axis=0)
                )


FUSED_LIMIT = 52 * 1024 * 1024


def dot_t(a, b):
    return lax.dot_general(a, b, (((1,), (1,)), ((), ())), preferred_element_type=F32)


def pair_dot(a, low, high_b, low_b):
    rows = a.shape[0]
    both = dot(jnp.concatenate([a, low], axis=0), jnp.concatenate([high_b, low_b], axis=1))
    width = high_b.shape[1]
    return both[:rows, :width] + both[rows:, :width] + both[:rows, width:]


def weave(*streams):
    order = []
    for n, (count, _, first, last) in enumerate(streams):
        order += [(first + (last - first) * (k + 0.5) / count, n) for k in range(count)]
    for _, n in sorted(order):
        next(streams[n][1], None)
    for _, stream, _, _ in streams:
        for _ in stream:
            pass


def base_solve(lowers, span):
    order = 2 * span
    base = BASE // 2
    lane = iota((base, order), 1)
    group = (lane % span) // base
    row16, lane16 = iota((BASE, order), 0), iota((BASE, order), 1)
    group16 = (lane16 % span) // base
    row_tok, lane_tok = row16 % base, lane16 % base
    before = (lane_tok < row_tok) | ((lane_tok == row_tok) & (lane16 // span < row16 // base))
    compact = []
    for n, low in enumerate(lowers):
        halves = []
        for j in range(2):
            total = jnp.zeros((base, order), F32)
            for blk in range(span // base):
                start = j * span + blk * base
                total = jnp.where(group == blk, low[start : start + base, :], total)
            halves.append(total)
        compact.append(jnp.where(before, jnp.concatenate(halves, axis=0), 0.0))
        if n % 2:
            yield
    own = (row16 % base == lane16 % base) & (row16 // base == lane16 // span)
    inv = [own.astype(F32) for _ in lowers]
    for s in range(BASE - 1):
        t, j = s // 2, s % 2
        pick = j * span + group16 * base + t
        for n, low in enumerate(compact):
            column = jnp.take_along_axis(low, pick, axis=1, mode="promise_in_bounds")
            inv[n] = inv[n] - column * inv[n][j * base + t : j * base + t + 1, :]
        yield
    return inv


def merge(inv, pieces, span):
    order = 2 * span
    tok_r = iota((order, order), 0) % span
    tok_c = iota((order, order), 1) % span
    width = BASE // 2
    zero = jnp.zeros((), BF16)
    while width < span:
        last = 2 * width == span
        diagonal = tok_r // width == tok_c // width
        corner = (tok_r // (2 * width) == tok_c // (2 * width)) & (tok_r // width != tok_c // width)
        second = ((iota((2 * width, order), 1) % span) // width) % 2 == 1
        odd, half, fill, wide, merged = [], [], [], [], []
        for n, t in enumerate(inv):
            odd.append(jnp.where(second, t, 0.0))
            th, tl = split(odd[n])
            high, low = pieces(n)
            if last:
                y = jnp.where(second, 0.0, pair_dot(th, tl, high, low))
            else:
                y = pair_dot(th, tl, jnp.where(corner, high, zero), jnp.where(corner, low, zero))
            half.append(y)
            parts = []
            for j in range(2):
                part = t[j * width : (j + 1) * width]
                if width < 16:
                    part = jnp.concatenate([part] * (16 // width), axis=0)
                parts.append((split(part), span // part.shape[0]))
            full = [
                jnp.concatenate([p[k] for p, count in parts for _ in range(count)], axis=0)
                for k in range(2)
            ]
            if not last:
                full = [jnp.where(diagonal, f, zero) for f in full]
            wide.append(full)
            yield
        for y, full in zip(half, wide):
            yh, yl = split(y)
            r = pair_dot(yh, yl, full[0], full[1])
            fill.append(jnp.where(second, 0.0, r) if last else r)
            yield
        for t, o, r in zip(inv, odd, fill):
            even, lower = t - o, o - r
            merged.append(
                jnp.concatenate(
                    [even[:width], lower[:width], even[width:], lower[width:]], axis=0
                )
            )
        inv = merged
        width *= 2
    return inv


def fused_kernel(
    seq_axis, peers, axis, q_hbm, k_hbm, v_hbm, b_hbm, g_hbm, w_hbm, y_ref,
    b_ref, q_ref, k_ref, v_ref, g_ref, beta_ref, stack_ref, turn_ref, source_ref, x_ref, start_ref,
    low_ref, inv_ref, weight_ref, eye_ref,
    maps, held, carry_ref, states, s_ref, o_ref, m_ref,
    mixed, weight, total, far_out, far_in, near_out, near_in, cross_out, cross_in,
    b_sem, kv_sem, q_sem, g_sem, load_sem, map_send, map_recv, back_send, back_recv,
    far_send, far_recv, near_send, near_recv, cross_send, cross_recv,
):
    heads, blocks, span = q_ref.shape[0], q_ref.shape[1], q_ref.shape[2]
    pairs = heads // 2
    parts = 2
    batch = blocks // parts
    seq = lax.axis_index(seq_axis)
    me = lax.axis_index(axis)
    chip, core = me // 2, me % 2
    sibling = 2 * chip + 1 - core
    across = 2 * (1 - chip) + core
    beyond = 2 * (1 - chip) + 1 - core
    width = y_ref.shape[1]

    def columns(h):
        return pl.ds(pl.multiple_of(h * HEAD_DIM, HEAD_DIM), HEAD_DIM)

    def fetch_kv(h):
        return (
            pltpu.make_async_copy(k_hbm.at[:, :, :, columns(h)], k_ref.at[h], kv_sem.at[0, h]),
            pltpu.make_async_copy(v_hbm.at[:, :, :, columns(h)], v_ref.at[h], kv_sem.at[1, h]),
        )

    def fetch_q(h):
        return pltpu.make_async_copy(q_hbm.at[:, :, columns(h)], q_ref.at[h], q_sem.at[h])

    def fetch_g(h):
        return pltpu.make_async_copy(g_hbm.at[:, :, columns(h)], g_ref.at[h], g_sem.at[h])

    def load(n):
        owner = (beyond, across, sibling, me)[n]
        return pltpu.make_async_copy(
            w_hbm.at[:, pl.ds(pl.multiple_of(owner * width, width), width)],
            weight.at[n],
            load_sem.at[n],
        )

    def start_kv(first, last):
        for n in range(2):
            for h in range(first, last):
                fetch_kv(h)[n].start()

    fetch_b = pltpu.make_async_copy(b_hbm, b_ref, b_sem)
    fetch_b.start()
    start_kv(0, 2)
    barrier = pltpu.get_barrier_semaphore()
    for other in (sibling, across):
        pl.semaphore_signal(barrier, inc=1, device_id={axis: other}, device_id_type=MESH)
    for away in range(1, peers):
        pl.semaphore_signal(
            barrier,
            inc=1,
            device_id={seq_axis: lax.rem(seq + away, peers)},
            device_id_type=MESH,
        )

    eye_ref[...] = (iota(eye_ref.shape, 0) == iota(eye_ref.shape, 1)).astype(F32)
    fetch_b.wait()
    for blk in range(blocks):
        window = slice(blk * span, (blk + 1) * span)
        beta_ref[blk] = jnp.concatenate([b_ref[:, 0, window], b_ref[:, 1, window]], axis=1)

    def place(it, n):
        pair, part = it
        return 2 * pair + n % 2, part * batch + n // 2

    count = 2 * batch

    def key_of(h, blk):
        return jnp.concatenate([k_ref[h, 0, blk], k_ref[h, 1, blk]], axis=0)

    def stack_of(h, blk):
        none = jnp.zeros((HEAD_DIM, HEAD_DIM), BF16)
        return jnp.concatenate(
            [
                jnp.concatenate([stack_ref[h, blk, 0], stack_ref[h, blk, 2]], axis=1),
                jnp.concatenate([stack_ref[h, blk, 1], none], axis=1),
            ],
            axis=0,
        )

    def solve(it):
        slot = it[1]
        grams, squares = [], []
        for n in range(count):
            key = key_of(*place(it, n))
            grams.append(dot_t(key, key))
            if n % 2:
                yield
        for n, g in enumerate(grams):
            squares.append(jnp.sum(eye_ref[...] * g, axis=0, keepdims=True))
            if n % 4 == 3:
                yield
        beta = jnp.concatenate(
            [beta_ref[place(it, n)[1], pl.ds(place(it, n)[0], 1), :] for n in range(count)], axis=0
        )
        norm = lax.rsqrt(jnp.concatenate(squares, axis=0) + 1e-06)
        value_weight = beta * norm
        weight_rows = value_weight * norm
        weight_ref[slot, 0] = weight_rows
        weight_ref[slot, 1] = value_weight
        weight_cols = weight_rows.T
        yield
        lowers = []
        for n, g in enumerate(grams):
            low = weight_cols[:, n : n + 1] * g
            lowers.append(low)
            low_ref[slot, n, 0], low_ref[slot, n, 1] = split(low)
            if n % 2:
                yield
        inv = yield from base_solve(lowers, span)
        for n in range(count):
            inv_ref[slot, n] = inv[n]

    def transit(it):
        slot = it[1]

        def pieces(n):
            return low_ref[slot, n, 0], low_ref[slot, n, 1]

        solved = yield from merge([inv_ref[slot, n] for n in range(count)], pieces, span)
        turns, writes, changes = [], [], []
        for n in range(count):
            h, blk = place(it, n)
            th, tl = split(solved[n] * weight_ref[slot, 0, n : n + 1, :])
            tv = (solved[n] * weight_ref[slot, 1, n : n + 1, :]).astype(BF16)
            key = key_of(h, blk)
            value = jnp.concatenate([v_ref[h, 0, blk], v_ref[h, 1, blk]], axis=0)
            turns.append(
                dot(jnp.concatenate([th, tl], axis=1), jnp.concatenate([key, key], axis=0))
            )
            writes.append(dot(tv, value))
            yield
        for n in range(count):
            h, blk = place(it, n)
            turn_h, turn_l = split(turns[n])
            stack_ref[h, blk, 0], stack_ref[h, blk, 1] = turn_h, turn_l
            stack_ref[h, blk, 2] = writes[n].astype(BF16)
            stack = stack_of(h, blk)
            key_t = key_of(h, blk).T
            changes.append(dot(jnp.concatenate([key_t, key_t], axis=1), stack))
            yield
        for n in range(count):
            step = eye_ref[...] - changes[n][:, :HEAD_DIM]
            turn_ref[slot, n, 0], turn_ref[slot, n, 1] = split(step)
            source_ref[slot, n] = changes[n][:, HEAD_DIM:]
            yield

    def compose(it):
        slot = it[1]
        pair, _ = it
        states_now = [None if it[1] == 0 else x_ref[2 * pair + i] for i in range(2)]
        for n in range(count):
            h, blk = place(it, n)
            i = n % 2
            if blk == 0:
                turn_h, turn_l = turn_ref[slot, n, 0], turn_ref[slot, n, 1]
                states_now[i] = jnp.concatenate(
                    [turn_h.astype(F32) + turn_l.astype(F32), source_ref[slot, n]], axis=1
                )
                yield
                continue
            high, low = split(states_now[i])
            start_ref[h, blk, 0] = high[:, :HEAD_DIM]
            start_ref[h, blk, 1] = high[:, HEAD_DIM:]
            turn_h, turn_l = turn_ref[slot, n, 0], turn_ref[slot, n, 1]
            moved = dot(
                jnp.concatenate([turn_h, turn_l, turn_h], axis=1),
                jnp.concatenate([high, high, low], axis=0),
            )
            states_now[i] = jnp.concatenate(
                [moved[:, :HEAD_DIM], moved[:, HEAD_DIM:] + source_ref[slot, n]], axis=1
            )
            if n >= count - 2:
                x_ref[h] = states_now[i]
            yield

    def a_stream(it, first=0.0, last=1.0):
        return 7 * count // 4 + BASE + 1, solve(it), first, last

    def b_stream(it, first=0.0, last=1.0):
        return 9 * count, transit(it), first, last

    def c_stream(it, first=0.0, last=1.0):
        return count, compose(it), first, last

    def owner_of(pair, i):
        side = lax.rem(pair + core, 2)
        return peers // 2 - 2 + side + i * (3 - 2 * side)

    def send_map(pair, i, source):
        h = 2 * pair + i
        return pltpu.make_async_remote_copy(
            src_ref=maps.at[h],
            dst_ref=held.at[pair, source],
            send_sem=map_send.at[h],
            recv_sem=map_recv.at[pair // 2, source],
            device_id={seq_axis: owner_of(pair, i)},
            device_id_type=MESH,
        )

    def send_state(pair, i, target):
        h = 2 * pair + i
        return pltpu.make_async_remote_copy(
            src_ref=states.at[pair, target],
            dst_ref=s_ref.at[h],
            send_sem=back_send.at[pair // 2, target],
            recv_sem=back_recv.at[h],
            device_id={seq_axis: target},
            device_id_type=MESH,
        )

    def post(pair):
        for i in range(2):
            h = 2 * pair + i
            maps[h, 0] = x_ref[h, :, :HEAD_DIM].astype(BF16)
            maps[h, 1] = x_ref[h, :, HEAD_DIM:].astype(BF16)

            @pl.when((seq != owner_of(pair, i)) & (seq != peers - 1))
            def _():
                send_map(pair, i, seq).start()

            @pl.when(seq == owner_of(pair, i))
            def _():
                held[pair, seq] = maps[h]

    def chain(pair):
        for i in range(2):

            @pl.when(seq == owner_of(pair, i))
            def _():
                carry_ref[...] = jnp.zeros((HEAD_DIM, HEAD_DIM), F32)
                for k in range(peers - 1):

                    @pl.when(seq != k)
                    def _():
                        send_map(pair, i, k).wait_recv()

                    high, low = split(carry_ref[...])
                    turn = held[pair, k, 0]
                    state = held[pair, k, 1].astype(F32) + dot(
                        jnp.concatenate([turn, turn], axis=1),
                        jnp.concatenate([high, low], axis=0),
                    )
                    carry_ref[...] = state
                    states[pair, k + 1] = state.astype(BF16)

                    @pl.when(seq != k + 1)
                    def _():
                        send_state(pair, i, k + 1).start()

                    @pl.when(seq == k + 1)
                    def _():
                        s_ref[2 * pair + i] = states[pair, k + 1]

    @pl.when(seq == 0)
    def _():
        s_ref[...] = jnp.zeros(s_ref.shape, BF16)

    def wait_kv(pair):
        for i in range(2):
            for copy in fetch_kv(2 * pair + i):
                copy.wait()

    def after_values(pair, stream):
        for i in range(2):
            fetch_kv(2 * pair + i)[1].wait()
        yield from stream

    for h in range(2):
        fetch_kv(h)[0].wait()
    start_kv(2, heads)
    for h in range(heads):
        fetch_q(h).start()
    for n in range(4):
        load(n).start()
    for h in range(heads):
        fetch_g(h).start()
    weave(
        a_stream((0, 0), 0.0, 1.0),
        a_stream((0, 1), 0.8, 2.0),
        (9 * count, after_values(0, transit((0, 0))), 1.0, 2.1),
    )

    def step(pair, _):
        wait_kv(pair)
        weave(
            a_stream((pair, 0), 0.0, 1.0),
            b_stream((pair - 1, 1), 0.0, 1.0),
            c_stream((pair - 1, 0), 0.0, 1.0),
            a_stream((pair, 1), 1.05, 2.0),
            b_stream((pair, 0), 1.05, 2.0),
            c_stream((pair - 1, 1), 1.05, 2.0),
        )

        @pl.when(pair == 1)
        def _():
            pl.semaphore_wait(barrier, peers + 1)

        post(pair - 1)
        return 0

    lax.fori_loop(1, pairs, step, 0)
    weave(
        b_stream((pairs - 1, 1), 0.0, 9.0),
        c_stream((pairs - 1, 0), 0.0, 6.0),
        c_stream((pairs - 1, 1), 8.1, 9.1),
    )
    post(pairs - 1)
    for h in range(heads):
        fetch_q(h).wait()

    def read(pair, _):
        causal = iota((span, 2 * span), 1) % span <= iota((span, 2 * span), 0)
        for i in range(2):
            h = 2 * pair + i
            scores = []
            for blk in range(blocks):
                found = jnp.where(causal, dot_t(q_ref[h, blk], key_of(h, blk)), 0.0).astype(BF16)
                scores.append(jnp.concatenate([found, found], axis=1))
            drawn = [dot(score, stack_of(h, blk)) for blk, score in enumerate(scores)]
            for blk in range(blocks):
                kept = (q_ref[h, blk].astype(F32) - drawn[blk][:, :HEAD_DIM]).astype(BF16)
                if blk == 0:
                    m_ref[h, blk] = kept
                    o_ref[h, blk] = drawn[blk][:, HEAD_DIM:]
                    continue
                out = dot(kept, jnp.concatenate([start_ref[h, blk, 0], start_ref[h, blk, 1]], axis=1))
                m_ref[h, blk] = out[:, :HEAD_DIM].astype(BF16)
                o_ref[h, blk] = out[:, HEAD_DIM:] + drawn[blk][:, HEAD_DIM:]

        return 0

    def link(pair, _):
        chain(pair)
        return 0

    lax.fori_loop(0, 2, link, 0)
    lax.fori_loop(0, pairs // 2, read, 0)
    lax.fori_loop(2, pairs, link, 0)
    lax.fori_loop(pairs // 2, pairs, read, 0)
    for h in range(heads):
        fetch_g(h).wait()

    def wait_state(pair):
        for i in range(2):

            @pl.when((seq != owner_of(pair, i)) & (seq != 0))
            def _():
                send_state(pair, i, seq).wait_recv()

    def blend(pair, t):
        for i in range(2):
            h = 2 * pair + i
            query = q_ref[h, t].astype(F32)
            unit = lax.rsqrt(jnp.sum(query * query, axis=1, keepdims=True) + 1e-06)
            seen = unit * (o_ref[h, t] + dot(m_ref[h, t], s_ref[h]))
            scale = lax.rsqrt(jnp.mean(seen * seen, axis=1, keepdims=True) + 1e-06)
            gate = g_ref[h, t].astype(F32)
            mixed[t, h] = (seen * scale * (gate / (1.0 + jnp.exp(-gate)))).astype(BF16)

    def blend_pair(pair):
        wait_state(pair)
        for blk in range(blocks):
            blend(pair, blk)

    def settle(pair, _):
        blend_pair(pair)
        return 0

    lax.fori_loop(0, pairs - 1, settle, 0)

    sizes = [1, 1] + [2] * ((blocks - 4) // 2) + [1, 1]
    starts = [sum(sizes[:t]) for t in range(len(sizes))]

    def rows(t):
        return pl.ds(starts[t] * span, sizes[t] * span)

    def send(source, target, send_sem, recv_sem, t, device):
        return pltpu.make_async_remote_copy(
            src_ref=source.at[rows(t)],
            dst_ref=target.at[rows(t)],
            send_sem=send_sem.at[t],
            recv_sem=recv_sem.at[t],
            device_id={axis: device},
            device_id_type=MESH,
        )

    def far(t):
        return send(far_out, far_in, far_send, far_recv, t, sibling)

    def near(t):
        return send(near_out, near_in, near_send, near_recv, t, sibling)

    def cross(t):
        return send(cross_out, cross_in, cross_send, cross_recv, t, across)

    def pass_on(t):
        far(t).wait()
        cross_out[rows(t)] = (total[rows(t)] + far_in[rows(t)].astype(F32)).astype(BF16)
        cross(t).start()

    def mixed_of(t, first, last):
        return jnp.concatenate(
            [
                jnp.concatenate([mixed[starts[t] + b, h] for h in range(first, last)], axis=1)
                for b in range(sizes[t])
            ],
            axis=0,
        )

    def product(t, n):
        return dot(mixed_of(t, 0, heads), weight[n])

    def finish_piece(t):
        for b in range(sizes[t]):
            blend(pairs - 1, starts[t] + b)

    count_pieces = len(sizes)
    early = (heads - 2) * HEAD_DIM
    load(0).wait()
    total[rows(0)] = dot(mixed_of(0, 0, heads - 2), weight[0, :early, :])
    wait_state(pairs - 1)
    finish_piece(0)
    late = dot(mixed_of(0, heads - 2, heads), weight[0, early:, :])
    far_out[rows(0)] = (total[rows(0)] + late).astype(BF16)
    far(0).start()
    load(1).wait()
    finish_piece(1)
    total[rows(0)] = product(0, 1)
    for t in range(1, count_pieces):
        if t > 1:
            finish_piece(t)
        far_out[rows(t)] = product(t, 0).astype(BF16)
        far(t).start()
        pass_on(t - 1)
        total[rows(t)] = product(t, 1)
    load(2).wait()
    for t in range(count_pieces):
        near_out[rows(t)] = product(t, 2).astype(BF16)
        near(t).start()
        if t == 0:
            pass_on(count_pieces - 1)
    load(3).wait()
    for t in range(count_pieces):
        total[rows(t)] = product(t, 3)
    for t in range(count_pieces):
        near(t).wait()
        total[rows(t)] = total[rows(t)] + near_in[rows(t)].astype(F32)
    for pair in range(pairs):
        for i in range(2):

            @pl.when((seq != owner_of(pair, i)) & (seq != peers - 1))
            def _():
                send_map(pair, i, seq).wait_send()

            @pl.when(seq == owner_of(pair, i))
            def _():
                for k in range(1, peers):

                    @pl.when(seq != k)
                    def _():
                        send_state(pair, i, k).wait_send()
    for t in range(count_pieces):
        cross(t).wait()
        y_ref[rows(t)] = (total[rows(t)] + cross_in[rows(t)].astype(F32)).astype(BF16)


def fused(queries, keys, values, betas, gate, out_weight, seq_axis, axis):
    tokens, depth = queries.shape
    heads = depth // HEAD_DIM
    peers = lax.axis_size(seq_axis)
    width = out_weight.shape[1] // lax.axis_size(axis)
    blocks = tokens // SPAN
    batch = blocks // 2
    hbm = pl.BlockSpec(memory_space=pltpu.HBM)
    piece = (tokens, width)
    pieces = blocks // 2 + 2
    square = (HEAD_DIM, HEAD_DIM)
    wide = (HEAD_DIM, 2 * HEAD_DIM)
    two = (2,) + square
    pairs = heads // 2
    dma = pltpu.SemaphoreType.DMA
    per_head = (heads, blocks, SPAN, HEAD_DIM)
    both = (heads, 2, blocks, SPAN, HEAD_DIM)
    return pl.pallas_call(
        functools.partial(fused_kernel, seq_axis, peers, axis),
        in_specs=[hbm] * 6,
        out_specs=pl.BlockSpec(memory_space=pltpu.VMEM),
        out_shape=jax.ShapeDtypeStruct(piece, BF16),
        scratch_shapes=[
            pltpu.VMEM(betas.shape, F32),
            pltpu.VMEM(per_head, BF16),
            pltpu.VMEM(both, BF16),
            pltpu.VMEM(both, BF16),
            pltpu.VMEM(per_head, BF16),
            pltpu.VMEM((blocks, heads, 2 * SPAN), F32),
            pltpu.VMEM((heads, blocks, 3) + square, BF16),
            pltpu.VMEM((2, 2 * batch) + two, BF16),
            pltpu.VMEM((2, 2 * batch) + square, F32),
            pltpu.VMEM((heads,) + wide, F32),
            pltpu.VMEM((heads, blocks) + two, BF16),
            pltpu.VMEM((2, 2 * batch) + two, BF16),
            pltpu.VMEM((2, 2 * batch, BASE, 2 * SPAN), F32),
            pltpu.VMEM((2, 2, 2 * batch, 2 * SPAN), F32),
            pltpu.VMEM(square, F32),
            pltpu.VMEM((heads,) + two, BF16),
            pltpu.VMEM((pairs, peers) + two, BF16),
            pltpu.VMEM(square, F32),
            pltpu.VMEM((pairs, peers) + square, BF16),
            pltpu.VMEM((heads,) + square, BF16),
            pltpu.VMEM(per_head, F32),
            pltpu.VMEM(per_head, BF16),
            pltpu.VMEM((blocks, heads, SPAN, HEAD_DIM), BF16),
            pltpu.VMEM((4, depth, width), BF16),
            pltpu.VMEM(piece, F32),
        ]
        + [pltpu.VMEM(piece, BF16)] * 6
        + [
            dma,
            dma((2, heads)),
            dma((heads,)),
            dma((heads,)),
            dma((4,)),
            dma((heads,)),
            dma((pairs // 2, peers)),
            dma((pairs // 2, peers)),
            dma((heads,)),
        ]
        + [dma((pieces,))] * 6,
        compiler_params=pltpu.CompilerParams(
            collective_id=0, has_side_effects=True, vmem_limit_bytes=FUSED_LIMIT
        ),
    )(
        queries.reshape(blocks, SPAN, depth),
        keys.reshape(2, blocks, SPAN, depth),
        values.reshape(2, blocks, SPAN, depth),
        pltpu.with_memory_space_constraint(betas, pltpu.HBM),
        gate.reshape(blocks, SPAN, depth),
        out_weight,
    )


def start_state(maps, axis):
    peers, index = lax.axis_size(axis), lax.axis_index(axis)
    heads = maps.shape[0]
    held = lax.all_gather(maps, axis, axis=0, tiled=True)
    states = pl.pallas_call(
        functools.partial(chain_kernel, peers),
        out_shape=jax.ShapeDtypeStruct((held.shape[0], HEAD_DIM, HEAD_DIM), BF16),
        compiler_params=pltpu.CompilerParams(vmem_limit_bytes=VMEM_LIMIT),
    )(held)
    return lax.dynamic_slice_in_dim(states, index * heads, heads, 0)


def out_kernel(o_ref, m_ref, s_ref, g_ref, w_ref, y_ref, mixed_ref):
    @pl.when(pl.program_id(0) == 0)
    def _():
        for h in range(s_ref.shape[0]):
            cols = slice(h * HEAD_DIM, (h + 1) * HEAD_DIM)
            seen = o_ref[:, cols] + dot(m_ref[:, cols], s_ref[h])
            scale = lax.rsqrt(jnp.mean(seen * seen, axis=1, keepdims=True) + 1e-06)
            gate = g_ref[:, cols].astype(F32)
            mixed_ref[:, cols] = (seen * scale * (gate / (1.0 + jnp.exp(-gate)))).astype(BF16)

    y_ref[...] = dot(mixed_ref[...], w_ref[...]).astype(BF16)


def project(local, reach, states, gate, out_weight):
    tokens, width = local.shape
    total = out_weight.shape[1]
    tile = 512
    whole = pl.BlockSpec((tokens, width), lambda n: (0, 0))
    return pl.pallas_call(
        out_kernel,
        grid=(total // tile,),
        in_specs=[
            whole,
            whole,
            pl.BlockSpec(states.shape, lambda n: (0, 0, 0)),
            whole,
            pl.BlockSpec((width, tile), lambda n: (0, n)),
        ],
        out_specs=pl.BlockSpec((tokens, tile), lambda n: (0, n)),
        out_shape=jax.ShapeDtypeStruct((tokens, total), BF16),
        scratch_shapes=[pltpu.VMEM((tokens, width), BF16)],
        compiler_params=pltpu.CompilerParams(
            dimension_semantics=("arbitrary",), vmem_limit_bytes=VMEM_LIMIT
        ),
    )(local, reach, states, gate, out_weight)


def per_device(queries, keys, values, betas, gate, out_weight):
    heads, _, tokens = betas.shape
    peers, index = lax.axis_size("ctx"), lax.axis_size("head")
    if index == 4 and peers >= 4 and peers % 2 == 0 and heads % 8 == 0 and tokens % (8 * SPAN) == 0:
        return fused(queries, keys, values, betas, gate, out_weight, "ctx", "head")
    beta_cols = betas.transpose(2, 1, 0).reshape(2 * tokens, heads)
    local, reach, maps = mix(queries, keys, values, beta_cols)
    states = start_state(maps, "ctx")
    partial_sum = project(local, reach, states, gate, out_weight)
    return lax.psum_scatter(partial_sum, "head", scatter_dimension=1, tiled=True)


def solution(mesh):
    return jax.shard_map(
        per_device,
        mesh=mesh,
        in_specs=(
            P("ctx", "head"),
            P(None, "ctx", "head"),
            P(None, "ctx", "head"),
            P("head", None, "ctx"),
            P("ctx", "head"),
            P("head", None),
        ),
        out_specs=P("ctx", "head"),
        check_vma=False,
    )
```
